128 devices in a mesh: mesh: 2 (over core), dom: 64 (over z, x, y).
Axes of the slice: x: 4, y: 4, z: 4, core: 2. Of those that a mesh axis runs over, the one named last changes fastest.
Arguments:
- donor_fields: float32 [5, 512, 16384], P(None, None, ('mesh', 'dom')), may hold values from -6 to 6
- interp_weights: float32 [3, 8, 262144], P(None, None, ('mesh', 'dom')), may hold values from -1 to 1, as said below
- donor_owner: int32 [262144, 1], P(('mesh', 'dom')), may hold values from 0 to 63, as said below
- donor_element: int32 [262144], P(('mesh', 'dom')), may hold values from 0 to 127
- geometry: float32 [4, 16384], P(None, ('mesh', 'dom')), may hold values from 0.25 to 4
- wall_flag: int32 [2, 1024], P(None, ('mesh', 'dom')), may hold values 0 or 1
- forcing: float32 [512, 16384], P(None, ('mesh', 'dom')), may hold values from -6 to 6
Outputs:
- velocity: float32 [512, 16384], P(None, ('mesh', 'dom'))
- residual: float32 [512, 16384], P(None, ('mesh', 'dom'))
- interface_values: float32 [5, 262144], P(None, ('mesh', 'dom'))
The draws below stay inside these ranges and needn't reach their ends.
Inputs may be any that keep to these rules, and one draw needn't show every extreme that they name: `interp_weights`: for each receptor and direction, the 8 entries are the Lagrange polynomials of the order-7 Gauss-Lobatto-Legendre points evaluated at one point of [-1, 1]. `donor_owner`: the receptors of block q of a mesh (the rows of one device) name donor dom indices from q - 2 to q + 2 only; among them one index is named exactly 1024 times and no index more often.
All inputs are finite; a program needn't handle non-finite values. No bound on the sum of `wall_flag` on one device may be relied on, other than what follows from the above.
Results may differ from the reference program's by a relative error of at most 0.00026.
Values sent between devices are 32-bit elements; how exact they have to be, the bound alone decides.
No kernel may reach another device: no remote copies, remote signals or barrier semaphores. Data moves between devices by JAX's collectives and lax.ppermute only.
A program may use at most 192 MiB of HBM per device.

```python
import math
import jax
import jax.numpy as jnp
import numpy as np
from jax import lax

FIELDS = 5
EX = 8
EY = 16
EZ_DEV = 1
ITERS = 3
PTS = 512
E_DEV = 128
E_TOTAL = 16384
R_DEV = 2048
R_TOTAL = 262144
CAP = 1024
W_TOTAL = 1024
N_MESH = 2
N_DOM = 64


def legendre_pair_drawn(values, degree):
    previous = values * 0.0 + 1.0
    current = values * 1.0
    for poly_order in range(2, degree + 1):
        previous, current = (current, ((2 * poly_order - 1) * values * current - (poly_order - 1) * previous) / poly_order)
    return (current, previous)


def gll_abscissae():
    degree = 7
    points_count = degree + 1
    abscissae = np.cos(np.pi * np.arange(points_count) / degree)
    for newton_turn in range(80):
        top_poly, lower_poly = legendre_pair_drawn(abscissae, degree)
        abscissae = abscissae - (abscissae * top_poly - lower_poly) / (points_count * top_poly)
    return np.sort(abscissae)


def draw_interp_weights(key, part):
    abscissae = gll_abscissae()
    location = jax.random.uniform(key, (3, R_TOTAL), jnp.float32, -1.0, 1.0)
    basis_rows = []
    for node_index in range(8):
        product = jnp.ones_like(location)
        for partner in range(8):
            if partner != node_index:
                product = product * (location - abscissae[partner]) / (abscissae[node_index] - abscissae[partner])
        basis_rows.append(product)
    return jnp.stack(basis_rows, 1).astype(jnp.float32)


def draw_donor_owner(key, part):
    block_count = N_MESH * N_DOM
    slab_index = jnp.arange(block_count, dtype=jnp.int32) % N_DOM
    lowest = jnp.maximum(slab_index - 2, 0)
    highest = jnp.minimum(slab_index + 2, N_DOM - 1)
    window = highest - lowest + 1
    hot_owner = lowest + jax.random.randint(jax.random.fold_in(key, 11), (block_count,), 0, window)
    picks = jax.random.randint(jax.random.fold_in(key, 13), (block_count, R_DEV), 0, (window - 1)[:, None])
    other_owner = lowest[:, None] + picks
    other_owner = other_owner + (other_owner >= hot_owner[:, None]).astype(jnp.int32)
    block_keys = jax.random.split(jax.random.fold_in(key, 17), block_count)
    ranks = jax.vmap(lambda one_key: jax.random.permutation(one_key, R_DEV))(block_keys)
    owner = jnp.where(ranks < CAP, hot_owner[:, None], other_owner)
    return owner.reshape(R_TOTAL, 1).astype(jnp.int32)


def place_ends(values, own_key, smallest, largest):
    index_at = [jax.random.randint(jax.random.fold_in(own_key, axis), (), 0, length) for axis, length in enumerate(values.shape)]
    main_axis = values.shape.index(max(values.shape))
    next_to = index_at[:main_axis] + [(index_at[main_axis] + 1) % values.shape[main_axis]] + index_at[main_axis + 1:]
    return values.at[tuple(index_at)].set(smallest).at[tuple(next_to)].set(largest)


def shard_levels(own_key, shape, pieces, least, top_value):
    loudness = 1.0
    for axis_at, blocks in pieces:
        draws = jax.random.uniform(jax.random.fold_in(jax.random.fold_in(own_key, 6), axis_at), (blocks,), jnp.float32, least / len(pieces), top_value / len(pieces))
        loudness = loudness * jnp.repeat(jnp.exp(draws), shape[axis_at] // blocks).reshape((-1,) + (1,) * (len(shape) - 1 - axis_at))
    return loudness


def noise(key, dims, deviation, bound, shards=(), kind=jnp.bfloat16):
    values = jax.random.normal(key, dims, jnp.float32) * deviation
    if len(shards) > 0:
        values = shard_levels(key, dims, shards, -0.22, 0.18) * values
    return jnp.clip(values, min=-bound, max=bound).astype(kind)


def setup_inputs(seed: int = 0) -> dict:
    seeds = jax.random.split(jax.random.key(seed), 8)
    donor_fields = noise(seeds[0], (FIELDS, PTS, E_TOTAL), 1.0, 6.0, ((2, 128),), jnp.float32)
    interp_weights = draw_interp_weights(jax.random.fold_in(seeds[7], 71), 0)
    donor_owner = draw_donor_owner(jax.random.fold_in(seeds[7], 71), 0)
    donor_element = place_ends(jax.random.randint(seeds[3], (R_TOTAL,), 0, E_DEV), jax.random.fold_in(seeds[3], 1), 0, E_DEV - 1).astype(jnp.int32)
    geometry = jnp.clip(jnp.exp(math.log(4.0) - 2.7725887 * jax.random.uniform(seeds[4], (4, E_TOTAL), jnp.float32) ** shard_levels(seeds[4], (4, E_TOTAL), ((1, 128),), -0.2, 0.2)), 0.25, 4.0)
    wall_flag = place_ends((jax.random.randint(seeds[5], (2, W_TOTAL), 0, 4) < 3).astype(jnp.int32), jax.random.fold_in(seeds[5], 1), 0, 1)
    forcing = noise(seeds[6], (PTS, E_TOTAL), 1.0, 6.0, ((1, 128),), jnp.float32)
    return {"donor_fields": donor_fields, "interp_weights": interp_weights, "donor_owner": donor_owner, "donor_element": donor_element, "geometry": geometry, "wall_flag": wall_flag, "forcing": forcing}


HIGHEST = lax.Precision.HIGHEST


def legendre_pair(values, degree):
    previous = values * 0.0 + 1.0
    current = values * 1.0
    for poly_order in range(2, degree + 1):
        previous, current = current, ((2 * poly_order - 1) * values * current - (poly_order - 1) * previous) / poly_order
    return current, previous


def gll_tables():
    degree = 7
    points_count = degree + 1
    abscissae = np.cos(np.pi * np.arange(points_count) / degree)
    for newton_turn in range(80):
        top_poly, lower_poly = legendre_pair(abscissae, degree)
        abscissae = abscissae - (abscissae * top_poly - lower_poly) / (points_count * top_poly)
    abscissae = np.sort(abscissae)
    top_poly, lower_poly = legendre_pair(abscissae, degree)
    quad_weights = 2.0 / (degree * points_count * top_poly * top_poly)
    identity_mat = np.eye(points_count)
    spacing = abscissae[:, None] - abscissae[None, :] + identity_mat
    derivative = (top_poly[:, None] / (top_poly[None, :] * spacing)) * (1.0 - identity_mat)
    derivative[0, 0] = -degree * points_count / 4.0
    derivative[degree, degree] = degree * points_count / 4.0
    return jnp.asarray(derivative, jnp.float32), jnp.asarray(quad_weights, jnp.float32)


def cube_weights(quad_weights):
    return quad_weights[:, None, None, None] * quad_weights[None, :, None, None] * quad_weights[None, None, :, None]


def local_operator(field_data, geometry, derivative, quad_weights):
    weights_cube = cube_weights(quad_weights)
    grad_x = jnp.einsum('ai,kjie->kjae', derivative, field_data, precision=HIGHEST)
    grad_y = jnp.einsum('aj,kjie->kaie', derivative, field_data, precision=HIGHEST)
    grad_z = jnp.einsum('ak,kjie->ajie', derivative, field_data, precision=HIGHEST)
    result = jnp.einsum('ai,kjae->kjie', derivative, grad_x * (weights_cube * geometry[0]), precision=HIGHEST)
    result = result + jnp.einsum('aj,kaie->kjie', derivative, grad_y * (weights_cube * geometry[1]), precision=HIGHEST)
    result = result + jnp.einsum('ak,ajie->kjie', derivative, grad_z * (weights_cube * geometry[2]), precision=HIGHEST)
    return result + (weights_cube * geometry[3]) * field_data


def local_diagonal(geometry, derivative, quad_weights):
    stiff_diag = jnp.sum(derivative * derivative * quad_weights[:, None], axis=0)
    along_x = (quad_weights[:, None, None] * quad_weights[None, :, None] * stiff_diag[None, None, :])[..., None]
    along_y = (quad_weights[:, None, None] * stiff_diag[None, :, None] * quad_weights[None, None, :])[..., None]
    along_z = (stiff_diag[:, None, None] * quad_weights[None, :, None] * quad_weights[None, None, :])[..., None]
    return along_x * geometry[0] + along_y * geometry[1] + along_z * geometry[2] + cube_weights(quad_weights) * geometry[3]


def direct_sum(field_data):
    paired = field_data[:, :, :, -1, :, :, :-1] + field_data[:, :, :, 0, :, :, 1:]
    field_data = field_data.at[:, :, :, -1, :, :, :-1].set(paired).at[:, :, :, 0, :, :, 1:].set(paired)
    paired = field_data[:, :, -1, :, :, :-1, :] + field_data[:, :, 0, :, :, 1:, :]
    field_data = field_data.at[:, :, -1, :, :, :-1, :].set(paired).at[:, :, 0, :, :, 1:, :].set(paired)
    paired = field_data[:, -1, :, :, :-1, :, :] + field_data[:, 0, :, :, 1:, :, :]
    field_data = field_data.at[:, -1, :, :, :-1, :, :].set(paired).at[:, 0, :, :, 1:, :, :].set(paired)
    return field_data


def reference(donor_fields, interp_weights, donor_owner, donor_element, geometry, wall_flag, forcing):
    derivative, quad_weights = gll_tables()
    elem_dev = EX * EY * EZ_DEV
    elem_mesh = elem_dev * N_DOM
    rec_mesh = R_DEV * N_DOM
    layers = EZ_DEV * N_DOM
    receptor_mesh = jnp.arange(R_TOTAL, dtype=jnp.int32) // rec_mesh
    target = ((1 - receptor_mesh) * elem_mesh + donor_owner[:, 0] * elem_dev + donor_element).astype(jnp.int32)
    blocks = N_MESH * N_DOM
    target_blocks = target.reshape(blocks, R_DEV)
    weight_blocks = jnp.transpose(interp_weights.reshape(3, 8, blocks, R_DEV), (2, 0, 1, 3))

    def evaluate(block_pair):
        target_row, weight_row = block_pair
        gathered = jnp.take(donor_fields, target_row, axis=2).reshape(FIELDS, 8, 8, 8, R_DEV)
        reduced = jnp.einsum('fkjib,ib->fkjb', gathered, weight_row[0], precision=HIGHEST)
        reduced = jnp.einsum('fkjb,jb->fkb', reduced, weight_row[1], precision=HIGHEST)
        return jnp.einsum('fkb,kb->fb', reduced, weight_row[2], precision=HIGHEST)

    evaluated = lax.map(evaluate, (target_blocks, weight_blocks))
    interface_values = jnp.transpose(evaluated, (1, 0, 2)).reshape(FIELDS, R_TOTAL)

    brick_shape = (8, 8, 8, layers, EY, EX)
    flat_shape = (8, 8, 8, elem_mesh)
    weights_cube = cube_weights(quad_weights)
    velocities = []
    residuals = []
    for mesh_index in range(N_MESH):
        first_column = mesh_index * elem_mesh
        mesh_geometry = geometry[:, first_column:first_column + elem_mesh]
        source = forcing[:, first_column:first_column + elem_mesh].reshape(flat_shape)
        received = interface_values[0, mesh_index * rec_mesh:(mesh_index + 1) * rec_mesh]
        received = received.reshape(N_DOM, 2, EZ_DEV, EY, 8, 8)
        side_values = jnp.transpose(received, (1, 4, 5, 0, 2, 3)).reshape(2, 8, 8, layers, EY)
        wall_bits = wall_flag[:, mesh_index * EX * layers:(mesh_index + 1) * EX * layers].reshape(2, layers, EX)
        wall_bits = wall_bits.astype(jnp.float32)
        zero_brick = jnp.zeros(brick_shape, jnp.float32)
        rec_value = zero_brick.at[:, :, 0, :, :, 0].set(side_values[0]).at[:, :, -1, :, :, -1].set(side_values[1])
        rec_mark = zero_brick.at[:, :, 0, :, :, 0].set(1.0).at[:, :, -1, :, :, -1].set(1.0)
        wall_low = jnp.broadcast_to(wall_bits[0], (8, 8, layers, EX))
        wall_high = jnp.broadcast_to(wall_bits[1], (8, 8, layers, EX))
        wall_mark = zero_brick.at[:, 0, :, :, 0, :].set(wall_low).at[:, -1, :, :, -1, :].set(wall_high)
        diag_brick = local_diagonal(mesh_geometry, derivative, quad_weights).reshape(brick_shape)
        unit_brick = jnp.ones(brick_shape, jnp.float32)
        summed = direct_sum(jnp.stack([rec_value, rec_mark, wall_mark, unit_brick, diag_brick], 0))
        summed = summed.reshape((5,) + flat_shape)
        free_mask = 1.0 - jnp.minimum(summed[1] + summed[2], 1.0)
        boundary = summed[0] / jnp.maximum(summed[1], 1.0)
        multiplicity = summed[3]
        inverse = free_mask / summed[4]

        def apply_operator(vector):
            local_term = local_operator(vector, mesh_geometry, derivative, quad_weights)
            return free_mask * direct_sum(local_term.reshape((1,) + brick_shape))[0].reshape(flat_shape)

        def inner(left, right):
            return jnp.sum(left * right / multiplicity)

        loaded = (weights_cube * mesh_geometry[3]) * source - local_operator(boundary, mesh_geometry, derivative, quad_weights)
        rhs = free_mask * direct_sum(loaded.reshape((1,) + brick_shape))[0].reshape(flat_shape)
        solution = jnp.zeros(flat_shape, jnp.float32)
        residual_now = rhs
        precond = inverse * residual_now
        direction = precond
        precond_norm = inner(residual_now, precond)
        for iteration in range(ITERS):
            operator_image = apply_operator(direction)
            step_length = precond_norm / inner(direction, operator_image)
            solution = solution + step_length * direction
            residual_now = residual_now - step_length * operator_image
            if iteration + 1 < ITERS:
                precond = inverse * residual_now
                norm_next = inner(residual_now, precond)
                direction = precond + (norm_next / precond_norm) * direction
                precond_norm = norm_next
        velocities.append((boundary + solution).reshape(PTS, elem_mesh))
        residuals.append(residual_now.reshape(PTS, elem_mesh))
    return jnp.concatenate(velocities, 1), jnp.concatenate(residuals, 1), interface_values
```

```python
import functools

import jax
import jax.numpy as jnp
import numpy as np
from jax import lax
from jax.experimental import pallas as pl
from jax.experimental.pallas import tpu as pltpu
from jax.sharding import PartitionSpec as P

HIGHEST = lax.Precision.HIGHEST
N_DOM = 64
N_REC = 2048
CAP = 1024
FIELDS = 5
LANES = 128
BLOCK = 256
ALIGNED = [[4 * g + t for t in range(4)] for g in range(16)]
SHIFTED = [[(4 * g + 2 + t) % N_DOM for t in range(4)] for g in range(16)]
UP = [(i, i + 1) for i in range(N_DOM - 1)]
DOWN = [(i + 1, i) for i in range(N_DOM - 1)]


def legendre_pair(values, degree):
    previous = values * 0.0 + 1.0
    current = values * 1.0
    for order in range(2, degree + 1):
        previous, current = (
            current,
            ((2 * order - 1) * values * current - (order - 1) * previous) / order,
        )
    return current, previous


def gll_tables():
    degree = 7
    count = degree + 1
    nodes = np.cos(np.pi * np.arange(count) / degree)
    for _ in range(80):
        top, lower = legendre_pair(nodes, degree)
        nodes = nodes - (nodes * top - lower) / (count * top)
    nodes = np.sort(nodes)
    top, lower = legendre_pair(nodes, degree)
    weights = 2.0 / (degree * count * top * top)
    identity = np.eye(count)
    spacing = nodes[:, None] - nodes[None, :] + identity
    derivative = top[:, None] / (top[None, :] * spacing) * (1.0 - identity)
    derivative[0, 0] = -degree * count / 4.0
    derivative[degree, degree] = degree * count / 4.0
    return nodes, weights, derivative


NODES, WEIGHTS, DERIV = gll_tables()
STIFF = DERIV.T @ (WEIGHTS[:, None] * DERIV)
STIFF = 0.5 * (STIFF + STIFF.T)
BARY = np.array([1.0 / np.prod([NODES[i] - NODES[j] for j in range(8) if j != i]) for i in range(8)])


def x_matrix():
    out = np.zeros((512, 256))
    for k in range(8):
        for j in range(8):
            row = (k * 8 + j) * 8
            col = row % 256
            out[row : row + 8, col : col + 8] = WEIGHTS[k] * WEIGHTS[j] * STIFF
    return out.astype(np.float32)


def iota(shape, dim):
    return lax.broadcasted_iota(jnp.int32, shape, dim)


def w_column():
    row = iota((8, LANES), 0)
    out = jnp.full((8, LANES), float(WEIGHTS[0]), jnp.float32)
    for i in range(1, 8):
        out = jnp.where(row == i, float(WEIGHTS[i]), out)
    return out


def s_column():
    row = iota((8, LANES), 0)
    out = jnp.full((8, LANES), float(STIFF[0, 0]), jnp.float32)
    for i in range(1, 8):
        out = jnp.where(row == i, float(STIFF[i, i]), out)
    return out


def sum_xy(ref, planes):
    rows = planes * 8
    lane = iota((rows, LANES), 1)
    low = ref[pl.ds(0, rows, stride=8), :]
    high = ref[pl.ds(7, rows, stride=8), :]
    ref[pl.ds(7, rows, stride=8), :] = high + jnp.where(
        lane % 8 < 7, pltpu.roll(low, LANES - 1, 1), 0.0
    )
    ref[pl.ds(0, rows, stride=8), :] = low + jnp.where(lane % 8 > 0, pltpu.roll(high, 1, 1), 0.0)
    lane = iota((8, LANES), 1)
    for k in range(planes):
        low = ref[k * 64 : k * 64 + 8, :]
        high = ref[k * 64 + 56 : k * 64 + 64, :]
        ref[k * 64 + 56 : k * 64 + 64, :] = high + jnp.where(
            lane < 120, pltpu.roll(low, LANES - 8, 1), 0.0
        )
        ref[k * 64 : k * 64 + 8, :] = low + jnp.where(lane >= 8, pltpu.roll(high, 8, 1), 0.0)


def apply_local(v_ref, geometry, xmat_ref, out_ref, planes, dot_with_v=False):
    wcol = w_column()
    gx = geometry[0:1, :]
    gyw = geometry[1:2, :] * wcol
    gzw = geometry[2:3, :] * wcol
    gmw = geometry[3:4, :] * wcol
    total = jnp.zeros((8, LANES), jnp.float32)
    if len(planes) == 8:
        along_x = [
            lax.dot(
                xmat_ref[256 * h : 256 * h + 256, :],
                v_ref[256 * h : 256 * h + 256, :],
                precision=HIGHEST,
                preferred_element_type=jnp.float32,
            )
            for h in range(2)
        ]
        for h in range(2):
            out_ref[256 * h : 256 * h + 256, :] = along_x[h]
    else:
        for at, k in enumerate(planes):
            h = k // 4
            out_ref[at * 64 : at * 64 + 64, :] = lax.dot(
                xmat_ref[k * 64 : k * 64 + 64, :],
                v_ref[256 * h : 256 * h + 256, :],
                precision=HIGHEST,
                preferred_element_type=jnp.float32,
            )
    for at, k in enumerate(planes):
        plane = [v_ref[(k * 8 + j) * 8 : (k * 8 + j) * 8 + 8, :] for j in range(8)]
        for j in range(8):
            ysum = plane[0] * float(STIFF[j, 0] * WEIGHTS[k])
            for jj in range(1, 8):
                ysum = ysum + plane[jj] * float(STIFF[j, jj] * WEIGHTS[k])
            zsum = None
            for kk in range(8):
                term = v_ref[(kk * 8 + j) * 8 : (kk * 8 + j) * 8 + 8, :] * float(
                    STIFF[k, kk] * WEIGHTS[j]
                )
                zsum = term if zsum is None else zsum + term
            row = (at * 8 + j) * 8
            value = (
                out_ref[row : row + 8, :] * gx
                + gyw * ysum
                + gzw * zsum
                + gmw * (plane[j] * float(WEIGHTS[k] * WEIGHTS[j]))
            )
            out_ref[row : row + 8, :] = value
            if dot_with_v:
                total = total + value * plane[j]
    return total


def lane_value(value, at):
    return jnp.where(iota((1, LANES), 1) == at, value, 0.0)


def route_kernel(place_ref, weights_ref, owner_ref, element_ref, near_ref, far_ref, moves_ref, slots_ref):
    q = place_ref[0]
    width = N_REC
    lane = iota((8, width), 1)
    row = iota((8, width), 0)
    distance = owner_ref[...] - q + 2
    mine = distance == row
    count = mine.astype(jnp.int32)
    step = 1
    while step < width:
        count = count + jnp.where(lane >= step, pltpu.roll(count, step, 1), 0)
        step *= 2
    moves = jnp.where(mine, lane - (count - 1), 0)
    totals = count[:, width - 1 : width]
    node_rows = iota((8, width), 0)
    node = jnp.full((8, width), float(NODES[0]), jnp.float32)
    for i in range(1, 8):
        node = jnp.where(node_rows == i, float(NODES[i]), node)
    coords = [jnp.sum(weights_ref[d] * node, axis=0, keepdims=True) for d in range(3)]
    words = element_ref[...].astype(jnp.float32)
    base = jnp.where(row % 4 == 3, words, 0.0)
    for d in range(3):
        base = jnp.where(row % 4 == d, coords[d], base)
    packs = [base, base, base]
    for b in range(11):
        step = 1 << b
        incoming = pltpu.roll(moves, width - step, 1)
        moved = (incoming >> b) & 1
        for n in range(3):
            first = jnp.broadcast_to(moved[2 * n : 2 * n + 1, :], (8, width))
            if n < 2:
                second = jnp.broadcast_to(moved[2 * n + 1 : 2 * n + 2, :], (8, width))
                first = jnp.where(row < 4, first, second)
            packs[n] = jnp.where(first == 1, pltpu.roll(packs[n], width - step, 1), packs[n])
        moves = jnp.where(moved == 1, incoming, jnp.where((moves >> b) & 1 == 1, 0, moves))
    moves_ref[...] = moves[:, :CAP]
    slots_ref[...] = jnp.full(slots_ref.shape, -1.0, jnp.float32)
    lane = iota((4, CAP), 1)
    for s in range(5):
        at = (s % 2) * 4
        slots_ref[s + 4] = jnp.where(
            lane < totals[s : s + 1, :], packs[s // 2][at : at + 4, :CAP], -1.0
        )
    r = q % 4
    rs = (q + 2) % 4
    for t in range(4):
        near_ref[t] = slots_ref[t - r + 6]
        off = t - rs
        inside = (r + off >= 0) & (r + off <= 3)
        far_ref[t] = slots_ref[jnp.where(inside, 0, off + 6)]


def split_kernel(fields_ref, out_ref):
    for f in range(FIELDS):
        value = fields_ref[f]
        high = value.astype(jnp.bfloat16)
        out_ref[f, :, 0:LANES] = high
        out_ref[f, :, LANES : 2 * LANES] = (value - high.astype(jnp.float32)).astype(jnp.bfloat16)


def basis_rows(coordinate):
    gaps = [coordinate - float(NODES[i]) for i in range(8)]
    before = [None] * 8
    after = [None] * 8
    for i in range(1, 8):
        before[i] = gaps[i - 1] if i == 1 else before[i - 1] * gaps[i - 1]
    for i in range(6, -1, -1):
        after[i] = gaps[i + 1] if i == 6 else after[i + 1] * gaps[i + 1]
    out = []
    for i in range(8):
        if i == 0:
            value = after[0]
        elif i == 7:
            value = before[7]
        else:
            value = before[i] * after[i]
        out.append(value * float(BARY[i]))
    return out


def eval_kernel(near_ref, far_ref, fields_ref, near_out_ref, far_out_ref):
    for source, target in ((near_ref, near_out_ref), (far_ref, far_out_ref)):
        valid = (source[:, 3, :] >= 0.0).astype(jnp.int32)
        for c in range(4):
            blocks = (jnp.sum(valid[c : c + 1, :]) + BLOCK - 1) // BLOCK

            def one_block(b, carry, c=c, source=source, target=target):
                start = pl.multiple_of(b * BLOCK, BLOCK)
                words = source[c, :, pl.ds(start, BLOCK)]
                element = words[3:4, :].astype(jnp.int32)
                hot = (iota((LANES, BLOCK), 0) == element).astype(jnp.float32).astype(jnp.bfloat16)
                hot = jnp.concatenate([hot, hot], axis=0)
                along = [basis_rows(words[d : d + 1, :]) for d in range(3)]
                row = iota((8, BLOCK), 0)
                wx = jnp.broadcast_to(along[0][0], (8, BLOCK))
                for i in range(1, 8):
                    wx = jnp.where(row == i, along[0][i], wx)
                for f in range(FIELDS):
                    picked = lax.dot(
                        fields_ref[f], hot, preferred_element_type=jnp.float32
                    )
                    over_k = picked[0:64, :] * along[2][0]
                    for k in range(1, 8):
                        over_k = over_k + picked[64 * k : 64 * k + 64, :] * along[2][k]
                    over_j = over_k[0:8, :] * along[1][0]
                    for j in range(1, 8):
                        over_j = over_j + over_k[8 * j : 8 * j + 8, :] * along[1][j]
                    target[c, f : f + 1, pl.ds(start, BLOCK)] = jnp.sum(
                        over_j * wx, axis=0, keepdims=True
                    )
                return carry

            lax.fori_loop(0, blocks, one_block, 0)


def unpack_kernel(place_ref, near_ref, far_ref, moves_ref, owner_ref, out_ref):
    q = place_ref[0]
    r = q % 4
    rs = (q + 2) % 4
    width = N_REC
    zeros = jnp.zeros((FIELDS, CAP), jnp.float32)
    values = []
    for s in range(5):
        off = s - 2
        inside = (r + off >= 0) & (r + off <= 3)
        near = near_ref[jnp.clip(r + off, 0, 3)]
        far = far_ref[jnp.clip(rs + off, 0, 3)]
        values.append(jnp.concatenate([jnp.where(inside, near, far), zeros], axis=1))
    moves = jnp.concatenate([moves_ref[...], jnp.zeros((8, CAP), jnp.int32)], axis=1)
    for b in range(10, -1, -1):
        step = 1 << b
        incoming = pltpu.roll(moves, step, 1)
        moved = (incoming >> b) & 1
        for s in range(5):
            flag = jnp.broadcast_to(moved[s : s + 1, :], (FIELDS, width))
            values[s] = jnp.where(flag == 1, pltpu.roll(values[s], step, 1), values[s])
        moves = jnp.where(moved == 1, incoming, jnp.where((moves >> b) & 1 == 1, 0, moves))
    distance = jnp.broadcast_to(owner_ref[...] - q + 2, (FIELDS, width))
    out = values[0]
    for s in range(1, 5):
        out = jnp.where(distance == s, values[s], out)
    out_ref[...] = out


def prep_kernel(
    place_ref, geometry_ref, wall_ref, forcing_ref, below_ref, above_ref,
    inverse_ref, free_ref, load_ref, plane_ref,
):
    q = place_ref[0]
    wcol = w_column()
    scol = s_column()

    def diagonal(geometry, k, j):
        wk, wj = float(WEIGHTS[k]), float(WEIGHTS[j])
        sk, sj = float(STIFF[k, k]), float(STIFF[j, j])
        return (
            geometry[0:1, :] * (scol * (wk * wj))
            + geometry[1:2, :] * (wcol * (wk * sj))
            + geometry[2:3, :] * (wcol * (sk * wj))
            + geometry[3:4, :] * (wcol * (wk * wj))
        )

    geometry = geometry_ref[...]
    below = below_ref[0:8, :]
    above = above_ref[0:8, :]
    lane = iota((8, LANES), 1)
    row = iota((8, LANES), 0)
    zero = jnp.zeros((8, LANES), jnp.float32)

    def wall_plane(low, high):
        for j in range(8):
            plane_ref[8 * j : 8 * j + 8, :] = zero
        plane_ref[0:8, :] = jnp.where(lane < 8, low, 0.0) + zero
        plane_ref[56:64, :] = jnp.where(lane >= 120, high, 0.0) + zero
        sum_xy(plane_ref, 1)
        return plane_ref[...]

    wall = wall_plane(wall_ref[0:1, :], wall_ref[1:2, :])
    wall_below = wall_plane(below[4:5, :], below[5:6, :])
    wall_above = wall_plane(above[4:5, :], above[5:6, :])
    mark = jnp.where(
        ((row == 0) & (lane % 8 == 0)) | ((row == 7) & (lane % 8 == 7)), 1.0, 0.0
    )
    for j in range(8):
        plane_ref[8 * j : 8 * j + 8, :] = mark
    sum_xy(plane_ref, 1)
    rec = plane_ref[...]
    has_below = jnp.where(q > 0, 1.0, 0.0)
    has_above = jnp.where(q < N_DOM - 1, 1.0, 0.0)
    inner = 1.0 - jnp.minimum(rec + wall, 1.0)
    bottom = 1.0 - jnp.minimum(rec + rec * has_below + (wall + wall_below), 1.0)
    top = 1.0 - jnp.minimum(rec + rec * has_above + (wall + wall_above), 1.0)
    free_ref[0:64, :] = bottom
    free_ref[448:512, :] = top
    for k in range(1, 7):
        free_ref[64 * k : 64 * k + 64, :] = inner

    for k in range(8):
        for j in range(8):
            inverse_ref[(k * 8 + j) * 8 : (k * 8 + j) * 8 + 8, :] = diagonal(geometry, k, j)
    sum_xy(inverse_ref, 8)
    for j in range(8):
        plane_ref[8 * j : 8 * j + 8, :] = diagonal(below, 7, j)
    sum_xy(plane_ref, 1)
    inverse_ref[0:64, :] = inverse_ref[0:64, :] + plane_ref[...]
    for j in range(8):
        plane_ref[8 * j : 8 * j + 8, :] = diagonal(above, 0, j)
    sum_xy(plane_ref, 1)
    inverse_ref[448:512, :] = inverse_ref[448:512, :] + plane_ref[...]
    for k in range(8):
        at = slice(64 * k, 64 * k + 64)
        inverse_ref[at, :] = free_ref[at, :] / inverse_ref[at, :]

    for k in range(8):
        for j in range(8):
            at = slice((k * 8 + j) * 8, (k * 8 + j) * 8 + 8)
            load_ref[at, :] = forcing_ref[at, :] * (
                geometry[3:4, :] * (wcol * float(WEIGHTS[k] * WEIGHTS[j]))
            )
    sum_xy(load_ref, 8)
    for other_ref, k, base in ((below_ref, 7, 0), (above_ref, 0, 448)):
        for j in range(8):
            plane_ref[8 * j : 8 * j + 8, :] = other_ref[8 + 8 * j : 16 + 8 * j, :] * (
                other_ref[3:4, :] * (wcol * float(WEIGHTS[k] * WEIGHTS[j]))
            )
        sum_xy(plane_ref, 1)
        load_ref[base : base + 64, :] = load_ref[base : base + 64, :] + plane_ref[...]


def inverse_multiplicity(q):
    row = iota((64, LANES), 0)
    lane = iota((64, LANES), 1)
    i, j = row % 8, row // 8
    x, y = lane % 8, lane // 8
    along_x = ((i == 0) & (x > 0)) | ((i == 7) & (x < 7))
    along_y = ((j == 0) & (y > 0)) | ((j == 7) & (y < 15))
    inner = jnp.where(along_x, 0.5, 1.0) * jnp.where(along_y, 0.5, 1.0)
    return (
        inner,
        inner * jnp.where(q > 0, 0.5, 1.0),
        inner * jnp.where(q < N_DOM - 1, 0.5, 1.0),
    )


def krylov_step(q, w_ref, inverse_ref, geometry_ref, xmat_ref, v_ref, u_ref, at, moments):
    inner, bottom, top = inverse_multiplicity(q)
    norm = jnp.zeros((64, LANES), jnp.float32)
    for k in range(8):
        rows = slice(64 * k, 64 * k + 64)
        w = w_ref[rows, :]
        v = inverse_ref[rows, :] * w
        v_ref[rows, :] = v
        norm = norm + v * w * (bottom if k == 0 else top if k == 7 else inner)
    energy = apply_local(
        v_ref, geometry_ref[...], xmat_ref, u_ref, tuple(range(8)), dot_with_v=True
    )
    sum_xy(u_ref, 8)
    return moments + lane_value(jnp.sum(norm), at) + lane_value(jnp.sum(energy), at + 1)


def first_kernel(
    place_ref, near_ref, far_ref, geometry_ref, below_ref, above_ref, inverse_ref, free_ref,
    load_ref, xmat_ref, w_ref, u_ref, edge_ref, moments_ref, v_ref, face_ref,
):
    q = place_ref[0]
    r = q % 4
    rs = (q + 2) % 4
    pick_row = iota((16, LANES), 0)
    pick_lane = iota((16, LANES), 1)
    picks = [
        jnp.where(pick_lane == pick_row * 8 + (0 if s == 0 else 7), 1.0, 0.0) for s in range(2)
    ]

    def planes(off):
        inside = (r + off >= 0) & (r + off <= 3)
        exists = (q + off >= 0) & (q + off < N_DOM)
        near = near_ref[jnp.clip(r + off, 0, 3)]
        far = far_ref[jnp.clip(rs + off, 0, 3)]
        values = jnp.where(exists, jnp.where(inside, near, far), 0.0)
        out = []
        for s in range(2):
            plane = lax.dot_general(
                values[16 * s : 16 * s + 16, :], picks[s], (((0,), (0,)), ((), ())),
                precision=HIGHEST, preferred_element_type=jnp.float32,
            )
            out.append([plane[8 * k : 8 * k + 8, :] for k in range(8)])
        return out

    received = {off: planes(off) for off in range(-2, 3)}
    lane = iota((8, LANES), 1)
    j_row = iota((8, LANES), 0)
    low = (j_row == 0) & (lane >= 8)
    high = (j_row == 7) & (lane < 120)

    def sum_y(value):
        down = jnp.broadcast_to(pltpu.roll(value, LANES - 8, 1)[0:1, :], (8, LANES))
        up = jnp.broadcast_to(pltpu.roll(value, 8, 1)[7:8, :], (8, LANES))
        return value + jnp.where(high, down, 0.0) + jnp.where(low, up, 0.0)

    count_y = jnp.where(low | high, 2.0, 1.0)
    on_side = [jnp.where(lane % 8 == x, 1.0, 0.0) for x in (0, 7)]

    def boundary(off):
        out = []
        has_below = jnp.where(q + off > 0, 1.0, 0.0)
        has_above = jnp.where(q + off < N_DOM - 1, 1.0, 0.0)
        for s in range(2):
            side = []
            for k in range(8):
                total = received[off][s][k]
                count = count_y * on_side[s]
                if k == 0:
                    total = total + received[off - 1][s][7]
                    count = count + count * has_below
                if k == 7:
                    total = total + received[off + 1][s][0]
                    count = count + count * has_above
                side.append(sum_y(total) / jnp.maximum(count, 1.0))
            out.append(jnp.concatenate(side, axis=0))
        return out

    zero = jnp.zeros((64, LANES), jnp.float32)
    for k in range(8):
        v_ref[64 * k : 64 * k + 64, :] = zero
    for off, geometry, plane in ((-1, below_ref[0:4, :], 7), (1, above_ref[0:4, :], 0)):
        sides = boundary(off)
        v_ref[pl.ds(0, 64, stride=8), :] = sides[0]
        v_ref[pl.ds(7, 64, stride=8), :] = sides[1]
        at = 0 if off < 0 else 64
        apply_local(v_ref, geometry, xmat_ref, face_ref.at[at : at + 64, :], (plane,))
        sum_xy(face_ref.at[at : at + 64, :], 1)
    sides = boundary(0)
    v_ref[pl.ds(0, 64, stride=8), :] = sides[0]
    v_ref[pl.ds(7, 64, stride=8), :] = sides[1]
    edge_ref[0:64, :] = sides[0]
    edge_ref[64:128, :] = sides[1]
    apply_local(v_ref, geometry_ref[...], xmat_ref, u_ref, tuple(range(8)))
    sum_xy(u_ref, 8)
    u_ref[0:64, :] = u_ref[0:64, :] + face_ref[0:64, :]
    u_ref[448:512, :] = u_ref[448:512, :] + face_ref[64:128, :]
    for k in range(8):
        rows = slice(64 * k, 64 * k + 64)
        w_ref[rows, :] = free_ref[rows, :] * (load_ref[rows, :] - u_ref[rows, :])
    moments_ref[...] = krylov_step(
        q, w_ref, inverse_ref, geometry_ref, xmat_ref, v_ref, u_ref, 0,
        jnp.zeros((1, LANES), jnp.float32),
    )


def next_kernel(
    at, last, place_ref, w_old_ref, u_old_ref, below_ref, above_ref, geometry_ref, inverse_ref,
    free_ref, xmat_ref, moments_old_ref, w_ref, u_ref, moments_ref, v_ref,
):
    q = place_ref[0]
    for k in range(8):
        rows = slice(64 * k, 64 * k + 64)
        image = u_old_ref[rows, :]
        if k == 0:
            image = image + below_ref[...]
        if k == 7:
            image = image + above_ref[...]
        w_ref[rows, :] = free_ref[rows, :] * image - w_old_ref[rows, :]
    row = krylov_step(
        q, w_ref, inverse_ref, geometry_ref, xmat_ref, v_ref, u_ref, at, moments_old_ref[...]
    )
    moments_ref[...] = jnp.broadcast_to(row, moments_ref.shape)


def last_kernel(
    w0_ref, w1_ref, w2_ref, u_ref, below_ref, above_ref, inverse_ref, free_ref, edge_ref,
    moments_ref, velocity_ref, residual_ref,
):
    sums = jnp.sum(moments_ref[...], axis=0, keepdims=True)
    h0, a0, h2, a1, h4, a2 = [sums[:, m : m + 1] for m in range(6)]
    h1, h3 = a0 - h0, a1 - h2
    g00, g01, g02, g11, g12, g22 = a0, h2 + h1, h3 + h2, a1, h4 + h3, a2
    b0, b1, b2 = h0, h1, h2
    l10 = g01 / g00
    l20 = g02 / g00
    d1 = g11 - l10 * g01
    e12 = g12 - l10 * g02
    l21 = e12 / d1
    d2 = g22 - l20 * g02 - l21 * e12
    y1 = b1 - l10 * b0
    y2 = b2 - l20 * b0 - l21 * y1
    c2 = y2 / d2
    c1 = y1 / d1 - l21 * c2
    c0 = b0 / g00 - l10 * c1 - l20 * c2
    c0, c1, c2 = [jnp.broadcast_to(c, (64, LANES)) for c in (c0, c1, c2)]
    for k in range(8):
        rows = slice(64 * k, 64 * k + 64)
        image = u_ref[rows, :]
        if k == 0:
            image = image + below_ref[...]
        if k == 7:
            image = image + above_ref[...]
        w0, w1, w2 = w0_ref[rows, :], w1_ref[rows, :], w2_ref[rows, :]
        velocity_ref[rows, :] = inverse_ref[rows, :] * (c0 * w0 + c1 * w1 + c2 * w2)
        residual_ref[rows, :] = (
            w0 - c0 * (w1 + w0) - c1 * (w2 + w1) - c2 * (free_ref[rows, :] * image)
        )
    for s in range(2):
        rows = pl.ds(7 * s, 64, stride=8)
        velocity_ref[rows, :] = velocity_ref[rows, :] + edge_ref[64 * s : 64 * s + 64, :]


VMEM = pl.BlockSpec(memory_space=pltpu.VMEM)
SMEM = pl.BlockSpec(memory_space=pltpu.SMEM)


def call(kernel, operands, outs, scratch=(), flops=100_000, smem_first=True, name=None):
    specs = [VMEM] * len(operands)
    if smem_first:
        specs[0] = SMEM
    out_shape = [jax.ShapeDtypeStruct(shape, dtype) for shape, dtype in outs]
    return pl.pallas_call(
        kernel,
        out_shape=out_shape,
        in_specs=specs,
        out_specs=[VMEM] * len(outs),
        scratch_shapes=[pltpu.VMEM(shape, dtype) for shape, dtype in scratch],
        cost_estimate=pl.CostEstimate(flops=flops, bytes_accessed=1_000_000, transcendentals=0),
        name=name,
    )(*operands)


F32 = jnp.float32
FIELD = ((512, LANES), F32)


def to_all(value):
    return lax.all_to_all(value, "dom", 0, 0, tiled=True)


def to_group(value, groups):
    return lax.all_to_all(value, "dom", 0, 0, tiled=True, axis_index_groups=groups)


def body(donor_fields, interp_weights, donor_owner, donor_element, geometry, wall_flag, forcing):
    place = lax.axis_index("dom").astype(jnp.int32).reshape(1)
    xmat = jnp.asarray(x_matrix())
    donors = lax.ppermute(donor_fields, "mesh", [(0, 1), (1, 0)])
    owner = donor_owner.reshape(1, N_REC)
    element = donor_element.reshape(1, N_REC)
    near, far, moves = call(
        route_kernel, (place, interp_weights, owner, element),
        (((4, 4, CAP), F32), ((4, 4, CAP), F32), ((8, CAP), jnp.int32)),
        scratch=(((13, 4, CAP), F32),), name="route",
    )
    near_in = to_group(near, ALIGNED)
    far_in = to_group(far, SHIFTED)

    wall = jnp.tile(wall_flag.astype(F32), (1, 16))
    head = jnp.concatenate([geometry, wall, jnp.zeros((2, LANES), F32)], 0)
    below = lax.ppermute(jnp.concatenate([head, forcing[448:512]], 0), "dom", UP)
    above = lax.ppermute(jnp.concatenate([head, forcing[0:64]], 0), "dom", DOWN)
    inverse, free, load = call(
        prep_kernel, (place, geometry, wall, forcing, below, above),
        (FIELD, FIELD, FIELD), scratch=(((64, LANES), F32),), name="prep",
    )
    (fields,) = call(
        split_kernel, (donors,), (((FIELDS, 512, 256), jnp.bfloat16),), smem_first=False,
        name="split",
    )
    near_out, far_out = call(
        eval_kernel, (near_in, far_in, fields),
        (((4, FIELDS, CAP), F32), ((4, FIELDS, CAP), F32)),
        flops=7_000_000_000, smem_first=False, name="evaluate",
    )
    near_back = to_group(near_out, ALIGNED)
    far_back = to_group(far_out, SHIFTED)
    (interface,) = call(
        unpack_kernel, (place, near_back, far_back, moves, owner), (((FIELDS, N_REC), F32),),
        name="unpack",
    )
    received = jnp.broadcast_to(interface[0].reshape(1, 32, 64), (4, 32, 64))
    near_rec = to_group(received, ALIGNED)
    far_rec = to_group(received, SHIFTED)
    w0, u, edge, moments = call(
        first_kernel,
        (place, near_rec, far_rec, geometry, below, above, inverse, free, load, xmat),
        (FIELD, FIELD, ((128, LANES), F32), ((1, LANES), F32)),
        scratch=(FIELD, ((128, LANES), F32)), name="first",
    )

    def halo(u):
        return lax.ppermute(u[448:512], "dom", UP), lax.ppermute(u[0:64], "dom", DOWN)

    ws = [w0]
    for step in (1, 2):
        from_below, from_above = halo(u)
        w, u, moments = call(
            functools.partial(next_kernel, 2 * step, step == 2),
            (place, ws[-1], u, from_below, from_above, geometry, inverse, free, xmat, moments),
            (FIELD, FIELD, ((1 if step == 1 else N_DOM, LANES), F32)),
            scratch=(FIELD,), name=f"next{step}",
        )
        ws.append(w)
    from_below, from_above = halo(u)
    sums = to_all(moments)
    velocity, residual = call(
        last_kernel,
        (*ws, u, from_below, from_above, inverse, free, edge, sums),
        (FIELD, FIELD), smem_first=False, name="last",
    )
    return velocity, residual, interface


def solution(mesh):
    both = ("mesh", "dom")
    in_specs = (
        P(None, None, both), P(None, None, both), P(both, None), P(both), P(None, both),
        P(None, both), P(None, both),
    )
    out_specs = (P(None, both), P(None, both), P(None, both))
    return jax.shard_map(body, mesh=mesh, in_specs=in_specs, out_specs=out_specs, check_vma=False)
```

```python
import functools

import jax
import jax.numpy as jnp
import numpy as np
from jax import lax
from jax.experimental import pallas as pl
from jax.experimental.pallas import tpu as pltpu
from jax.sharding import PartitionSpec as P

HIGHEST = lax.Precision.HIGHEST
N_DOM = 64
N_REC = 2048
CAP = 1024
FIELDS = 5
LANES = 128
BLOCK = 512
CHUNK = 104


def both_ways(lows, distance):
    return [pair for q in lows for pair in ((q, q + distance), (q + distance, q))]


CROSS_1 = both_ways(range(1, N_DOM - 1, 2), 1)
INNER_1 = both_ways(range(0, N_DOM - 1, 2), 1)
CROSS_2 = both_ways([q for q in range(N_DOM - 2) if q % 4 >= 2], 2)
INNER_2 = both_ways([q for q in range(N_DOM - 2) if q % 4 < 2], 2)


def from_above(q):
    odd = q % 2 == 1
    late = q % 4 >= 2
    return odd, jnp.logical_not(odd), late, jnp.logical_not(late)


def legendre_pair(values, degree):
    previous = values * 0.0 + 1.0
    current = values * 1.0
    for order in range(2, degree + 1):
        previous, current = (
            current,
            ((2 * order - 1) * values * current - (order - 1) * previous) / order,
        )
    return current, previous


def gll_tables():
    degree = 7
    count = degree + 1
    nodes = np.cos(np.pi * np.arange(count) / degree)
    for _ in range(80):
        top, lower = legendre_pair(nodes, degree)
        nodes = nodes - (nodes * top - lower) / (count * top)
    nodes = np.sort(nodes)
    top, lower = legendre_pair(nodes, degree)
    weights = 2.0 / (degree * count * top * top)
    identity = np.eye(count)
    spacing = nodes[:, None] - nodes[None, :] + identity
    derivative = top[:, None] / (top[None, :] * spacing) * (1.0 - identity)
    derivative[0, 0] = -degree * count / 4.0
    derivative[degree, degree] = degree * count / 4.0
    return nodes, weights, derivative


NODES, WEIGHTS, DERIV = gll_tables()
STIFF = DERIV.T @ (WEIGHTS[:, None] * DERIV)
STIFF = 0.5 * (STIFF + STIFF.T)
BARY = np.array([1.0 / np.prod([NODES[i] - NODES[j] for j in range(8) if j != i]) for i in range(8)])


def x_matrix():
    out = np.zeros((512, 256))
    for k in range(8):
        for j in range(8):
            row = (k * 8 + j) * 8
            col = row % 256
            out[row : row + 8, col : col + 8] = WEIGHTS[k] * WEIGHTS[j] * STIFF
    return out.astype(np.float32)


def iota(shape, dim):
    return lax.broadcasted_iota(jnp.int32, shape, dim)


def w_column():
    row = iota((8, LANES), 0)
    out = jnp.full((8, LANES), float(WEIGHTS[0]), jnp.float32)
    for i in range(1, 8):
        out = jnp.where(row == i, float(WEIGHTS[i]), out)
    return out


def s_column():
    row = iota((8, LANES), 0)
    out = jnp.full((8, LANES), float(STIFF[0, 0]), jnp.float32)
    for i in range(1, 8):
        out = jnp.where(row == i, float(STIFF[i, i]), out)
    return out


def sum_xy(ref, planes):
    rows = planes * 8
    lane = iota((rows, LANES), 1)
    low = ref[pl.ds(0, rows, stride=8), :]
    high = ref[pl.ds(7, rows, stride=8), :]
    ref[pl.ds(7, rows, stride=8), :] = high + jnp.where(
        lane % 8 < 7, pltpu.roll(low, LANES - 1, 1), 0.0
    )
    ref[pl.ds(0, rows, stride=8), :] = low + jnp.where(lane % 8 > 0, pltpu.roll(high, 1, 1), 0.0)
    lane = iota((8, LANES), 1)
    for k in range(planes):
        low = ref[k * 64 : k * 64 + 8, :]
        high = ref[k * 64 + 56 : k * 64 + 64, :]
        ref[k * 64 + 56 : k * 64 + 64, :] = high + jnp.where(
            lane < 120, pltpu.roll(low, LANES - 8, 1), 0.0
        )
        ref[k * 64 : k * 64 + 8, :] = low + jnp.where(lane >= 8, pltpu.roll(high, 8, 1), 0.0)


def apply_local(v_ref, geometry, xmat_ref, out_ref, planes, dot_with_v=False):
    wcol = w_column()
    gx = geometry[0:1, :]
    gyw = geometry[1:2, :] * wcol
    gzw = geometry[2:3, :] * wcol
    gmw = geometry[3:4, :] * wcol
    total = jnp.zeros((8, LANES), jnp.float32)
    if len(planes) == 8:
        along_x = [
            lax.dot(
                xmat_ref[256 * h : 256 * h + 256, :],
                v_ref[256 * h : 256 * h + 256, :],
                precision=HIGHEST,
                preferred_element_type=jnp.float32,
            )
            for h in range(2)
        ]
        for h in range(2):
            out_ref[256 * h : 256 * h + 256, :] = along_x[h]
    else:
        for at, k in enumerate(planes):
            h = k // 4
            out_ref[at * 64 : at * 64 + 64, :] = lax.dot(
                xmat_ref[k * 64 : k * 64 + 64, :],
                v_ref[256 * h : 256 * h + 256, :],
                precision=HIGHEST,
                preferred_element_type=jnp.float32,
            )
    for at, k in enumerate(planes):
        plane = [v_ref[(k * 8 + j) * 8 : (k * 8 + j) * 8 + 8, :] for j in range(8)]
        for j in range(8):
            ysum = plane[0] * float(STIFF[j, 0] * WEIGHTS[k])
            for jj in range(1, 8):
                ysum = ysum + plane[jj] * float(STIFF[j, jj] * WEIGHTS[k])
            zsum = None
            for kk in range(8):
                term = v_ref[(kk * 8 + j) * 8 : (kk * 8 + j) * 8 + 8, :] * float(
                    STIFF[k, kk] * WEIGHTS[j]
                )
                zsum = term if zsum is None else zsum + term
            row = (at * 8 + j) * 8
            value = (
                out_ref[row : row + 8, :] * gx
                + gyw * ysum
                + gzw * zsum
                + gmw * (plane[j] * float(WEIGHTS[k] * WEIGHTS[j]))
            )
            out_ref[row : row + 8, :] = value
            if dot_with_v:
                total = total + value * plane[j]
    return total


def lane_value(value, at):
    return jnp.where(iota((1, LANES), 1) == at, value, 0.0)


def by_side(q, cross_1, inner_1, cross_2=None, inner_2=None):
    above = from_above(q)
    out = (jnp.where(above[0], inner_1, cross_1), jnp.where(above[0], cross_1, inner_1))
    if cross_2 is not None:
        out += (jnp.where(above[2], inner_2, cross_2), jnp.where(above[2], cross_2, inner_2))
    return out


def route_kernel(
    place_ref, weights_ref, owner_ref, element_ref, geometry_ref, wall_ref, forcing_ref,
    cross_1_ref, inner_1_ref, cross_2_ref, inner_2_ref, own_ref, moves_ref, slots_ref,
):
    q = place_ref[0]
    width = N_REC
    lane = iota((8, width), 1)
    row = iota((8, width), 0)
    distance = owner_ref[...] - q + 2
    mine = distance == row
    count = mine.astype(jnp.int32)
    step = 1
    while step < width:
        count = count + jnp.where(lane >= step, pltpu.roll(count, step, 1), 0)
        step *= 2
    moves = jnp.where(mine, lane - (count - 1), 0)
    totals = count[:, width - 1 : width]
    node_rows = iota((8, width), 0)
    node = jnp.full((8, width), float(NODES[0]), jnp.float32)
    for i in range(1, 8):
        node = jnp.where(node_rows == i, float(NODES[i]), node)
    coords = [jnp.sum(weights_ref[d] * node, axis=0, keepdims=True) for d in range(3)]
    words = element_ref[...].astype(jnp.float32) + 1.0
    base = jnp.where(row % 4 == 3, words, 0.0)
    for d in range(3):
        base = jnp.where(row % 4 == d, coords[d], base)
    packs = [base, base, base]
    for b in range(11):
        step = 1 << b
        incoming = pltpu.roll(moves, width - step, 1)
        moved = (incoming >> b) & 1
        for n in range(3):
            first = jnp.broadcast_to(moved[2 * n : 2 * n + 1, :], (8, width))
            if n < 2:
                second = jnp.broadcast_to(moved[2 * n + 1 : 2 * n + 2, :], (8, width))
                first = jnp.where(row < 4, first, second)
            packs[n] = jnp.where(first == 1, pltpu.roll(packs[n], width - step, 1), packs[n])
        moves = jnp.where(moved == 1, incoming, jnp.where((moves >> b) & 1 == 1, 0, moves))
    moves_ref[...] = moves[:, :CAP]
    lane = iota((4, CAP), 1)
    for s in range(5):
        at = (s % 2) * 4
        slot = jnp.where(lane < totals[s : s + 1, :], packs[s // 2][at : at + 4, :CAP], 0.0)
        for c in range(8):
            slots_ref[s, 4 * c : 4 * c + 4, :] = slot[:, c * LANES : (c + 1) * LANES]
    above = from_above(q)
    bottom, top = forcing_ref[0:64, :], forcing_ref[448:512, :]
    spread = jnp.where(iota((8, LANES), 1) % 8 == iota((8, LANES), 0), 1.0, 0.0)
    wall = lax.dot(
        wall_ref[...].astype(jnp.float32), spread, preferred_element_type=jnp.float32
    )
    for target_ref, up in ((cross_1_ref, above[0]), (inner_1_ref, above[1])):
        target_ref[0:32, :] = jnp.where(up, slots_ref[3], slots_ref[1])
        target_ref[32:36, :] = geometry_ref[...]
        target_ref[36:38, :] = wall
        target_ref[38:40, :] = jnp.zeros((2, LANES), jnp.float32)
        target_ref[40:104, :] = jnp.where(up, top, bottom)
    for target_ref, up in ((cross_2_ref, above[2]), (inner_2_ref, above[3])):
        target_ref[...] = jnp.where(up, slots_ref[4], slots_ref[0])
    own_ref[...] = slots_ref[2]


def split_kernel(fields_ref, out_ref):
    for f in range(FIELDS):
        value = fields_ref[f]
        high = value.astype(jnp.bfloat16)
        out_ref[f, :, 0:LANES] = high
        out_ref[f, :, LANES : 2 * LANES] = (value - high.astype(jnp.float32)).astype(jnp.bfloat16)


def basis_rows(coordinate):
    gaps = [coordinate - float(NODES[i]) for i in range(8)]
    before = [None] * 8
    after = [None] * 8
    for i in range(1, 8):
        before[i] = gaps[i - 1] if i == 1 else before[i - 1] * gaps[i - 1]
    for i in range(6, -1, -1):
        after[i] = gaps[i + 1] if i == 6 else after[i + 1] * gaps[i + 1]
    out = []
    for i in range(8):
        if i == 0:
            value = after[0]
        elif i == 7:
            value = before[7]
        else:
            value = before[i] * after[i]
        out.append(value * float(BARY[i]))
    return out


def eval_kernel(*refs):
    sources, fields_ref, targets = refs[0:5], refs[5], refs[6:11]
    for source, target in zip(sources, targets):
        words = source[0:32, :]
        valid = jnp.where((iota((32, LANES), 0) % 4 == 3) & (words > 0.0), 1, 0)
        blocks = (jnp.sum(valid) + BLOCK - 1) // BLOCK

        def one_block(b, carry, source=source, target=target):
            start = pl.multiple_of(b * BLOCK, BLOCK)
            tiles = source[pl.ds(pl.multiple_of(b * 16, 16), 16), :]
            words = jnp.concatenate([tiles[4 * n : 4 * n + 4, :] for n in range(4)], axis=1)
            element = words[3:4, :].astype(jnp.int32) - 1
            hot = (iota((LANES, BLOCK), 0) == element).astype(jnp.float32).astype(jnp.bfloat16)
            hot = jnp.concatenate([hot, hot], axis=0)
            along = [basis_rows(words[d : d + 1, :]) for d in range(3)]
            row = iota((8, BLOCK), 0)
            wx = jnp.broadcast_to(along[0][0], (8, BLOCK))
            for i in range(1, 8):
                wx = jnp.where(row == i, along[0][i], wx)
            for f in range(FIELDS):
                picked = lax.dot(
                    fields_ref[f], hot, preferred_element_type=jnp.float32
                )
                over_k = picked[0:64, :] * along[2][0]
                for k in range(1, 8):
                    over_k = over_k + picked[64 * k : 64 * k + 64, :] * along[2][k]
                over_j = over_k[0:8, :] * along[1][0]
                for j in range(1, 8):
                    over_j = over_j + over_k[8 * j : 8 * j + 8, :] * along[1][j]
                target[f : f + 1, pl.ds(start, BLOCK)] = jnp.sum(
                    over_j * wx, axis=0, keepdims=True
                )
            return carry

        lax.fori_loop(0, blocks, one_block, 0)


def unpack_kernel(
    place_ref, cross_1_ref, inner_1_ref, cross_2_ref, inner_2_ref, own_ref, moves_ref, owner_ref,
    out_ref, share_ref,
):
    q = place_ref[0]
    width = N_REC
    below_1, above_1, below_2, above_2 = by_side(
        q, cross_1_ref[...], inner_1_ref[...], cross_2_ref[...], inner_2_ref[...]
    )
    zeros = jnp.zeros((FIELDS, CAP), jnp.float32)
    values = [
        jnp.concatenate([value, zeros], axis=1)
        for value in (below_2, below_1, own_ref[...], above_1, above_2)
    ]
    moves = jnp.concatenate([moves_ref[...], jnp.zeros((8, CAP), jnp.int32)], axis=1)
    for b in range(10, -1, -1):
        step = 1 << b
        incoming = pltpu.roll(moves, step, 1)
        moved = (incoming >> b) & 1
        for s in range(5):
            flag = jnp.broadcast_to(moved[s : s + 1, :], (FIELDS, width))
            values[s] = jnp.where(flag == 1, pltpu.roll(values[s], step, 1), values[s])
        moves = jnp.where(moved == 1, incoming, jnp.where((moves >> b) & 1 == 1, 0, moves))
    distance = jnp.broadcast_to(owner_ref[...] - q + 2, (FIELDS, width))
    out = values[0]
    for s in range(1, 5):
        out = jnp.where(distance == s, values[s], out)
    out_ref[...] = out
    for n in range(16):
        share_ref[n : n + 1, :] = out[0:1, n * LANES : (n + 1) * LANES]


def prep_kernel(
    place_ref, geometry_ref, wall_ref, forcing_ref, cross_ref, inner_ref,
    inverse_ref, free_ref, load_ref, beside_ref, plane_ref, below_ref, above_ref,
):
    q = place_ref[0]
    below_ref[...], above_ref[...] = by_side(q, cross_ref[32:104, :], inner_ref[32:104, :])
    beside_ref[0:8, :] = below_ref[0:8, :]
    beside_ref[8:16, :] = above_ref[0:8, :]
    wcol = w_column()
    scol = s_column()

    def diagonal(geometry, k, j):
        wk, wj = float(WEIGHTS[k]), float(WEIGHTS[j])
        sk, sj = float(STIFF[k, k]), float(STIFF[j, j])
        return (
            geometry[0:1, :] * (scol * (wk * wj))
            + geometry[1:2, :] * (wcol * (wk * sj))
            + geometry[2:3, :] * (wcol * (sk * wj))
            + geometry[3:4, :] * (wcol * (wk * wj))
        )

    geometry = geometry_ref[...]
    below = below_ref[0:8, :]
    above = above_ref[0:8, :]
    lane = iota((8, LANES), 1)
    row = iota((8, LANES), 0)
    zero = jnp.zeros((8, LANES), jnp.float32)

    def wall_plane(low, high):
        for j in range(8):
            plane_ref[8 * j : 8 * j + 8, :] = zero
        plane_ref[0:8, :] = jnp.where(lane < 8, low, 0.0) + zero
        plane_ref[56:64, :] = jnp.where(lane >= 120, high, 0.0) + zero
        sum_xy(plane_ref, 1)
        return plane_ref[...]

    spread = jnp.where(lane % 8 == row, 1.0, 0.0)
    flags = lax.dot(
        wall_ref[...].astype(jnp.float32), spread, preferred_element_type=jnp.float32
    )
    wall = wall_plane(flags[0:1, :], flags[1:2, :])
    wall_below = wall_plane(below[4:5, :], below[5:6, :])
    wall_above = wall_plane(above[4:5, :], above[5:6, :])
    mark = jnp.where(
        ((row == 0) & (lane % 8 == 0)) | ((row == 7) & (lane % 8 == 7)), 1.0, 0.0
    )
    for j in range(8):
        plane_ref[8 * j : 8 * j + 8, :] = mark
    sum_xy(plane_ref, 1)
    rec = plane_ref[...]
    has_below = jnp.where(q > 0, 1.0, 0.0)
    has_above = jnp.where(q < N_DOM - 1, 1.0, 0.0)
    inner = 1.0 - jnp.minimum(rec + wall, 1.0)
    bottom = 1.0 - jnp.minimum(rec + rec * has_below + (wall + wall_below), 1.0)
    top = 1.0 - jnp.minimum(rec + rec * has_above + (wall + wall_above), 1.0)
    free_ref[0:64, :] = bottom
    free_ref[448:512, :] = top
    for k in range(1, 7):
        free_ref[64 * k : 64 * k + 64, :] = inner

    for k in range(8):
        for j in range(8):
            inverse_ref[(k * 8 + j) * 8 : (k * 8 + j) * 8 + 8, :] = diagonal(geometry, k, j)
    sum_xy(inverse_ref, 8)
    for j in range(8):
        plane_ref[8 * j : 8 * j + 8, :] = diagonal(below, 7, j)
    sum_xy(plane_ref, 1)
    inverse_ref[0:64, :] = inverse_ref[0:64, :] + plane_ref[...]
    for j in range(8):
        plane_ref[8 * j : 8 * j + 8, :] = diagonal(above, 0, j)
    sum_xy(plane_ref, 1)
    inverse_ref[448:512, :] = inverse_ref[448:512, :] + plane_ref[...]
    for k in range(8):
        at = slice(64 * k, 64 * k + 64)
        inverse_ref[at, :] = free_ref[at, :] / inverse_ref[at, :]

    for k in range(8):
        for j in range(8):
            at = slice((k * 8 + j) * 8, (k * 8 + j) * 8 + 8)
            load_ref[at, :] = forcing_ref[at, :] * (
                geometry[3:4, :] * (wcol * float(WEIGHTS[k] * WEIGHTS[j]))
            )
    sum_xy(load_ref, 8)
    for other_ref, k, base in ((below_ref, 7, 0), (above_ref, 0, 448)):
        for j in range(8):
            plane_ref[8 * j : 8 * j + 8, :] = other_ref[8 + 8 * j : 16 + 8 * j, :] * (
                other_ref[3:4, :] * (wcol * float(WEIGHTS[k] * WEIGHTS[j]))
            )
        sum_xy(plane_ref, 1)
        load_ref[base : base + 64, :] = load_ref[base : base + 64, :] + plane_ref[...]


def inverse_multiplicity(q):
    row = iota((64, LANES), 0)
    lane = iota((64, LANES), 1)
    i, j = row % 8, row // 8
    x, y = lane % 8, lane // 8
    along_x = ((i == 0) & (x > 0)) | ((i == 7) & (x < 7))
    along_y = ((j == 0) & (y > 0)) | ((j == 7) & (y < 15))
    inner = jnp.where(along_x, 0.5, 1.0) * jnp.where(along_y, 0.5, 1.0)
    return (
        inner,
        inner * jnp.where(q > 0, 0.5, 1.0),
        inner * jnp.where(q < N_DOM - 1, 0.5, 1.0),
    )


def krylov_step(q, w_ref, inverse_ref, geometry_ref, xmat_ref, v_ref, u_ref, at, moments):
    inner, bottom, top = inverse_multiplicity(q)
    norm = jnp.zeros((64, LANES), jnp.float32)
    for k in range(8):
        rows = slice(64 * k, 64 * k + 64)
        w = w_ref[rows, :]
        v = inverse_ref[rows, :] * w
        v_ref[rows, :] = v
        norm = norm + v * w * (bottom if k == 0 else top if k == 7 else inner)
    energy = apply_local(
        v_ref, geometry_ref[...], xmat_ref, u_ref, tuple(range(8)), dot_with_v=True
    )
    sum_xy(u_ref, 8)
    return moments + lane_value(jnp.sum(norm), at) + lane_value(jnp.sum(energy), at + 1)


def first_kernel(
    place_ref, own_ref, cross_1_ref, inner_1_ref, cross_2_ref, inner_2_ref, geometry_ref,
    beside_ref, inverse_ref, free_ref, load_ref, xmat_ref, w_ref, u_ref, edge_ref, moments_ref, cross_ref, inner_ref, v_ref, face_ref,
):
    q = place_ref[0]
    below_1, above_1, below_2, above_2 = by_side(
        q, cross_1_ref[...], inner_1_ref[...], cross_2_ref[...], inner_2_ref[...]
    )
    pick_row = iota((8, LANES), 0)
    pick_lane = iota((8, LANES), 1)
    picks = [
        [
            jnp.where(pick_lane == pick_row * 16 + (8 * odd + 7 * s), 1.0, 0.0)
            for odd in range(2)
        ]
        for s in range(2)
    ]

    def planes(values):
        out = []
        for s in range(2):
            halves = [
                lax.dot_general(
                    values[8 * s : 8 * s + 8, :], picks[s][odd], (((0,), (0,)), ((), ())),
                    precision=HIGHEST, preferred_element_type=jnp.float32,
                )
                for odd in range(2)
            ]
            plane = halves[0][0:64, :] + halves[1][64:128, :]
            out.append([plane[8 * k : 8 * k + 8, :] for k in range(8)])
        return out

    layers = (below_2, below_1, own_ref[...], above_1, above_2)
    received = {off: planes(values) for off, values in zip(range(-2, 3), layers)}
    lane = iota((8, LANES), 1)
    j_row = iota((8, LANES), 0)
    low = (j_row == 0) & (lane >= 8)
    high = (j_row == 7) & (lane < 120)

    def sum_y(value):
        down = jnp.broadcast_to(pltpu.roll(value, LANES - 8, 1)[0:1, :], (8, LANES))
        up = jnp.broadcast_to(pltpu.roll(value, 8, 1)[7:8, :], (8, LANES))
        return value + jnp.where(high, down, 0.0) + jnp.where(low, up, 0.0)

    count_y = jnp.where(low | high, 2.0, 1.0)
    on_side = [jnp.where(lane % 8 == x, 1.0, 0.0) for x in (0, 7)]

    def boundary(off):
        out = []
        has_below = jnp.where(q + off > 0, 1.0, 0.0)
        has_above = jnp.where(q + off < N_DOM - 1, 1.0, 0.0)
        for s in range(2):
            side = []
            for k in range(8):
                total = received[off][s][k]
                count = count_y * on_side[s]
                if k == 0:
                    total = total + received[off - 1][s][7]
                    count = count + count * has_below
                if k == 7:
                    total = total + received[off + 1][s][0]
                    count = count + count * has_above
                side.append(sum_y(total) / jnp.maximum(count, 1.0))
            out.append(jnp.concatenate(side, axis=0))
        return out

    zero = jnp.zeros((64, LANES), jnp.float32)
    for k in range(8):
        v_ref[64 * k : 64 * k + 64, :] = zero
    for off, geometry, plane in ((-1, beside_ref[0:4, :], 7), (1, beside_ref[8:12, :], 0)):
        sides = boundary(off)
        v_ref[pl.ds(0, 64, stride=8), :] = sides[0]
        v_ref[pl.ds(7, 64, stride=8), :] = sides[1]
        at = 0 if off < 0 else 64
        apply_local(v_ref, geometry, xmat_ref, face_ref.at[at : at + 64, :], (plane,))
        sum_xy(face_ref.at[at : at + 64, :], 1)
    sides = boundary(0)
    v_ref[pl.ds(0, 64, stride=8), :] = sides[0]
    v_ref[pl.ds(7, 64, stride=8), :] = sides[1]
    edge_ref[0:64, :] = sides[0]
    edge_ref[64:128, :] = sides[1]
    apply_local(v_ref, geometry_ref[...], xmat_ref, u_ref, tuple(range(8)))
    sum_xy(u_ref, 8)
    u_ref[0:64, :] = u_ref[0:64, :] + face_ref[0:64, :]
    u_ref[448:512, :] = u_ref[448:512, :] + face_ref[64:128, :]
    for k in range(8):
        rows = slice(64 * k, 64 * k + 64)
        w_ref[rows, :] = free_ref[rows, :] * (load_ref[rows, :] - u_ref[rows, :])
    moments_ref[...] = krylov_step(
        q, w_ref, inverse_ref, geometry_ref, xmat_ref, v_ref, u_ref, 0,
        jnp.zeros((1, LANES), jnp.float32),
    )
    send_faces(q, u_ref, cross_ref, inner_ref)


def send_faces(q, u_ref, cross_ref, inner_ref):
    up = from_above(q)[0]
    bottom, top = u_ref[0:64, :], u_ref[448:512, :]
    cross_ref[...] = jnp.where(up, top, bottom)
    inner_ref[...] = jnp.where(up, bottom, top)


def next_kernel(
    at, place_ref, w_old_ref, u_old_ref, cross_in_ref, inner_in_ref, geometry_ref, inverse_ref,
    free_ref, xmat_ref, moments_old_ref, w_ref, u_ref, moments_ref, cross_ref, inner_ref, v_ref,
):
    q = place_ref[0]
    below, above = by_side(q, cross_in_ref[...], inner_in_ref[...])
    for k in range(8):
        rows = slice(64 * k, 64 * k + 64)
        image = u_old_ref[rows, :]
        if k == 0:
            image = image + below
        if k == 7:
            image = image + above
        w_ref[rows, :] = free_ref[rows, :] * image - w_old_ref[rows, :]
    row = krylov_step(
        q, w_ref, inverse_ref, geometry_ref, xmat_ref, v_ref, u_ref, at, moments_old_ref[...]
    )
    moments_ref[...] = jnp.broadcast_to(row, moments_ref.shape)
    send_faces(q, u_ref, cross_ref, inner_ref)


def last_kernel(
    place_ref, w0_ref, w1_ref, w2_ref, u_ref, cross_in_ref, inner_in_ref, inverse_ref, free_ref,
    edge_ref, moments_ref, velocity_ref, residual_ref,
):
    below, above = by_side(place_ref[0], cross_in_ref[...], inner_in_ref[...])
    sums = jnp.sum(moments_ref[...], axis=0, keepdims=True)
    h0, a0, h2, a1, h4, a2 = [sums[:, m : m + 1] for m in range(6)]
    h1, h3 = a0 - h0, a1 - h2
    g00, g01, g02, g11, g12, g22 = a0, h2 + h1, h3 + h2, a1, h4 + h3, a2
    b0, b1, b2 = h0, h1, h2
    l10 = g01 / g00
    l20 = g02 / g00
    d1 = g11 - l10 * g01
    e12 = g12 - l10 * g02
    l21 = e12 / d1
    d2 = g22 - l20 * g02 - l21 * e12
    y1 = b1 - l10 * b0
    y2 = b2 - l20 * b0 - l21 * y1
    c2 = y2 / d2
    c1 = y1 / d1 - l21 * c2
    c0 = b0 / g00 - l10 * c1 - l20 * c2
    c0, c1, c2 = [jnp.broadcast_to(c, (64, LANES)) for c in (c0, c1, c2)]
    for k in range(8):
        rows = slice(64 * k, 64 * k + 64)
        image = u_ref[rows, :]
        if k == 0:
            image = image + below
        if k == 7:
            image = image + above
        w0, w1, w2 = w0_ref[rows, :], w1_ref[rows, :], w2_ref[rows, :]
        velocity_ref[rows, :] = inverse_ref[rows, :] * (c0 * w0 + c1 * w1 + c2 * w2)
        residual_ref[rows, :] = (
            w0 - c0 * (w1 + w0) - c1 * (w2 + w1) - c2 * (free_ref[rows, :] * image)
        )
    for s in range(2):
        rows = pl.ds(7 * s, 64, stride=8)
        velocity_ref[rows, :] = velocity_ref[rows, :] + edge_ref[64 * s : 64 * s + 64, :]


VMEM = pl.BlockSpec(memory_space=pltpu.VMEM)
SMEM = pl.BlockSpec(memory_space=pltpu.SMEM)


def call(kernel, operands, outs, scratch=(), flops=100_000, smem_first=True, name=None, mib=12):
    specs = [VMEM] * len(operands)
    if smem_first:
        specs[0] = SMEM
    out_shape = [jax.ShapeDtypeStruct(shape, dtype) for shape, dtype in outs]
    return pl.pallas_call(
        kernel,
        out_shape=out_shape,
        in_specs=specs,
        out_specs=[VMEM] * len(outs),
        scratch_shapes=[pltpu.VMEM(shape, dtype) for shape, dtype in scratch],
        cost_estimate=pl.CostEstimate(flops=flops, bytes_accessed=1_000_000, transcendentals=0),
        compiler_params=pltpu.CompilerParams(vmem_limit_bytes=mib * 1024 * 1024),
        name=name,
    )(*operands)


F32 = jnp.float32
FIELD = ((512, LANES), F32)


def to_all(value):
    return lax.all_to_all(value, "dom", 0, 0, tiled=True)


def to_neighbours(cross_1, inner_1, cross_2=None, inner_2=None):
    lists = ((cross_1, CROSS_1), (cross_2, CROSS_2), (inner_1, INNER_1), (inner_2, INNER_2))
    moved = [None if value is None else lax.ppermute(value, "dom", pairs) for value, pairs in lists]
    return [moved[n] for n in (0, 2, 1, 3) if moved[n] is not None]


def body(donor_fields, interp_weights, donor_owner, donor_element, geometry, wall_flag, forcing):
    place = lax.axis_index("dom").astype(jnp.int32).reshape(1)
    xmat = jnp.asarray(x_matrix())
    donors = lax.ppermute(donor_fields, "mesh", [(0, 1), (1, 0)])
    owner = donor_owner.reshape(1, N_REC)
    element = donor_element.reshape(1, N_REC)
    asked = ((32, LANES), F32)
    with_head = ((CHUNK, LANES), F32)
    *requests, own, moves = call(
        route_kernel, (place, interp_weights, owner, element, geometry, wall_flag, forcing),
        (with_head, with_head, asked, asked, asked, ((8, CAP), jnp.int32)),
        scratch=(((5, 32, LANES), F32),), name="route", mib=60,
    )
    requests = to_neighbours(*requests)
    (fields,) = call(
        split_kernel, (donors,), (((FIELDS, 512, 256), jnp.bfloat16),), smem_first=False,
        name="split",
    )
    answers = call(
        eval_kernel, (*requests, own, fields), (((FIELDS, CAP), F32),) * 5,
        flops=7_000_000_000, smem_first=False, name="evaluate", mib=24,
    )
    answered = to_neighbours(*answers[0:4])
    inverse, free, load, beside = call(
        prep_kernel, (place, geometry, wall_flag, forcing, requests[0], requests[1]),
        (FIELD, FIELD, FIELD, ((16, LANES), F32)),
        scratch=(((64, LANES), F32), ((72, LANES), F32), ((72, LANES), F32)), name="prep",
    )
    interface, share = call(
        unpack_kernel, (place, *answered, answers[4], moves, owner),
        (((FIELDS, N_REC), F32), ((16, LANES), F32)), name="unpack",
    )
    face = ((64, LANES), F32)
    w0, u, edge, moments, *faces = call(
        first_kernel,
        (place, share, *to_neighbours(share, share, share, share), geometry, beside, inverse, free,
         load, xmat),
        (FIELD, FIELD, ((128, LANES), F32), ((1, LANES), F32), face, face),
        scratch=(FIELD, ((128, LANES), F32)), name="first",
    )
    ws = [w0]
    for step in (1, 2):
        w, u, moments, *faces = call(
            functools.partial(next_kernel, 2 * step),
            (place, ws[-1], u, *to_neighbours(*faces), geometry, inverse, free, xmat, moments),
            (FIELD, FIELD, ((1 if step == 1 else N_DOM, LANES), F32), face, face),
            scratch=(FIELD,), name=f"next{step}",
        )
        ws.append(w)
    faces = to_neighbours(*faces)
    sums = to_all(moments)
    velocity, residual = call(
        last_kernel, (place, *ws, u, *faces, inverse, free, edge, sums),
        (FIELD, FIELD), name="last",
    )
    return velocity, residual, interface


def solution(mesh):
    both = ("mesh", "dom")
    in_specs = (
        P(None, None, both), P(None, None, both), P(both, None), P(both), P(None, both),
        P(None, both), P(None, both),
    )
    out_specs = (P(None, both), P(None, both), P(None, both))
    return jax.shard_map(body, mesh=mesh, in_specs=in_specs, out_specs=out_specs, check_vma=False)
```

```python
import functools

import jax
import jax.numpy as jnp
import numpy as np
from jax import lax
from jax.experimental import pallas as pl
from jax.experimental.pallas import tpu as pltpu
from jax.sharding import PartitionSpec as P


HIGHEST = lax.Precision.HIGHEST
N_DOM = 64
N_REC = 2048
CAP = 1024
FIELDS = 5
LANES = 128
BLOCK = 512
CHUNK = 104


def both_ways(lows, distance):
    return [pair for q in lows for pair in ((q, q + distance), (q + distance, q))]


CROSS_1 = both_ways(range(1, N_DOM - 1, 2), 1)
INNER_1 = both_ways(range(0, N_DOM - 1, 2), 1)
CROSS_2 = both_ways([q for q in range(N_DOM - 2) if q % 4 >= 2], 2)
INNER_2 = both_ways([q for q in range(N_DOM - 2) if q % 4 < 2], 2)


def from_above(q):
    odd = q % 2 == 1
    late = q % 4 >= 2
    return odd, jnp.logical_not(odd), late, jnp.logical_not(late)


def legendre_pair(values, degree):
    previous = values * 0.0 + 1.0
    current = values * 1.0
    for order in range(2, degree + 1):
        previous, current = (
            current,
            ((2 * order - 1) * values * current - (order - 1) * previous) / order,
        )
    return current, previous


def gll_tables():
    degree = 7
    count = degree + 1
    nodes = np.cos(np.pi * np.arange(count) / degree)
    for _ in range(80):
        top, lower = legendre_pair(nodes, degree)
        nodes = nodes - (nodes * top - lower) / (count * top)
    nodes = np.sort(nodes)
    top, lower = legendre_pair(nodes, degree)
    weights = 2.0 / (degree * count * top * top)
    identity = np.eye(count)
    spacing = nodes[:, None] - nodes[None, :] + identity
    derivative = top[:, None] / (top[None, :] * spacing) * (1.0 - identity)
    derivative[0, 0] = -degree * count / 4.0
    derivative[degree, degree] = degree * count / 4.0
    return nodes, weights, derivative


NODES, WEIGHTS, DERIV = gll_tables()
STIFF = DERIV.T @ (WEIGHTS[:, None] * DERIV)
STIFF = 0.5 * (STIFF + STIFF.T)
BARY = np.array([1.0 / np.prod([NODES[i] - NODES[j] for j in range(8) if j != i]) for i in range(8)])


def x_matrix():
    out = np.zeros((512, 256))
    for k in range(8):
        for j in range(8):
            row = (k * 8 + j) * 8
            col = row % 256
            out[row : row + 8, col : col + 8] = WEIGHTS[k] * WEIGHTS[j] * STIFF
    return out.astype(np.float32)


def iota(shape, dim):
    return lax.broadcasted_iota(jnp.int32, shape, dim)


def w_column():
    row = iota((8, LANES), 0)
    out = jnp.full((8, LANES), float(WEIGHTS[0]), jnp.float32)
    for i in range(1, 8):
        out = jnp.where(row == i, float(WEIGHTS[i]), out)
    return out


def s_column():
    row = iota((8, LANES), 0)
    out = jnp.full((8, LANES), float(STIFF[0, 0]), jnp.float32)
    for i in range(1, 8):
        out = jnp.where(row == i, float(STIFF[i, i]), out)
    return out


def sum_xy(ref, planes):
    rows = planes * 8
    lane = iota((rows, LANES), 1)
    low = ref[pl.ds(0, rows, stride=8), :]
    high = ref[pl.ds(7, rows, stride=8), :]
    ref[pl.ds(7, rows, stride=8), :] = high + jnp.where(
        lane % 8 < 7, pltpu.roll(low, LANES - 1, 1), 0.0
    )
    ref[pl.ds(0, rows, stride=8), :] = low + jnp.where(lane % 8 > 0, pltpu.roll(high, 1, 1), 0.0)
    lane = iota((8, LANES), 1)
    for k in range(planes):
        low = ref[k * 64 : k * 64 + 8, :]
        high = ref[k * 64 + 56 : k * 64 + 64, :]
        ref[k * 64 + 56 : k * 64 + 64, :] = high + jnp.where(
            lane < 120, pltpu.roll(low, LANES - 8, 1), 0.0
        )
        ref[k * 64 : k * 64 + 8, :] = low + jnp.where(lane >= 8, pltpu.roll(high, 8, 1), 0.0)


def apply_local(v_ref, geometry, xmat_ref, out_ref, planes, dot_with_v=False):
    wcol = w_column()
    gx = geometry[0:1, :]
    gyw = geometry[1:2, :] * wcol
    gzw = geometry[2:3, :] * wcol
    gmw = geometry[3:4, :] * wcol
    total = jnp.zeros((8, LANES), jnp.float32)
    if len(planes) == 8:
        along_x = [
            lax.dot(
                xmat_ref[256 * h : 256 * h + 256, :],
                v_ref[256 * h : 256 * h + 256, :],
                precision=HIGHEST,
                preferred_element_type=jnp.float32,
            )
            for h in range(2)
        ]
        for h in range(2):
            out_ref[256 * h : 256 * h + 256, :] = along_x[h]
    else:
        for at, k in enumerate(planes):
            h = k // 4
            out_ref[at * 64 : at * 64 + 64, :] = lax.dot(
                xmat_ref[k * 64 : k * 64 + 64, :],
                v_ref[256 * h : 256 * h + 256, :],
                precision=HIGHEST,
                preferred_element_type=jnp.float32,
            )
    for at, k in enumerate(planes):
        plane = [v_ref[(k * 8 + j) * 8 : (k * 8 + j) * 8 + 8, :] for j in range(8)]
        for j in range(8):
            ysum = plane[0] * float(STIFF[j, 0] * WEIGHTS[k])
            for jj in range(1, 8):
                ysum = ysum + plane[jj] * float(STIFF[j, jj] * WEIGHTS[k])
            zsum = None
            for kk in range(8):
                term = v_ref[(kk * 8 + j) * 8 : (kk * 8 + j) * 8 + 8, :] * float(
                    STIFF[k, kk] * WEIGHTS[j]
                )
                zsum = term if zsum is None else zsum + term
            row = (at * 8 + j) * 8
            value = (
                out_ref[row : row + 8, :] * gx
                + gyw * ysum
                + gzw * zsum
                + gmw * (plane[j] * float(WEIGHTS[k] * WEIGHTS[j]))
            )
            out_ref[row : row + 8, :] = value
            if dot_with_v:
                total = total + value * plane[j]
    return total


def lane_value(value, at):
    return jnp.where(iota((1, LANES), 1) == at, value, 0.0)


def by_side(q, cross_1, inner_1, cross_2=None, inner_2=None):
    above = from_above(q)
    out = (jnp.where(above[0], inner_1, cross_1), jnp.where(above[0], cross_1, inner_1))
    if cross_2 is not None:
        out += (jnp.where(above[2], inner_2, cross_2), jnp.where(above[2], cross_2, inner_2))
    return out


def route_kernel(
    place_ref, weights_ref, owner_ref, element_ref, geometry_ref, wall_ref, forcing_ref,
    cross_1_ref, inner_1_ref, cross_2_ref, inner_2_ref, own_ref, moves_ref, slots_ref,
):
    q = place_ref[0]
    width = N_REC
    lane = iota((8, width), 1)
    row = iota((8, width), 0)
    distance = owner_ref[...] - q + 2
    mine = distance == row
    count = mine.astype(jnp.int32)
    step = 1
    while step < width:
        count = count + jnp.where(lane >= step, pltpu.roll(count, step, 1), 0)
        step *= 2
    moves = jnp.where(mine, lane - (count - 1), 0)
    totals = count[:, width - 1 : width]
    node_rows = iota((8, width), 0)
    node = jnp.full((8, width), float(NODES[0]), jnp.float32)
    for i in range(1, 8):
        node = jnp.where(node_rows == i, float(NODES[i]), node)
    coords = [jnp.sum(weights_ref[d] * node, axis=0, keepdims=True) for d in range(3)]
    words = element_ref[...].astype(jnp.float32) + 1.0
    base = jnp.where(row % 4 == 3, words, 0.0)
    for d in range(3):
        base = jnp.where(row % 4 == d, coords[d], base)
    packs = [base, base, base]
    for b in range(11):
        step = 1 << b
        incoming = pltpu.roll(moves, width - step, 1)
        moved = (incoming >> b) & 1
        for n in range(3):
            first = jnp.broadcast_to(moved[2 * n : 2 * n + 1, :], (8, width))
            if n < 2:
                second = jnp.broadcast_to(moved[2 * n + 1 : 2 * n + 2, :], (8, width))
                first = jnp.where(row < 4, first, second)
            packs[n] = jnp.where(first == 1, pltpu.roll(packs[n], width - step, 1), packs[n])
        moves = jnp.where(moved == 1, incoming, jnp.where((moves >> b) & 1 == 1, 0, moves))
    moves_ref[...] = moves[:, :CAP]
    lane = iota((4, CAP), 1)
    for s in range(5):
        at = (s % 2) * 4
        slot = jnp.where(lane < totals[s : s + 1, :], packs[s // 2][at : at + 4, :CAP], 0.0)
        for c in range(8):
            slots_ref[s, 4 * c : 4 * c + 4, :] = slot[:, c * LANES : (c + 1) * LANES]
    above = from_above(q)
    bottom, top = forcing_ref[0:64, :], forcing_ref[448:512, :]
    spread = jnp.where(iota((8, LANES), 1) % 8 == iota((8, LANES), 0), 1.0, 0.0)
    wall = lax.dot(
        wall_ref[...].astype(jnp.float32), spread, preferred_element_type=jnp.float32
    )
    for target_ref, up in ((cross_1_ref, above[0]), (inner_1_ref, above[1])):
        target_ref[0:32, :] = jnp.where(up, slots_ref[3], slots_ref[1])
        target_ref[32:36, :] = geometry_ref[...]
        target_ref[36:38, :] = wall
        target_ref[38:40, :] = jnp.zeros((2, LANES), jnp.float32)
        target_ref[40:104, :] = jnp.where(up, top, bottom)
    for target_ref, up in ((cross_2_ref, above[2]), (inner_2_ref, above[3])):
        target_ref[...] = jnp.where(up, slots_ref[4], slots_ref[0])
    own_ref[...] = slots_ref[2]


def split_kernel(fields_ref, out_ref):
    for f in range(FIELDS):
        value = fields_ref[f]
        high = value.astype(jnp.bfloat16)
        out_ref[f, :, 0:LANES] = high
        out_ref[f, :, LANES : 2 * LANES] = (value - high.astype(jnp.float32)).astype(jnp.bfloat16)


def basis_rows(coordinate):
    gaps = [coordinate - float(NODES[i]) for i in range(8)]
    before = [None] * 8
    after = [None] * 8
    for i in range(1, 8):
        before[i] = gaps[i - 1] if i == 1 else before[i - 1] * gaps[i - 1]
    for i in range(6, -1, -1):
        after[i] = gaps[i + 1] if i == 6 else after[i + 1] * gaps[i + 1]
    out = []
    for i in range(8):
        if i == 0:
            value = after[0]
        elif i == 7:
            value = before[7]
        else:
            value = before[i] * after[i]
        out.append(value * float(BARY[i]))
    return out


def eval_kernel(*refs):
    sources, fields_ref, targets = refs[0:5], refs[5], refs[6:11]
    for source, target in zip(sources, targets):
        words = source[0:32, :]
        valid = jnp.where((iota((32, LANES), 0) % 4 == 3) & (words > 0.0), 1, 0)
        blocks = (jnp.sum(valid) + BLOCK - 1) // BLOCK

        def one_block(b, carry, source=source, target=target):
            start = pl.multiple_of(b * BLOCK, BLOCK)
            tiles = source[pl.ds(pl.multiple_of(b * 16, 16), 16), :]
            words = jnp.concatenate([tiles[4 * n : 4 * n + 4, :] for n in range(4)], axis=1)
            element = words[3:4, :].astype(jnp.int32) - 1
            hot = (iota((LANES, BLOCK), 0) == element).astype(jnp.float32).astype(jnp.bfloat16)
            hot = jnp.concatenate([hot, hot], axis=0)
            along = [basis_rows(words[d : d + 1, :]) for d in range(3)]
            row = iota((8, BLOCK), 0)
            wx = jnp.broadcast_to(along[0][0], (8, BLOCK))
            for i in range(1, 8):
                wx = jnp.where(row == i, along[0][i], wx)
            for f in range(FIELDS):
                picked = lax.dot(
                    fields_ref[f], hot, preferred_element_type=jnp.float32
                )
                over_k = picked[0:64, :] * along[2][0]
                for k in range(1, 8):
                    over_k = over_k + picked[64 * k : 64 * k + 64, :] * along[2][k]
                over_j = over_k[0:8, :] * along[1][0]
                for j in range(1, 8):
                    over_j = over_j + over_k[8 * j : 8 * j + 8, :] * along[1][j]
                target[f : f + 1, pl.ds(start, BLOCK)] = jnp.sum(
                    over_j * wx, axis=0, keepdims=True
                )
            return carry

        lax.fori_loop(0, blocks, one_block, 0)


def unpack_kernel(
    place_ref, cross_1_ref, inner_1_ref, cross_2_ref, inner_2_ref, own_ref, moves_ref, owner_ref,
    out_ref, share_ref,
):
    q = place_ref[0]
    width = N_REC
    below_1, above_1, below_2, above_2 = by_side(
        q, cross_1_ref[...], inner_1_ref[...], cross_2_ref[...], inner_2_ref[...]
    )
    zeros = jnp.zeros((FIELDS, CAP), jnp.float32)
    values = [
        jnp.concatenate([value, zeros], axis=1)
        for value in (below_2, below_1, own_ref[...], above_1, above_2)
    ]
    moves = jnp.concatenate([moves_ref[...], jnp.zeros((8, CAP), jnp.int32)], axis=1)
    for b in range(10, -1, -1):
        step = 1 << b
        incoming = pltpu.roll(moves, step, 1)
        moved = (incoming >> b) & 1
        for s in range(5):
            flag = jnp.broadcast_to(moved[s : s + 1, :], (FIELDS, width))
            values[s] = jnp.where(flag == 1, pltpu.roll(values[s], step, 1), values[s])
        moves = jnp.where(moved == 1, incoming, jnp.where((moves >> b) & 1 == 1, 0, moves))
    distance = jnp.broadcast_to(owner_ref[...] - q + 2, (FIELDS, width))
    out = values[0]
    for s in range(1, 5):
        out = jnp.where(distance == s, values[s], out)
    out_ref[...] = out
    for n in range(16):
        share_ref[n : n + 1, :] = out[0:1, n * LANES : (n + 1) * LANES]


def prep_kernel(
    place_ref, geometry_ref, wall_ref, forcing_ref, cross_ref, inner_ref,
    inverse_ref, free_ref, load_ref, beside_ref, plane_ref, below_ref, above_ref,
):
    q = place_ref[0]
    below_ref[...], above_ref[...] = by_side(q, cross_ref[32:104, :], inner_ref[32:104, :])
    beside_ref[0:8, :] = below_ref[0:8, :]
    beside_ref[8:16, :] = above_ref[0:8, :]
    wcol = w_column()
    scol = s_column()

    def diagonal(geometry, k, j):
        wk, wj = float(WEIGHTS[k]), float(WEIGHTS[j])
        sk, sj = float(STIFF[k, k]), float(STIFF[j, j])
        return (
            geometry[0:1, :] * (scol * (wk * wj))
            + geometry[1:2, :] * (wcol * (wk * sj))
            + geometry[2:3, :] * (wcol * (sk * wj))
            + geometry[3:4, :] * (wcol * (wk * wj))
        )

    geometry = geometry_ref[...]
    below = below_ref[0:8, :]
    above = above_ref[0:8, :]
    lane = iota((8, LANES), 1)
    row = iota((8, LANES), 0)
    zero = jnp.zeros((8, LANES), jnp.float32)

    def wall_plane(low, high):
        for j in range(8):
            plane_ref[8 * j : 8 * j + 8, :] = zero
        plane_ref[0:8, :] = jnp.where(lane < 8, low, 0.0) + zero
        plane_ref[56:64, :] = jnp.where(lane >= 120, high, 0.0) + zero
        sum_xy(plane_ref, 1)
        return plane_ref[...]

    spread = jnp.where(lane % 8 == row, 1.0, 0.0)
    flags = lax.dot(
        wall_ref[...].astype(jnp.float32), spread, preferred_element_type=jnp.float32
    )
    wall = wall_plane(flags[0:1, :], flags[1:2, :])
    wall_below = wall_plane(below[4:5, :], below[5:6, :])
    wall_above = wall_plane(above[4:5, :], above[5:6, :])
    mark = jnp.where(
        ((row == 0) & (lane % 8 == 0)) | ((row == 7) & (lane % 8 == 7)), 1.0, 0.0
    )
    for j in range(8):
        plane_ref[8 * j : 8 * j + 8, :] = mark
    sum_xy(plane_ref, 1)
    rec = plane_ref[...]
    has_below = jnp.where(q > 0, 1.0, 0.0)
    has_above = jnp.where(q < N_DOM - 1, 1.0, 0.0)
    inner = 1.0 - jnp.minimum(rec + wall, 1.0)
    bottom = 1.0 - jnp.minimum(rec + rec * has_below + (wall + wall_below), 1.0)
    top = 1.0 - jnp.minimum(rec + rec * has_above + (wall + wall_above), 1.0)
    free_ref[0:64, :] = bottom
    free_ref[448:512, :] = top
    for k in range(1, 7):
        free_ref[64 * k : 64 * k + 64, :] = inner

    for k in range(8):
        for j in range(8):
            inverse_ref[(k * 8 + j) * 8 : (k * 8 + j) * 8 + 8, :] = diagonal(geometry, k, j)
    sum_xy(inverse_ref, 8)
    for j in range(8):
        plane_ref[8 * j : 8 * j + 8, :] = diagonal(below, 7, j)
    sum_xy(plane_ref, 1)
    inverse_ref[0:64, :] = inverse_ref[0:64, :] + plane_ref[...]
    for j in range(8):
        plane_ref[8 * j : 8 * j + 8, :] = diagonal(above, 0, j)
    sum_xy(plane_ref, 1)
    inverse_ref[448:512, :] = inverse_ref[448:512, :] + plane_ref[...]
    for k in range(8):
        at = slice(64 * k, 64 * k + 64)
        inverse_ref[at, :] = free_ref[at, :] / inverse_ref[at, :]

    for k in range(8):
        for j in range(8):
            at = slice((k * 8 + j) * 8, (k * 8 + j) * 8 + 8)
            load_ref[at, :] = forcing_ref[at, :] * (
                geometry[3:4, :] * (wcol * float(WEIGHTS[k] * WEIGHTS[j]))
            )
    sum_xy(load_ref, 8)
    for other_ref, k, base in ((below_ref, 7, 0), (above_ref, 0, 448)):
        for j in range(8):
            plane_ref[8 * j : 8 * j + 8, :] = other_ref[8 + 8 * j : 16 + 8 * j, :] * (
                other_ref[3:4, :] * (wcol * float(WEIGHTS[k] * WEIGHTS[j]))
            )
        sum_xy(plane_ref, 1)
        load_ref[base : base + 64, :] = load_ref[base : base + 64, :] + plane_ref[...]


def inverse_multiplicity(q):
    row = iota((64, LANES), 0)
    lane = iota((64, LANES), 1)
    i, j = row % 8, row // 8
    x, y = lane % 8, lane // 8
    along_x = ((i == 0) & (x > 0)) | ((i == 7) & (x < 7))
    along_y = ((j == 0) & (y > 0)) | ((j == 7) & (y < 15))
    inner = jnp.where(along_x, 0.5, 1.0) * jnp.where(along_y, 0.5, 1.0)
    return (
        inner,
        inner * jnp.where(q > 0, 0.5, 1.0),
        inner * jnp.where(q < N_DOM - 1, 0.5, 1.0),
    )


def krylov_step(q, w_ref, inverse_ref, geometry_ref, xmat_ref, v_ref, u_ref, at, moments):
    inner, bottom, top = inverse_multiplicity(q)
    norm = jnp.zeros((64, LANES), jnp.float32)
    for k in range(8):
        rows = slice(64 * k, 64 * k + 64)
        w = w_ref[rows, :]
        v = inverse_ref[rows, :] * w
        v_ref[rows, :] = v
        norm = norm + v * w * (bottom if k == 0 else top if k == 7 else inner)
    energy = apply_local(
        v_ref, geometry_ref[...], xmat_ref, u_ref, tuple(range(8)), dot_with_v=True
    )
    sum_xy(u_ref, 8)
    return moments + lane_value(jnp.sum(norm), at) + lane_value(jnp.sum(energy), at + 1)


def first_kernel(
    place_ref, own_ref, cross_1_ref, inner_1_ref, cross_2_ref, inner_2_ref, geometry_ref,
    beside_ref, inverse_ref, free_ref, load_ref, xmat_ref, w_ref, u_ref, edge_ref, moments_ref, cross_ref, inner_ref, v_ref, face_ref,
):
    q = place_ref[0]
    below_1, above_1, below_2, above_2 = by_side(
        q, cross_1_ref[...], inner_1_ref[...], cross_2_ref[...], inner_2_ref[...]
    )
    pick_row = iota((8, LANES), 0)
    pick_lane = iota((8, LANES), 1)
    picks = [
        [
            jnp.where(pick_lane == pick_row * 16 + (8 * odd + 7 * s), 1.0, 0.0)
            for odd in range(2)
        ]
        for s in range(2)
    ]

    def planes(values):
        out = []
        for s in range(2):
            halves = [
                lax.dot_general(
                    values[8 * s : 8 * s + 8, :], picks[s][odd], (((0,), (0,)), ((), ())),
                    precision=HIGHEST, preferred_element_type=jnp.float32,
                )
                for odd in range(2)
            ]
            plane = halves[0][0:64, :] + halves[1][64:128, :]
            out.append([plane[8 * k : 8 * k + 8, :] for k in range(8)])
        return out

    layers = (below_2, below_1, own_ref[...], above_1, above_2)
    received = {off: planes(values) for off, values in zip(range(-2, 3), layers)}
    lane = iota((8, LANES), 1)
    j_row = iota((8, LANES), 0)
    low = (j_row == 0) & (lane >= 8)
    high = (j_row == 7) & (lane < 120)

    def sum_y(value):
        down = jnp.broadcast_to(pltpu.roll(value, LANES - 8, 1)[0:1, :], (8, LANES))
        up = jnp.broadcast_to(pltpu.roll(value, 8, 1)[7:8, :], (8, LANES))
        return value + jnp.where(high, down, 0.0) + jnp.where(low, up, 0.0)

    count_y = jnp.where(low | high, 2.0, 1.0)
    on_side = [jnp.where(lane % 8 == x, 1.0, 0.0) for x in (0, 7)]

    def boundary(off):
        out = []
        has_below = jnp.where(q + off > 0, 1.0, 0.0)
        has_above = jnp.where(q + off < N_DOM - 1, 1.0, 0.0)
        for s in range(2):
            side = []
            for k in range(8):
                total = received[off][s][k]
                count = count_y * on_side[s]
                if k == 0:
                    total = total + received[off - 1][s][7]
                    count = count + count * has_below
                if k == 7:
                    total = total + received[off + 1][s][0]
                    count = count + count * has_above
                side.append(sum_y(total) / jnp.maximum(count, 1.0))
            out.append(jnp.concatenate(side, axis=0))
        return out

    zero = jnp.zeros((64, LANES), jnp.float32)
    for k in range(8):
        v_ref[64 * k : 64 * k + 64, :] = zero
    for off, geometry, plane in ((-1, beside_ref[0:4, :], 7), (1, beside_ref[8:12, :], 0)):
        sides = boundary(off)
        v_ref[pl.ds(0, 64, stride=8), :] = sides[0]
        v_ref[pl.ds(7, 64, stride=8), :] = sides[1]
        at = 0 if off < 0 else 64
        apply_local(v_ref, geometry, xmat_ref, face_ref.at[at : at + 64, :], (plane,))
        sum_xy(face_ref.at[at : at + 64, :], 1)
    sides = boundary(0)
    v_ref[pl.ds(0, 64, stride=8), :] = sides[0]
    v_ref[pl.ds(7, 64, stride=8), :] = sides[1]
    edge_ref[0:64, :] = sides[0]
    edge_ref[64:128, :] = sides[1]
    apply_local(v_ref, geometry_ref[...], xmat_ref, u_ref, tuple(range(8)))
    sum_xy(u_ref, 8)
    u_ref[0:64, :] = u_ref[0:64, :] + face_ref[0:64, :]
    u_ref[448:512, :] = u_ref[448:512, :] + face_ref[64:128, :]
    for k in range(8):
        rows = slice(64 * k, 64 * k + 64)
        w_ref[rows, :] = free_ref[rows, :] * (load_ref[rows, :] - u_ref[rows, :])
    moments_ref[...] = krylov_step(
        q, w_ref, inverse_ref, geometry_ref, xmat_ref, v_ref, u_ref, 0,
        jnp.zeros((1, LANES), jnp.float32),
    )
    send_faces(q, u_ref, cross_ref, inner_ref)


def send_faces(q, u_ref, cross_ref, inner_ref):
    up = from_above(q)[0]
    bottom, top = u_ref[0:64, :], u_ref[448:512, :]
    cross_ref[...] = jnp.where(up, top, bottom)
    inner_ref[...] = jnp.where(up, bottom, top)


def next_kernel(
    at, place_ref, w_old_ref, u_old_ref, cross_in_ref, inner_in_ref, geometry_ref, inverse_ref,
    free_ref, xmat_ref, moments_old_ref, w_ref, u_ref, moments_ref, cross_ref, inner_ref, v_ref,
):
    q = place_ref[0]
    below, above = by_side(q, cross_in_ref[...], inner_in_ref[...])
    for k in range(8):
        rows = slice(64 * k, 64 * k + 64)
        image = u_old_ref[rows, :]
        if k == 0:
            image = image + below
        if k == 7:
            image = image + above
        w_ref[rows, :] = free_ref[rows, :] * image - w_old_ref[rows, :]
    row = krylov_step(
        q, w_ref, inverse_ref, geometry_ref, xmat_ref, v_ref, u_ref, at, moments_old_ref[...]
    )
    moments_ref[...] = jnp.broadcast_to(row, moments_ref.shape)
    send_faces(q, u_ref, cross_ref, inner_ref)


def image_kernel(place_ref, u_ref, cross_in_ref, inner_in_ref, free_ref, image_ref):
    below, above = by_side(place_ref[0], cross_in_ref[...], inner_in_ref[...])
    image_ref[...] = free_ref[...] * u_ref[...]
    image_ref[0:64, :] = image_ref[0:64, :] + free_ref[0:64, :] * below
    image_ref[448:512, :] = image_ref[448:512, :] + free_ref[448:512, :] * above


def last_kernel(
    w0_ref, w1_ref, w2_ref, image_ref, inverse_ref, edge_ref, moments_ref, velocity_ref,
    residual_ref,
):
    sums = jnp.sum(moments_ref[...], axis=0, keepdims=True)
    h0, a0, h2, a1, h4, a2 = [sums[:, m : m + 1] for m in range(6)]
    h1, h3 = a0 - h0, a1 - h2
    g00, g01, g02, g11, g12, g22 = a0, h2 + h1, h3 + h2, a1, h4 + h3, a2
    b0, b1, b2 = h0, h1, h2
    l10 = g01 / g00
    l20 = g02 / g00
    d1 = g11 - l10 * g01
    e12 = g12 - l10 * g02
    l21 = e12 / d1
    d2 = g22 - l20 * g02 - l21 * e12
    y1 = b1 - l10 * b0
    y2 = b2 - l20 * b0 - l21 * y1
    c2 = y2 / d2
    c1 = y1 / d1 - l21 * c2
    c0 = b0 / g00 - l10 * c1 - l20 * c2
    c0, c1, c2 = [jnp.broadcast_to(c, (64, LANES)) for c in (c0, c1, c2)]
    for k in range(8):
        rows = slice(64 * k, 64 * k + 64)
        w0, w1, w2 = w0_ref[rows, :], w1_ref[rows, :], w2_ref[rows, :]
        velocity_ref[rows, :] = inverse_ref[rows, :] * (c0 * w0 + c1 * w1 + c2 * w2)
        residual_ref[rows, :] = (
            w0 - c0 * (w1 + w0) - c1 * (w2 + w1) - c2 * image_ref[rows, :]
        )
    for s in range(2):
        rows = pl.ds(7 * s, 64, stride=8)
        velocity_ref[rows, :] = velocity_ref[rows, :] + edge_ref[64 * s : 64 * s + 64, :]


VMEM = pl.BlockSpec(memory_space=pltpu.VMEM)
SMEM = pl.BlockSpec(memory_space=pltpu.SMEM)


def call(kernel, operands, outs, scratch=(), flops=100_000, smem_first=True, mib=12):
    specs = [VMEM] * len(operands)
    if smem_first:
        specs[0] = SMEM
    out_shape = [jax.ShapeDtypeStruct(shape, dtype) for shape, dtype in outs]
    return pl.pallas_call(
        kernel,
        out_shape=out_shape,
        in_specs=specs,
        out_specs=[VMEM] * len(outs),
        scratch_shapes=[pltpu.VMEM(shape, dtype) for shape, dtype in scratch],
        cost_estimate=pl.CostEstimate(flops=flops, bytes_accessed=1_000_000, transcendentals=0),
        compiler_params=pltpu.CompilerParams(vmem_limit_bytes=mib * 1024 * 1024),
    )(*operands)


F32 = jnp.float32
FIELD = ((512, LANES), F32)


def to_all(value):
    return lax.all_to_all(value, "dom", 0, 0, tiled=True)


def to_neighbours(cross_1, inner_1, cross_2=None, inner_2=None):
    lists = ((cross_1, CROSS_1), (cross_2, CROSS_2), (inner_1, INNER_1), (inner_2, INNER_2))
    moved = []
    for value, pairs in lists:
        moved.append(None if value is None else lax.ppermute(value, "dom", pairs))
    return [moved[n] for n in (0, 2, 1, 3) if moved[n] is not None]


def body(donor_fields, interp_weights, donor_owner, donor_element, geometry, wall_flag, forcing):
    place = lax.axis_index("dom").astype(jnp.int32).reshape(1)
    xmat = jnp.asarray(x_matrix())
    donors = lax.ppermute(donor_fields, "mesh", [(0, 1), (1, 0)])
    owner = donor_owner.reshape(1, N_REC)
    element = donor_element.reshape(1, N_REC)
    asked = ((32, LANES), F32)
    with_head = ((CHUNK, LANES), F32)
    *requests, own, moves = call(
        route_kernel, (place, interp_weights, owner, element, geometry, wall_flag, forcing),
        (with_head, with_head, asked, asked, asked, ((8, CAP), jnp.int32)),
        scratch=(((5, 32, LANES), F32),), mib=60,
    )
    requests = to_neighbours(*requests)
    (fields,) = call(
        split_kernel, (donors,), (((FIELDS, 512, 256), jnp.bfloat16),), smem_first=False,
    )
    answers = call(
        eval_kernel, (*requests, own, fields), (((FIELDS, CAP), F32),) * 5,
        flops=7_000_000_000, smem_first=False, mib=24,
    )
    answered = to_neighbours(*answers[0:4])
    inverse, free, load, beside = call(
        prep_kernel, (place, geometry, wall_flag, forcing, requests[0], requests[1]),
        (FIELD, FIELD, FIELD, ((16, LANES), F32)),
        scratch=(((64, LANES), F32), ((72, LANES), F32), ((72, LANES), F32)),
    )
    interface, share = call(
        unpack_kernel, (place, *answered, answers[4], moves, owner),
        (((FIELDS, N_REC), F32), ((16, LANES), F32)),
    )
    face = ((64, LANES), F32)
    w0, u, edge, moments, *faces = call(
        first_kernel,
        (place, share, *to_neighbours(share, share, share, share), geometry, beside, inverse, free,
         load, xmat),
        (FIELD, FIELD, ((128, LANES), F32), ((1, LANES), F32), face, face),
        scratch=(FIELD, ((128, LANES), F32)),
    )
    ws = [w0]
    for step in (1, 2):
        w, u, moments, *faces = call(
            functools.partial(next_kernel, 2 * step),
            (place, ws[-1], u, *to_neighbours(*faces), geometry, inverse, free, xmat, moments),
            (FIELD, FIELD, ((1 if step == 1 else N_DOM, LANES), F32), face, face),
            scratch=(FIELD,),
        )
        ws.append(w)
    sums = to_all(moments)
    (image,) = call(image_kernel, (place, u, *to_neighbours(*faces), free), (FIELD,))
    velocity, residual = call(
        last_kernel, (*ws, image, inverse, edge, sums), (FIELD, FIELD), smem_first=False,
    )
    return velocity, residual, interface


def solution(mesh):
    both = ("mesh", "dom")
    in_specs = (
        P(None, None, both), P(None, None, both), P(both, None), P(both), P(None, both),
        P(None, both), P(None, both),
    )
    out_specs = (P(None, both), P(None, both), P(None, both))

    return jax.shard_map(body, mesh=mesh, in_specs=in_specs, out_specs=out_specs, check_vma=False)
```

```python
import functools

import jax
import jax.numpy as jnp
import numpy as np
from jax import lax
from jax.experimental import pallas as pl
from jax.experimental.pallas import tpu as pltpu
from jax.sharding import PartitionSpec as P


HIGHEST = lax.Precision.HIGHEST
N_DOM = 64
N_REC = 2048
CAP = 1024
FIELDS = 5
LANES = 128
BLOCK = 512
CHUNK = 104


def both_ways(lows, distance):
    return [pair for q in lows for pair in ((q, q + distance), (q + distance, q))]


CROSS_1 = both_ways(range(1, N_DOM - 1, 2), 1)
INNER_1 = both_ways(range(0, N_DOM - 1, 2), 1)
CROSS_2 = both_ways([q for q in range(N_DOM - 2) if q % 4 >= 2], 2)
INNER_2 = both_ways([q for q in range(N_DOM - 2) if q % 4 < 2], 2)


def from_above(q):
    odd = q % 2 == 1
    late = q % 4 >= 2
    return odd, jnp.logical_not(odd), late, jnp.logical_not(late)


def legendre_pair(values, degree):
    previous = values * 0.0 + 1.0
    current = values * 1.0
    for order in range(2, degree + 1):
        previous, current = (
            current,
            ((2 * order - 1) * values * current - (order - 1) * previous) / order,
        )
    return current, previous


def gll_tables():
    degree = 7
    count = degree + 1
    nodes = np.cos(np.pi * np.arange(count) / degree)
    for _ in range(80):
        top, lower = legendre_pair(nodes, degree)
        nodes = nodes - (nodes * top - lower) / (count * top)
    nodes = np.sort(nodes)
    top, lower = legendre_pair(nodes, degree)
    weights = 2.0 / (degree * count * top * top)
    identity = np.eye(count)
    spacing = nodes[:, None] - nodes[None, :] + identity
    derivative = top[:, None] / (top[None, :] * spacing) * (1.0 - identity)
    derivative[0, 0] = -degree * count / 4.0
    derivative[degree, degree] = degree * count / 4.0
    return nodes, weights, derivative


NODES, WEIGHTS, DERIV = gll_tables()
STIFF = DERIV.T @ (WEIGHTS[:, None] * DERIV)
STIFF = 0.5 * (STIFF + STIFF.T)
BARY = np.array([1.0 / np.prod([NODES[i] - NODES[j] for j in range(8) if j != i]) for i in range(8)])


def x_matrix():
    out = np.zeros((512, 256))
    for k in range(8):
        for j in range(8):
            row = (k * 8 + j) * 8
            col = row % 256
            out[row : row + 8, col : col + 8] = WEIGHTS[k] * WEIGHTS[j] * STIFF
    return out.astype(np.float32)


def iota(shape, dim):
    return lax.broadcasted_iota(jnp.int32, shape, dim)


def w_column():
    row = iota((8, LANES), 0)
    out = jnp.full((8, LANES), float(WEIGHTS[0]), jnp.float32)
    for i in range(1, 8):
        out = jnp.where(row == i, float(WEIGHTS[i]), out)
    return out


def s_column():
    row = iota((8, LANES), 0)
    out = jnp.full((8, LANES), float(STIFF[0, 0]), jnp.float32)
    for i in range(1, 8):
        out = jnp.where(row == i, float(STIFF[i, i]), out)
    return out


def sum_xy(ref, planes):
    rows = planes * 8
    lane = iota((rows, LANES), 1)
    low = ref[pl.ds(0, rows, stride=8), :]
    high = ref[pl.ds(7, rows, stride=8), :]
    ref[pl.ds(7, rows, stride=8), :] = high + jnp.where(
        lane % 8 < 7, pltpu.roll(low, LANES - 1, 1), 0.0
    )
    ref[pl.ds(0, rows, stride=8), :] = low + jnp.where(lane % 8 > 0, pltpu.roll(high, 1, 1), 0.0)
    lane = iota((8, LANES), 1)
    for k in range(planes):
        low = ref[k * 64 : k * 64 + 8, :]
        high = ref[k * 64 + 56 : k * 64 + 64, :]
        ref[k * 64 + 56 : k * 64 + 64, :] = high + jnp.where(
            lane < 120, pltpu.roll(low, LANES - 8, 1), 0.0
        )
        ref[k * 64 : k * 64 + 8, :] = low + jnp.where(lane >= 8, pltpu.roll(high, 8, 1), 0.0)


def apply_local(v_ref, geometry, xmat_ref, out_ref, planes, dot_with_v=False):
    wcol = w_column()
    gx = geometry[0:1, :]
    gyw = geometry[1:2, :] * wcol
    gzw = geometry[2:3, :] * wcol
    gmw = geometry[3:4, :] * wcol
    total = jnp.zeros((8, LANES), jnp.float32)
    if len(planes) == 8:
        along_x = [
            lax.dot(
                xmat_ref[256 * h : 256 * h + 256, :],
                v_ref[256 * h : 256 * h + 256, :],
                precision=HIGHEST,
                preferred_element_type=jnp.float32,
            )
            for h in range(2)
        ]
        for h in range(2):
            out_ref[256 * h : 256 * h + 256, :] = along_x[h]
    else:
        for at, k in enumerate(planes):
            h = k // 4
            out_ref[at * 64 : at * 64 + 64, :] = lax.dot(
                xmat_ref[k * 64 : k * 64 + 64, :],
                v_ref[256 * h : 256 * h + 256, :],
                precision=HIGHEST,
                preferred_element_type=jnp.float32,
            )
    for at, k in enumerate(planes):
        plane = [v_ref[(k * 8 + j) * 8 : (k * 8 + j) * 8 + 8, :] for j in range(8)]
        for j in range(8):
            ysum = plane[0] * float(STIFF[j, 0] * WEIGHTS[k])
            for jj in range(1, 8):
                ysum = ysum + plane[jj] * float(STIFF[j, jj] * WEIGHTS[k])
            zsum = None
            for kk in range(8):
                term = v_ref[(kk * 8 + j) * 8 : (kk * 8 + j) * 8 + 8, :] * float(
                    STIFF[k, kk] * WEIGHTS[j]
                )
                zsum = term if zsum is None else zsum + term
            row = (at * 8 + j) * 8
            value = (
                out_ref[row : row + 8, :] * gx
                + gyw * ysum
                + gzw * zsum
                + gmw * (plane[j] * float(WEIGHTS[k] * WEIGHTS[j]))
            )
            out_ref[row : row + 8, :] = value
            if dot_with_v:
                total = total + value * plane[j]
    return total


def lane_value(value, at):
    return jnp.where(iota((1, LANES), 1) == at, value, 0.0)


def by_side(q, cross_1, inner_1, cross_2=None, inner_2=None):
    above = from_above(q)
    out = (jnp.where(above[0], inner_1, cross_1), jnp.where(above[0], cross_1, inner_1))
    if cross_2 is not None:
        out += (jnp.where(above[2], inner_2, cross_2), jnp.where(above[2], cross_2, inner_2))
    return out


def route_kernel(
    place_ref, weights_ref, owner_ref, element_ref, geometry_ref, wall_ref, forcing_ref,
    cross_1_ref, inner_1_ref, cross_2_ref, inner_2_ref, own_ref, moves_ref, slots_ref,
):
    q = place_ref[0]
    width = N_REC
    lane = iota((8, width), 1)
    row = iota((8, width), 0)
    distance = owner_ref[...] - q + 2
    mine = distance == row
    count = mine.astype(jnp.int32)
    step = 1
    while step < width:
        count = count + jnp.where(lane >= step, pltpu.roll(count, step, 1), 0)
        step *= 2
    moves = jnp.where(mine, lane - (count - 1), 0)
    totals = count[:, width - 1 : width]
    node_rows = iota((8, width), 0)
    node = jnp.full((8, width), float(NODES[0]), jnp.float32)
    for i in range(1, 8):
        node = jnp.where(node_rows == i, float(NODES[i]), node)
    coords = [jnp.sum(weights_ref[d] * node, axis=0, keepdims=True) for d in range(3)]
    words = element_ref[...].astype(jnp.float32) + 1.0
    base = jnp.where(row % 4 == 3, words, 0.0)
    for d in range(3):
        base = jnp.where(row % 4 == d, coords[d], base)
    packs = [base, base, base]
    for b in range(11):
        step = 1 << b
        incoming = pltpu.roll(moves, width - step, 1)
        moved = (incoming >> b) & 1
        for n in range(3):
            first = jnp.broadcast_to(moved[2 * n : 2 * n + 1, :], (8, width))
            if n < 2:
                second = jnp.broadcast_to(moved[2 * n + 1 : 2 * n + 2, :], (8, width))
                first = jnp.where(row < 4, first, second)
            packs[n] = jnp.where(first == 1, pltpu.roll(packs[n], width - step, 1), packs[n])
        moves = jnp.where(moved == 1, incoming, jnp.where((moves >> b) & 1 == 1, 0, moves))
    moves_ref[...] = moves[:, :CAP]
    lane = iota((4, CAP), 1)
    for s in range(5):
        at = (s % 2) * 4
        slot = jnp.where(lane < totals[s : s + 1, :], packs[s // 2][at : at + 4, :CAP], 0.0)
        for c in range(8):
            slots_ref[s, 4 * c : 4 * c + 4, :] = slot[:, c * LANES : (c + 1) * LANES]
    above = from_above(q)
    bottom, top = forcing_ref[0:64, :], forcing_ref[448:512, :]
    spread = jnp.where(iota((8, LANES), 1) % 8 == iota((8, LANES), 0), 1.0, 0.0)
    wall = lax.dot(
        wall_ref[...].astype(jnp.float32), spread, preferred_element_type=jnp.float32
    )
    for target_ref, up in ((cross_1_ref, above[0]), (inner_1_ref, above[1])):
        target_ref[0:32, :] = jnp.where(up, slots_ref[3], slots_ref[1])
        target_ref[32:36, :] = geometry_ref[...]
        target_ref[36:38, :] = wall
        target_ref[38:40, :] = jnp.zeros((2, LANES), jnp.float32)
        target_ref[40:104, :] = jnp.where(up, top, bottom)
    for target_ref, up in ((cross_2_ref, above[2]), (inner_2_ref, above[3])):
        target_ref[...] = jnp.where(up, slots_ref[4], slots_ref[0])
    own_ref[...] = slots_ref[2]


def split_kernel(fields_ref, out_ref):
    for f in range(FIELDS):
        value = fields_ref[f]
        high = value.astype(jnp.bfloat16)
        out_ref[f, :, 0:LANES] = high
        out_ref[f, :, LANES : 2 * LANES] = (value - high.astype(jnp.float32)).astype(jnp.bfloat16)


def basis_rows(coordinate):
    gaps = [coordinate - float(NODES[i]) for i in range(8)]
    before = [None] * 8
    after = [None] * 8
    for i in range(1, 8):
        before[i] = gaps[i - 1] if i == 1 else before[i - 1] * gaps[i - 1]
    for i in range(6, -1, -1):
        after[i] = gaps[i + 1] if i == 6 else after[i + 1] * gaps[i + 1]
    out = []
    for i in range(8):
        if i == 0:
            value = after[0]
        elif i == 7:
            value = before[7]
        else:
            value = before[i] * after[i]
        out.append(value * float(BARY[i]))
    return out


def eval_kernel(*refs):
    sources, fields_ref, targets = refs[0:5], refs[5], refs[6:11]
    for source, target in zip(sources, targets):
        words = source[0:32, :]
        valid = jnp.where((iota((32, LANES), 0) % 4 == 3) & (words > 0.0), 1, 0)
        blocks = (jnp.sum(valid) + BLOCK - 1) // BLOCK

        def one_block(b, carry, source=source, target=target):
            start = pl.multiple_of(b * BLOCK, BLOCK)
            tiles = source[pl.ds(pl.multiple_of(b * 16, 16), 16), :]
            words = jnp.concatenate([tiles[4 * n : 4 * n + 4, :] for n in range(4)], axis=1)
            element = words[3:4, :].astype(jnp.int32) - 1
            hot = (iota((LANES, BLOCK), 0) == element).astype(jnp.float32).astype(jnp.bfloat16)
            hot = jnp.concatenate([hot, hot], axis=0)
            along = [basis_rows(words[d : d + 1, :]) for d in range(3)]
            row = iota((8, BLOCK), 0)
            wx = jnp.broadcast_to(along[0][0], (8, BLOCK))
            for i in range(1, 8):
                wx = jnp.where(row == i, along[0][i], wx)
            for f in range(FIELDS):
                picked = lax.dot(
                    fields_ref[f], hot, preferred_element_type=jnp.float32
                )
                over_k = picked[0:64, :] * along[2][0]
                for k in range(1, 8):
                    over_k = over_k + picked[64 * k : 64 * k + 64, :] * along[2][k]
                over_j = over_k[0:8, :] * along[1][0]
                for j in range(1, 8):
                    over_j = over_j + over_k[8 * j : 8 * j + 8, :] * along[1][j]
                target[f : f + 1, pl.ds(start, BLOCK)] = jnp.sum(
                    over_j * wx, axis=0, keepdims=True
                )
            return carry

        lax.fori_loop(0, blocks, one_block, 0)


def unpack_kernel(
    place_ref, cross_1_ref, inner_1_ref, cross_2_ref, inner_2_ref, own_ref, moves_ref, owner_ref,
    out_ref,
):
    q = place_ref[0]
    width = N_REC
    below_1, above_1, below_2, above_2 = by_side(
        q, cross_1_ref[...], inner_1_ref[...], cross_2_ref[...], inner_2_ref[...]
    )
    zeros = jnp.zeros((FIELDS, CAP), jnp.float32)
    values = [
        jnp.concatenate([value, zeros], axis=1)
        for value in (below_2, below_1, own_ref[...], above_1, above_2)
    ]
    moves = jnp.concatenate([moves_ref[...], jnp.zeros((8, CAP), jnp.int32)], axis=1)
    for b in range(10, -1, -1):
        step = 1 << b
        incoming = pltpu.roll(moves, step, 1)
        moved = (incoming >> b) & 1
        for s in range(5):
            flag = jnp.broadcast_to(moved[s : s + 1, :], (FIELDS, width))
            values[s] = jnp.where(flag == 1, pltpu.roll(values[s], step, 1), values[s])
        moves = jnp.where(moved == 1, incoming, jnp.where((moves >> b) & 1 == 1, 0, moves))
    distance = jnp.broadcast_to(owner_ref[...] - q + 2, (FIELDS, width))
    out = values[0]
    for s in range(1, 5):
        out = jnp.where(distance == s, values[s], out)
    out_ref[...] = out


def share_kernel(
    place_ref, cross_1_ref, inner_1_ref, cross_2_ref, inner_2_ref, own_ref, moves_ref, owner_ref,
    share_ref,
):
    q = place_ref[0]
    width = N_REC
    below_1, above_1, below_2, above_2 = by_side(
        q, *(ref[0:1, :] for ref in (cross_1_ref, inner_1_ref, cross_2_ref, inner_2_ref))
    )
    row = iota((8, CAP), 0)
    values = jnp.broadcast_to(below_2, (8, CAP))
    for s, value in ((1, below_1), (2, own_ref[0:1, :]), (3, above_1), (4, above_2)):
        values = jnp.where(row == s, value, values)
    values = jnp.concatenate([values, jnp.zeros((8, CAP), jnp.float32)], axis=1)
    moves = jnp.concatenate([moves_ref[...], jnp.zeros((8, CAP), jnp.int32)], axis=1)
    for b in range(10, -1, -1):
        step = 1 << b
        incoming = pltpu.roll(moves, step, 1)
        moved = (incoming >> b) & 1
        values = jnp.where(moved == 1, pltpu.roll(values, step, 1), values)
        moves = jnp.where(moved == 1, incoming, jnp.where((moves >> b) & 1 == 1, 0, moves))
    mine = iota((8, width), 0) == owner_ref[...] - q + 2
    out = jnp.sum(jnp.where(mine, values, 0.0), axis=0, keepdims=True)
    for n in range(16):
        share_ref[n : n + 1, :] = out[:, n * LANES : (n + 1) * LANES]


def prep_kernel(
    place_ref, geometry_ref, wall_ref, forcing_ref, cross_ref, inner_ref,
    inverse_ref, free_ref, load_ref, beside_ref, plane_ref, below_ref, above_ref,
):
    q = place_ref[0]
    below_ref[...], above_ref[...] = by_side(q, cross_ref[32:104, :], inner_ref[32:104, :])
    beside_ref[0:8, :] = below_ref[0:8, :]
    beside_ref[8:16, :] = above_ref[0:8, :]
    wcol = w_column()
    scol = s_column()

    def diagonal(geometry, k, j):
        wk, wj = float(WEIGHTS[k]), float(WEIGHTS[j])
        sk, sj = float(STIFF[k, k]), float(STIFF[j, j])
        return (
            geometry[0:1, :] * (scol * (wk * wj))
            + geometry[1:2, :] * (wcol * (wk * sj))
            + geometry[2:3, :] * (wcol * (sk * wj))
            + geometry[3:4, :] * (wcol * (wk * wj))
        )

    geometry = geometry_ref[...]
    below = below_ref[0:8, :]
    above = above_ref[0:8, :]
    lane = iota((8, LANES), 1)
    row = iota((8, LANES), 0)
    zero = jnp.zeros((8, LANES), jnp.float32)

    def wall_plane(low, high):
        for j in range(8):
            plane_ref[8 * j : 8 * j + 8, :] = zero
        plane_ref[0:8, :] = jnp.where(lane < 8, low, 0.0) + zero
        plane_ref[56:64, :] = jnp.where(lane >= 120, high, 0.0) + zero
        sum_xy(plane_ref, 1)
        return plane_ref[...]

    spread = jnp.where(lane % 8 == row, 1.0, 0.0)
    flags = lax.dot(
        wall_ref[...].astype(jnp.float32), spread, preferred_element_type=jnp.float32
    )
    wall = wall_plane(flags[0:1, :], flags[1:2, :])
    wall_below = wall_plane(below[4:5, :], below[5:6, :])
    wall_above = wall_plane(above[4:5, :], above[5:6, :])
    mark = jnp.where(
        ((row == 0) & (lane % 8 == 0)) | ((row == 7) & (lane % 8 == 7)), 1.0, 0.0
    )
    for j in range(8):
        plane_ref[8 * j : 8 * j + 8, :] = mark
    sum_xy(plane_ref, 1)
    rec = plane_ref[...]
    has_below = jnp.where(q > 0, 1.0, 0.0)
    has_above = jnp.where(q < N_DOM - 1, 1.0, 0.0)
    inner = 1.0 - jnp.minimum(rec + wall, 1.0)
    bottom = 1.0 - jnp.minimum(rec + rec * has_below + (wall + wall_below), 1.0)
    top = 1.0 - jnp.minimum(rec + rec * has_above + (wall + wall_above), 1.0)
    free_ref[0:64, :] = bottom
    free_ref[448:512, :] = top
    for k in range(1, 7):
        free_ref[64 * k : 64 * k + 64, :] = inner

    for k in range(8):
        for j in range(8):
            inverse_ref[(k * 8 + j) * 8 : (k * 8 + j) * 8 + 8, :] = diagonal(geometry, k, j)
    sum_xy(inverse_ref, 8)
    for j in range(8):
        plane_ref[8 * j : 8 * j + 8, :] = diagonal(below, 7, j)
    sum_xy(plane_ref, 1)
    inverse_ref[0:64, :] = inverse_ref[0:64, :] + plane_ref[...]
    for j in range(8):
        plane_ref[8 * j : 8 * j + 8, :] = diagonal(above, 0, j)
    sum_xy(plane_ref, 1)
    inverse_ref[448:512, :] = inverse_ref[448:512, :] + plane_ref[...]
    for k in range(8):
        at = slice(64 * k, 64 * k + 64)
        inverse_ref[at, :] = free_ref[at, :] / inverse_ref[at, :]

    for k in range(8):
        for j in range(8):
            at = slice((k * 8 + j) * 8, (k * 8 + j) * 8 + 8)
            load_ref[at, :] = forcing_ref[at, :] * (
                geometry[3:4, :] * (wcol * float(WEIGHTS[k] * WEIGHTS[j]))
            )
    sum_xy(load_ref, 8)
    for other_ref, k, base in ((below_ref, 7, 0), (above_ref, 0, 448)):
        for j in range(8):
            plane_ref[8 * j : 8 * j + 8, :] = other_ref[8 + 8 * j : 16 + 8 * j, :] * (
                other_ref[3:4, :] * (wcol * float(WEIGHTS[k] * WEIGHTS[j]))
            )
        sum_xy(plane_ref, 1)
        load_ref[base : base + 64, :] = load_ref[base : base + 64, :] + plane_ref[...]


def inverse_multiplicity(q):
    row = iota((64, LANES), 0)
    lane = iota((64, LANES), 1)
    i, j = row % 8, row // 8
    x, y = lane % 8, lane // 8
    along_x = ((i == 0) & (x > 0)) | ((i == 7) & (x < 7))
    along_y = ((j == 0) & (y > 0)) | ((j == 7) & (y < 15))
    inner = jnp.where(along_x, 0.5, 1.0) * jnp.where(along_y, 0.5, 1.0)
    return (
        inner,
        inner * jnp.where(q > 0, 0.5, 1.0),
        inner * jnp.where(q < N_DOM - 1, 0.5, 1.0),
    )


def krylov_step(q, w_ref, inverse_ref, geometry_ref, xmat_ref, v_ref, u_ref, at, moments):
    inner, bottom, top = inverse_multiplicity(q)
    norm = jnp.zeros((64, LANES), jnp.float32)
    for k in range(8):
        rows = slice(64 * k, 64 * k + 64)
        w = w_ref[rows, :]
        v = inverse_ref[rows, :] * w
        v_ref[rows, :] = v
        norm = norm + v * w * (bottom if k == 0 else top if k == 7 else inner)
    energy = apply_local(
        v_ref, geometry_ref[...], xmat_ref, u_ref, tuple(range(8)), dot_with_v=True
    )
    sum_xy(u_ref, 8)
    return moments + lane_value(jnp.sum(norm), at) + lane_value(jnp.sum(energy), at + 1)


def first_kernel(
    place_ref, own_ref, cross_in_ref, inner_in_ref, geometry_ref,
    beside_ref, inverse_ref, free_ref, load_ref, xmat_ref, w_ref, u_ref, edge_ref, lift_ref, moments_ref, cross_ref,
    inner_ref, v_ref, face_ref,
):
    q = place_ref[0]
    below, above = by_side(q, cross_in_ref[...], inner_in_ref[...])
    pick_row = iota((8, LANES), 0)
    pick_lane = iota((8, LANES), 1)
    picks = [
        [
            jnp.where(pick_lane == pick_row * 16 + (8 * odd + 7 * s), 1.0, 0.0)
            for odd in range(2)
        ]
        for s in range(2)
    ]

    def planes(values):
        out = []
        for s in range(2):
            halves = [
                lax.dot_general(
                    values[8 * s : 8 * s + 8, :], picks[s][odd], (((0,), (0,)), ((), ())),
                    precision=HIGHEST, preferred_element_type=jnp.float32,
                )
                for odd in range(2)
            ]
            plane = halves[0][0:64, :] + halves[1][64:128, :]
            out.append([plane[8 * k : 8 * k + 8, :] for k in range(8)])
        return out

    received = {off: planes(values) for off, values in ((-1, below), (0, own_ref[...]), (1, above))}
    lane = iota((8, LANES), 1)
    j_row = iota((8, LANES), 0)
    low = (j_row == 0) & (lane >= 8)
    high = (j_row == 7) & (lane < 120)

    def sum_y(value):
        down = jnp.broadcast_to(pltpu.roll(value, LANES - 8, 1)[0:1, :], (8, LANES))
        up = jnp.broadcast_to(pltpu.roll(value, 8, 1)[7:8, :], (8, LANES))
        return value + jnp.where(high, down, 0.0) + jnp.where(low, up, 0.0)

    count_y = jnp.where(low | high, 2.0, 1.0)
    on_side = [jnp.where(lane % 8 == x, 1.0, 0.0) for x in (0, 7)]

    def boundary(off):
        out = []
        has_below = jnp.where(q + off > 0, 1.0, 0.0)
        has_above = jnp.where(q + off < N_DOM - 1, 1.0, 0.0)
        for s in range(2):
            side = []
            for k in range(8):
                total = received[off][s][k]
                count = count_y * on_side[s]
                if k == 0:
                    if off >= 0:
                        total = total + received[off - 1][s][7]
                    count = count + count * has_below
                if k == 7:
                    if off <= 0:
                        total = total + received[off + 1][s][0]
                    count = count + count * has_above
                side.append(sum_y(total) / jnp.maximum(count, 1.0))
            out.append(jnp.concatenate(side, axis=0))
        return out

    zero = jnp.zeros((64, LANES), jnp.float32)
    for k in range(8):
        v_ref[64 * k : 64 * k + 64, :] = zero
    for off, geometry, plane in ((-1, beside_ref[0:4, :], 7), (1, beside_ref[8:12, :], 0)):
        sides = boundary(off)
        v_ref[pl.ds(0, 64, stride=8), :] = sides[0]
        v_ref[pl.ds(7, 64, stride=8), :] = sides[1]
        at = 0 if off < 0 else 64
        apply_local(v_ref, geometry, xmat_ref, face_ref.at[at : at + 64, :], (plane,))
        sum_xy(face_ref.at[at : at + 64, :], 1)
    sides = boundary(0)
    v_ref[pl.ds(0, 64, stride=8), :] = sides[0]
    v_ref[pl.ds(7, 64, stride=8), :] = sides[1]
    edge_ref[0:64, :] = sides[0]
    edge_ref[64:128, :] = sides[1]
    apply_local(v_ref, geometry_ref[...], xmat_ref, u_ref, tuple(range(8)))
    sum_xy(u_ref, 8)
    lift_ref[0:64, :] = u_ref[0:64, :]
    lift_ref[64:128, :] = u_ref[448:512, :]
    u_ref[0:64, :] = u_ref[0:64, :] + face_ref[0:64, :]
    u_ref[448:512, :] = u_ref[448:512, :] + face_ref[64:128, :]
    for k in range(8):
        rows = slice(64 * k, 64 * k + 64)
        w_ref[rows, :] = free_ref[rows, :] * (load_ref[rows, :] - u_ref[rows, :])
    moments_ref[...] = krylov_step(
        q, w_ref, inverse_ref, geometry_ref, xmat_ref, v_ref, u_ref, 0,
        jnp.zeros((1, LANES), jnp.float32),
    )
    send_faces(q, u_ref, cross_ref, inner_ref)
    up = from_above(q)[0]
    bottom, top = lift_ref[0:64, :], lift_ref[64:128, :]
    cross_ref[64:128, :] = jnp.where(up, top, bottom)
    inner_ref[64:128, :] = jnp.where(up, bottom, top)


def send_faces(q, u_ref, cross_ref, inner_ref):
    up = from_above(q)[0]
    bottom, top = u_ref[0:64, :], u_ref[448:512, :]
    cross_ref[0:64, :] = jnp.where(up, top, bottom)
    inner_ref[0:64, :] = jnp.where(up, bottom, top)


def next_kernel(
    at, place_ref, w_old_ref, u_old_ref, cross_in_ref, inner_in_ref, geometry_ref, inverse_ref,
    free_ref, xmat_ref, moments_old_ref, *refs,
):
    q = place_ref[0]
    if at == 2:
        load_ref, lift_ref, *refs = refs
    w_ref, u_ref, moments_ref, cross_ref, inner_ref, *refs = refs
    v_ref = refs[-1]
    below, above = by_side(q, cross_in_ref[...], inner_in_ref[...])
    for k in range(8):
        rows = slice(64 * k, 64 * k + 64)
        image = u_old_ref[rows, :]
        w_old = w_old_ref[rows, :]
        if k in (0, 7):
            other = below if k == 0 else above
            image = image + other[0:64, :]
            face = slice(0, 64) if k == 0 else slice(64, 128)
            if at == 2:
                w_old = free_ref[rows, :] * (
                    load_ref[rows, :] - (lift_ref[face, :] + other[64:128, :])
                )
                refs[0][face, :] = w_old
        w_ref[rows, :] = free_ref[rows, :] * image - w_old
    row = krylov_step(
        q, w_ref, inverse_ref, geometry_ref, xmat_ref, v_ref, u_ref, at, moments_old_ref[...]
    )
    moments_ref[...] = jnp.broadcast_to(row, moments_ref.shape)
    send_faces(q, u_ref, cross_ref, inner_ref)


def image_kernel(place_ref, u_ref, cross_in_ref, inner_in_ref, free_ref, image_ref):
    below, above = by_side(place_ref[0], cross_in_ref[...], inner_in_ref[...])
    image_ref[...] = free_ref[...] * u_ref[...]
    image_ref[0:64, :] = image_ref[0:64, :] + free_ref[0:64, :] * below
    image_ref[448:512, :] = image_ref[448:512, :] + free_ref[448:512, :] * above


def last_kernel(
    w0_ref, face_ref, w1_ref, w2_ref, image_ref, inverse_ref, edge_ref, moments_ref,
    velocity_ref, residual_ref,
):
    sums = jnp.sum(moments_ref[...], axis=0, keepdims=True)
    h0, a0, h2, a1, h4, a2 = [sums[:, m : m + 1] for m in range(6)]
    h1, h3 = a0 - h0, a1 - h2
    g00, g01, g02, g11, g12, g22 = a0, h2 + h1, h3 + h2, a1, h4 + h3, a2
    b0, b1, b2 = h0, h1, h2
    l10 = g01 / g00
    l20 = g02 / g00
    d1 = g11 - l10 * g01
    e12 = g12 - l10 * g02
    l21 = e12 / d1
    d2 = g22 - l20 * g02 - l21 * e12
    y1 = b1 - l10 * b0
    y2 = b2 - l20 * b0 - l21 * y1
    c2 = y2 / d2
    c1 = y1 / d1 - l21 * c2
    c0 = b0 / g00 - l10 * c1 - l20 * c2
    c0, c1, c2 = [jnp.broadcast_to(c, (64, LANES)) for c in (c0, c1, c2)]
    for k in range(8):
        rows = slice(64 * k, 64 * k + 64)
        w0, w1, w2 = w0_ref[rows, :], w1_ref[rows, :], w2_ref[rows, :]
        if k in (0, 7):
            w0 = face_ref[0:64, :] if k == 0 else face_ref[64:128, :]
        velocity_ref[rows, :] = inverse_ref[rows, :] * (c0 * w0 + c1 * w1 + c2 * w2)
        residual_ref[rows, :] = (
            w0 - c0 * (w1 + w0) - c1 * (w2 + w1) - c2 * image_ref[rows, :]
        )
    for s in range(2):
        rows = pl.ds(7 * s, 64, stride=8)
        velocity_ref[rows, :] = velocity_ref[rows, :] + edge_ref[64 * s : 64 * s + 64, :]


VMEM = pl.BlockSpec(memory_space=pltpu.VMEM)
SMEM = pl.BlockSpec(memory_space=pltpu.SMEM)


def call(kernel, operands, outs, scratch=(), flops=100_000, smem_first=True, mib=12):
    specs = [VMEM] * len(operands)
    if smem_first:
        specs[0] = SMEM
    out_shape = [jax.ShapeDtypeStruct(shape, dtype) for shape, dtype in outs]
    return pl.pallas_call(
        kernel,
        out_shape=out_shape,
        in_specs=specs,
        out_specs=[VMEM] * len(outs),
        scratch_shapes=[pltpu.VMEM(shape, dtype) for shape, dtype in scratch],
        cost_estimate=pl.CostEstimate(flops=flops, bytes_accessed=1_000_000, transcendentals=0),
        compiler_params=pltpu.CompilerParams(vmem_limit_bytes=mib * 1024 * 1024),
    )(*operands)


F32 = jnp.float32
FIELD = ((512, LANES), F32)


def to_all(value):
    return lax.all_to_all(value, "dom", 0, 0, tiled=True)


def to_neighbours(cross_1, inner_1, cross_2=None, inner_2=None):
    lists = ((cross_1, CROSS_1), (cross_2, CROSS_2), (inner_1, INNER_1), (inner_2, INNER_2))
    moved = []
    for value, pairs in lists:
        moved.append(None if value is None else lax.ppermute(value, "dom", pairs))
    return [moved[n] for n in (0, 2, 1, 3) if moved[n] is not None]


def body(donor_fields, interp_weights, donor_owner, donor_element, geometry, wall_flag, forcing):
    place = lax.axis_index("dom").astype(jnp.int32).reshape(1)
    xmat = jnp.asarray(x_matrix())
    donors = lax.ppermute(donor_fields, "mesh", [(0, 1), (1, 0)])
    owner = donor_owner.reshape(1, N_REC)
    element = donor_element.reshape(1, N_REC)
    asked = ((32, LANES), F32)
    with_head = ((CHUNK, LANES), F32)
    *requests, own, moves = call(
        route_kernel, (place, interp_weights, owner, element, geometry, wall_flag, forcing),
        (with_head, with_head, asked, asked, asked, ((8, CAP), jnp.int32)),
        scratch=(((5, 32, LANES), F32),), mib=60,
    )
    requests = to_neighbours(*requests)
    (fields,) = call(
        split_kernel, (donors,), (((FIELDS, 512, 256), jnp.bfloat16),), smem_first=False,
    )
    answers = call(
        eval_kernel, (*requests, own, fields), (((FIELDS, CAP), F32),) * 5,
        flops=7_000_000_000, smem_first=False, mib=24,
    )
    answered = to_neighbours(*answers[0:4])
    inverse, free, load, beside = call(
        prep_kernel, (place, geometry, wall_flag, forcing, requests[0], requests[1]),
        (FIELD, FIELD, FIELD, ((16, LANES), F32)),
        scratch=(((64, LANES), F32), ((72, LANES), F32), ((72, LANES), F32)),
    )
    unpacked = (place, *answered, answers[4], moves, owner)
    (share,) = call(share_kernel, unpacked, (((16, LANES), F32),))
    (interface,) = call(unpack_kernel, unpacked, (((FIELDS, N_REC), F32),))
    face = ((64, LANES), F32)
    two_faces = ((128, LANES), F32)
    w0, u, edge, lift, moments, *faces = call(
        first_kernel,
        (place, share, *to_neighbours(share, share), geometry, beside, inverse, free,
         load, xmat),
        (FIELD, FIELD, two_faces, two_faces, ((1, LANES), F32), two_faces, two_faces),
        scratch=(FIELD, two_faces),
    )
    fixed = (geometry, inverse, free, xmat)
    w1, u, moments, *faces, w0_faces = call(
        functools.partial(next_kernel, 2),
        (place, w0, u, *to_neighbours(*faces), *fixed, moments, load, lift),
        (FIELD, FIELD, ((1, LANES), F32), face, face, two_faces), scratch=(FIELD,),
    )
    w2, u, moments, *faces = call(
        functools.partial(next_kernel, 4),
        (place, w1, u, *to_neighbours(*faces), *fixed, moments),
        (FIELD, FIELD, ((N_DOM, LANES), F32), face, face), scratch=(FIELD,),
    )
    sums = to_all(moments)
    (image,) = call(image_kernel, (place, u, *to_neighbours(*faces), free), (FIELD,))
    velocity, residual = call(
        last_kernel, (w0, w0_faces, w1, w2, image, inverse, edge, sums), (FIELD, FIELD), smem_first=False,
    )
    return velocity, residual, interface


def solution(mesh):
    both = ("mesh", "dom")
    in_specs = (
        P(None, None, both), P(None, None, both), P(both, None), P(both), P(None, both),
        P(None, both), P(None, both),
    )
    out_specs = (P(None, both), P(None, both), P(None, both))

    return jax.shard_map(body, mesh=mesh, in_specs=in_specs, out_specs=out_specs, check_vma=False)
```

```python
import functools

import jax
import jax.numpy as jnp
import numpy as np
from jax import lax
from jax.experimental import pallas as pl
from jax.experimental.pallas import tpu as pltpu
from jax.sharding import PartitionSpec as P


HIGHEST = lax.Precision.HIGHEST
N_DOM = 64
N_REC = 2048
CAP = 1024
FIELDS = 5
BY_DOT = 3
LANES = 128
BLOCK = 512
CHUNK = 104


def both_ways(lows, distance):
    return [pair for q in lows for pair in ((q, q + distance), (q + distance, q))]


CROSS_1 = both_ways(range(1, N_DOM - 1, 2), 1)
INNER_1 = both_ways(range(0, N_DOM - 1, 2), 1)
CROSS_2 = both_ways([q for q in range(N_DOM - 2) if q % 4 >= 2], 2)
INNER_2 = both_ways([q for q in range(N_DOM - 2) if q % 4 < 2], 2)


def from_above(q):
    odd = q % 2 == 1
    late = q % 4 >= 2
    return odd, jnp.logical_not(odd), late, jnp.logical_not(late)


def legendre_pair(values, degree):
    previous = values * 0.0 + 1.0
    current = values * 1.0
    for order in range(2, degree + 1):
        previous, current = (
            current,
            ((2 * order - 1) * values * current - (order - 1) * previous) / order,
        )
    return current, previous


def gll_tables():
    degree = 7
    count = degree + 1
    nodes = np.cos(np.pi * np.arange(count) / degree)
    for _ in range(80):
        top, lower = legendre_pair(nodes, degree)
        nodes = nodes - (nodes * top - lower) / (count * top)
    nodes = np.sort(nodes)
    top, lower = legendre_pair(nodes, degree)
    weights = 2.0 / (degree * count * top * top)
    identity = np.eye(count)
    spacing = nodes[:, None] - nodes[None, :] + identity
    derivative = top[:, None] / (top[None, :] * spacing) * (1.0 - identity)
    derivative[0, 0] = -degree * count / 4.0
    derivative[degree, degree] = degree * count / 4.0
    return nodes, weights, derivative


NODES, WEIGHTS, DERIV = gll_tables()
STIFF = DERIV.T @ (WEIGHTS[:, None] * DERIV)
STIFF = 0.5 * (STIFF + STIFF.T)
BARY = np.array([1.0 / np.prod([NODES[i] - NODES[j] for j in range(8) if j != i]) for i in range(8)])


def x_matrix():
    full = np.kron(np.diag(WEIGHTS), STIFF).astype(np.float32)
    high = jnp.asarray(full).astype(jnp.bfloat16)
    low = (jnp.asarray(full) - high.astype(jnp.float32)).astype(jnp.bfloat16)
    return jnp.concatenate([high, high, low], axis=1)


def iota(shape, dim):
    return lax.broadcasted_iota(jnp.int32, shape, dim)


def w_column():
    row = iota((8, LANES), 0)
    out = jnp.full((8, LANES), float(WEIGHTS[0]), jnp.float32)
    for i in range(1, 8):
        out = jnp.where(row == i, float(WEIGHTS[i]), out)
    return out


def s_column():
    row = iota((8, LANES), 0)
    out = jnp.full((8, LANES), float(STIFF[0, 0]), jnp.float32)
    for i in range(1, 8):
        out = jnp.where(row == i, float(STIFF[i, i]), out)
    return out


def sum_xy(ref, planes):
    rows = planes * 8
    lane = iota((rows, LANES), 1)
    low = ref[pl.ds(0, rows, stride=8), :]
    high = ref[pl.ds(7, rows, stride=8), :]
    ref[pl.ds(7, rows, stride=8), :] = high + jnp.where(
        lane % 8 < 7, pltpu.roll(low, LANES - 1, 1), 0.0
    )
    ref[pl.ds(0, rows, stride=8), :] = low + jnp.where(lane % 8 > 0, pltpu.roll(high, 1, 1), 0.0)
    lane = iota((8, LANES), 1)
    for k in range(planes):
        low = ref[k * 64 : k * 64 + 8, :]
        high = ref[k * 64 + 56 : k * 64 + 64, :]
        ref[k * 64 + 56 : k * 64 + 64, :] = high + jnp.where(
            lane < 120, pltpu.roll(low, LANES - 8, 1), 0.0
        )
        ref[k * 64 : k * 64 + 8, :] = low + jnp.where(lane >= 8, pltpu.roll(high, 8, 1), 0.0)


def apply_local(v_ref, geometry, xmat_ref, out_ref, planes, dot_with_v=False):
    wcol = w_column()
    gx = geometry[0:1, :]
    gyw = geometry[1:2, :] * wcol
    gzw = geometry[2:3, :] * wcol
    gmw = geometry[3:4, :] * wcol
    total = jnp.zeros((8, LANES), jnp.float32)
    for at in range(0, len(planes), 2):
        pair = range(at, min(at + 2, len(planes)))
        value = [v_ref[planes[n] * 64 : planes[n] * 64 + 64, :] for n in pair]
        value = jnp.concatenate(value, axis=1) if len(value) > 1 else value[0]
        high = value.astype(jnp.bfloat16)
        low = (value - high.astype(jnp.float32)).astype(jnp.bfloat16)
        along_x = lax.dot(
            xmat_ref[...], jnp.concatenate([high, low, high], axis=0),
            preferred_element_type=jnp.float32,
        )
        for n in pair:
            out_ref[n * 64 : n * 64 + 64, :] = along_x[:, (n - at) * LANES : (n - at + 1) * LANES]
    for at, k in enumerate(planes):
        plane = [v_ref[(k * 8 + j) * 8 : (k * 8 + j) * 8 + 8, :] for j in range(8)]
        for j in range(8):
            ysum = plane[0] * float(STIFF[j, 0] * WEIGHTS[k])
            for jj in range(1, 8):
                ysum = ysum + plane[jj] * float(STIFF[j, jj] * WEIGHTS[k])
            zsum = None
            for kk in range(8):
                term = v_ref[(kk * 8 + j) * 8 : (kk * 8 + j) * 8 + 8, :] * float(
                    STIFF[k, kk] * WEIGHTS[j]
                )
                zsum = term if zsum is None else zsum + term
            row = (at * 8 + j) * 8
            value = (
                out_ref[row : row + 8, :] * (gx * float(WEIGHTS[k]))
                + gyw * ysum
                + gzw * zsum
                + gmw * (plane[j] * float(WEIGHTS[k] * WEIGHTS[j]))
            )
            out_ref[row : row + 8, :] = value
            if dot_with_v:
                total = total + value * plane[j]
    return total


def lane_value(value, at):
    return jnp.where(iota((1, LANES), 1) == at, value, 0.0)


def by_side(q, cross_1, inner_1, cross_2=None, inner_2=None):
    above = from_above(q)
    out = (jnp.where(above[0], inner_1, cross_1), jnp.where(above[0], cross_1, inner_1))
    if cross_2 is not None:
        out += (jnp.where(above[2], inner_2, cross_2), jnp.where(above[2], cross_2, inner_2))
    return out


def route_kernel(
    place_ref, weights_ref, owner_ref, element_ref, geometry_ref, wall_ref, forcing_ref,
    cross_1_ref, inner_1_ref, cross_2_ref, inner_2_ref, own_ref, moves_ref, slots_ref,
):
    q = place_ref[0]
    width = N_REC
    lane = iota((8, width), 1)
    row = iota((8, width), 0)
    distance = owner_ref[...] - q + 2
    mine = distance == row
    count = mine.astype(jnp.int32)
    step = 1
    while step < width:
        count = count + jnp.where(lane >= step, pltpu.roll(count, step, 1), 0)
        step *= 2
    moves = jnp.where(mine, lane - (count - 1), 0)
    totals = count[:, width - 1 : width]
    node_rows = iota((8, width), 0)
    node = jnp.full((8, width), float(NODES[0]), jnp.float32)
    for i in range(1, 8):
        node = jnp.where(node_rows == i, float(NODES[i]), node)
    coords = [jnp.sum(weights_ref[d] * node, axis=0, keepdims=True) for d in range(3)]
    words = element_ref[...].astype(jnp.float32) + 1.0
    base = jnp.where(row % 4 == 3, words, 0.0)
    for d in range(3):
        base = jnp.where(row % 4 == d, coords[d], base)
    packs = [base, base, base]
    for b in range(11):
        step = 1 << b
        incoming = pltpu.roll(moves, width - step, 1)
        moved = (incoming >> b) & 1
        for n in range(3):
            first = jnp.broadcast_to(moved[2 * n : 2 * n + 1, :], (8, width))
            if n < 2:
                second = jnp.broadcast_to(moved[2 * n + 1 : 2 * n + 2, :], (8, width))
                first = jnp.where(row < 4, first, second)
            packs[n] = jnp.where(first == 1, pltpu.roll(packs[n], width - step, 1), packs[n])
        moves = jnp.where(moved == 1, incoming, jnp.where((moves >> b) & 1 == 1, 0, moves))
    moves_ref[...] = moves[:, :CAP]
    lane = iota((4, CAP), 1)
    for s in range(5):
        at = (s % 2) * 4
        slot = jnp.where(lane < totals[s : s + 1, :], packs[s // 2][at : at + 4, :CAP], 0.0)
        for c in range(8):
            slots_ref[s, 4 * c : 4 * c + 4, :] = slot[:, c * LANES : (c + 1) * LANES]
    above = from_above(q)
    bottom, top = forcing_ref[0:64, :], forcing_ref[448:512, :]
    spread = jnp.where(iota((8, LANES), 1) % 8 == iota((8, LANES), 0), 1.0, 0.0)
    wall = lax.dot(
        wall_ref[...].astype(jnp.float32), spread, preferred_element_type=jnp.float32
    )
    for target_ref, up in ((cross_1_ref, above[0]), (inner_1_ref, above[1])):
        target_ref[0:32, :] = jnp.where(up, slots_ref[3], slots_ref[1])
        target_ref[32:36, :] = geometry_ref[...]
        target_ref[36:38, :] = wall
        target_ref[38:40, :] = jnp.zeros((2, LANES), jnp.float32)
        target_ref[40:104, :] = jnp.where(up, top, bottom)
    for target_ref, up in ((cross_2_ref, above[2]), (inner_2_ref, above[3])):
        target_ref[...] = jnp.where(up, slots_ref[4], slots_ref[0])
    own_ref[...] = slots_ref[2]


def split_kernel(fields_ref, out_ref):
    for f in range(BY_DOT):
        value = fields_ref[f]
        high = value.astype(jnp.bfloat16)
        out_ref[f, :, 0:LANES] = high
        out_ref[f, :, LANES : 2 * LANES] = (value - high.astype(jnp.float32)).astype(jnp.bfloat16)


def basis_rows(coordinate):
    gaps = [coordinate - float(NODES[i]) for i in range(8)]
    before = [None] * 8
    after = [None] * 8
    for i in range(1, 8):
        before[i] = gaps[i - 1] if i == 1 else before[i - 1] * gaps[i - 1]
    for i in range(6, -1, -1):
        after[i] = gaps[i + 1] if i == 6 else after[i + 1] * gaps[i + 1]
    out = []
    for i in range(8):
        if i == 0:
            value = after[0]
        elif i == 7:
            value = before[7]
        else:
            value = before[i] * after[i]
        out.append(value * float(BARY[i]))
    return out


def eval_kernel(*refs):
    fields_ref, donors_ref, *refs = refs
    half = len(refs) // 2
    for source, target in zip(refs[:half], refs[half:]):
        words = source[0:32, :]
        valid = jnp.where((iota((32, LANES), 0) % 4 == 3) & (words > 0.0), 1, 0)
        blocks = (jnp.sum(valid) + BLOCK - 1) // BLOCK

        def one_block(b, carry, source=source, target=target):
            start = pl.multiple_of(b * BLOCK, BLOCK)
            tiles = source[pl.ds(pl.multiple_of(b * 16, 16), 16), :]
            words = jnp.concatenate([tiles[4 * n : 4 * n + 4, :] for n in range(4)], axis=1)
            element = words[3:4, :].astype(jnp.int32) - 1
            hot_rows = iota((LANES, BLOCK), 0)
            hot = (hot_rows == element).astype(jnp.float32).astype(jnp.bfloat16)
            hot = jnp.concatenate([hot, hot], axis=0)
            element = jnp.maximum(element, 0)
            along = [basis_rows(words[d : d + 1, :]) for d in range(3)]
            row = iota((8, BLOCK), 0)
            wx = jnp.broadcast_to(along[0][0], (8, BLOCK))
            for i in range(1, 8):
                wx = jnp.where(row == i, along[0][i], wx)

            def by_gather(f, h):
                part = slice(h * LANES, h * LANES + LANES)
                index = jnp.broadcast_to(element[:, part], (8, LANES))
                wz = [jnp.broadcast_to(w[:, part], (8, LANES)) for w in along[2]]
                over_j = None
                for j in range(8):
                    over_k = None
                    for k in range(8):
                        row = 64 * k + 8 * j
                        term = wz[k] * jnp.take_along_axis(
                            donors_ref[f, row : row + 8, :], index, axis=1,
                            mode="promise_in_bounds",
                        )
                        over_k = term if over_k is None else over_k + term
                    term = over_k * along[1][j][:, part]
                    over_j = term if over_j is None else over_j + term
                target[f : f + 1, pl.ds(start + h * LANES, LANES)] = jnp.sum(
                    over_j * wx[:, part], axis=0, keepdims=True
                )

            gathers = [(f, h) for f in range(BY_DOT, FIELDS) for h in range(BLOCK // LANES)]
            for f in range(BY_DOT):
                picked = lax.dot(fields_ref[f], hot, preferred_element_type=jnp.float32)
                share = -(-len(gathers) // (BY_DOT - f))
                for work in gathers[:share]:
                    by_gather(*work)
                gathers = gathers[share:]
                over_k = picked[0:64, :] * along[2][0]
                for k in range(1, 8):
                    over_k = over_k + picked[64 * k : 64 * k + 64, :] * along[2][k]
                over_j = over_k[0:8, :] * along[1][0]
                for j in range(1, 8):
                    over_j = over_j + over_k[8 * j : 8 * j + 8, :] * along[1][j]
                target[f : f + 1, pl.ds(start, BLOCK)] = jnp.sum(
                    over_j * wx, axis=0, keepdims=True
                )
            return carry

        lax.fori_loop(0, blocks, one_block, 0)


def unpack_kernel(
    place_ref, cross_1_ref, inner_1_ref, cross_2_ref, inner_2_ref, own_ref, moves_ref, owner_ref,
    out_ref,
):
    q = place_ref[0]
    width = N_REC
    below_1, above_1, below_2, above_2 = by_side(
        q, cross_1_ref[...], inner_1_ref[...], cross_2_ref[...], inner_2_ref[...]
    )
    zeros = jnp.zeros((FIELDS, CAP), jnp.float32)
    values = [
        jnp.concatenate([value, zeros], axis=1)
        for value in (below_2, below_1, own_ref[...], above_1, above_2)
    ]
    moves = jnp.concatenate([moves_ref[...], jnp.zeros((8, CAP), jnp.int32)], axis=1)
    for b in range(10, -1, -1):
        step = 1 << b
        incoming = pltpu.roll(moves, step, 1)
        moved = (incoming >> b) & 1
        for s in range(5):
            flag = jnp.broadcast_to(moved[s : s + 1, :], (FIELDS, width))
            values[s] = jnp.where(flag == 1, pltpu.roll(values[s], step, 1), values[s])
        moves = jnp.where(moved == 1, incoming, jnp.where((moves >> b) & 1 == 1, 0, moves))
    distance = jnp.broadcast_to(owner_ref[...] - q + 2, (FIELDS, width))
    out = values[0]
    for s in range(1, 5):
        out = jnp.where(distance == s, values[s], out)
    out_ref[...] = out


def share_kernel(
    place_ref, cross_1_ref, inner_1_ref, cross_2_ref, inner_2_ref, own_ref, moves_ref, owner_ref,
    share_ref,
):
    q = place_ref[0]
    width = N_REC
    below_1, above_1, below_2, above_2 = by_side(
        q, *(ref[0:1, :] for ref in (cross_1_ref, inner_1_ref, cross_2_ref, inner_2_ref))
    )
    row = iota((8, CAP), 0)
    values = jnp.broadcast_to(below_2, (8, CAP))
    for s, value in ((1, below_1), (2, own_ref[0:1, :]), (3, above_1), (4, above_2)):
        values = jnp.where(row == s, value, values)
    values = jnp.concatenate([values, jnp.zeros((8, CAP), jnp.float32)], axis=1)
    moves = jnp.concatenate([moves_ref[...], jnp.zeros((8, CAP), jnp.int32)], axis=1)
    for b in range(10, -1, -1):
        step = 1 << b
        incoming = pltpu.roll(moves, step, 1)
        moved = (incoming >> b) & 1
        values = jnp.where(moved == 1, pltpu.roll(values, step, 1), values)
        moves = jnp.where(moved == 1, incoming, jnp.where((moves >> b) & 1 == 1, 0, moves))
    mine = iota((8, width), 0) == owner_ref[...] - q + 2
    out = jnp.sum(jnp.where(mine, values, 0.0), axis=0, keepdims=True)
    for n in range(16):
        share_ref[n : n + 1, :] = out[:, n * LANES : (n + 1) * LANES]


def prep_kernel(
    place_ref, geometry_ref, wall_ref, forcing_ref, cross_ref, inner_ref,
    inverse_ref, free_ref, load_ref, beside_ref, plane_ref, below_ref, above_ref,
):
    q = place_ref[0]
    below_ref[...], above_ref[...] = by_side(q, cross_ref[32:104, :], inner_ref[32:104, :])
    beside_ref[0:8, :] = below_ref[0:8, :]
    beside_ref[8:16, :] = above_ref[0:8, :]
    wcol = w_column()
    scol = s_column()

    def diagonal(geometry, k, j):
        wk, wj = float(WEIGHTS[k]), float(WEIGHTS[j])
        sk, sj = float(STIFF[k, k]), float(STIFF[j, j])
        return (
            geometry[0:1, :] * (scol * (wk * wj))
            + geometry[1:2, :] * (wcol * (wk * sj))
            + geometry[2:3, :] * (wcol * (sk * wj))
            + geometry[3:4, :] * (wcol * (wk * wj))
        )

    geometry = geometry_ref[...]
    below = below_ref[0:8, :]
    above = above_ref[0:8, :]
    lane = iota((8, LANES), 1)
    row = iota((8, LANES), 0)
    zero = jnp.zeros((8, LANES), jnp.float32)

    def wall_plane(low, high):
        for j in range(8):
            plane_ref[8 * j : 8 * j + 8, :] = zero
        plane_ref[0:8, :] = jnp.where(lane < 8, low, 0.0) + zero
        plane_ref[56:64, :] = jnp.where(lane >= 120, high, 0.0) + zero
        sum_xy(plane_ref, 1)
        return plane_ref[...]

    spread = jnp.where(lane % 8 == row, 1.0, 0.0)
    flags = lax.dot(
        wall_ref[...].astype(jnp.float32), spread, preferred_element_type=jnp.float32
    )
    wall = wall_plane(flags[0:1, :], flags[1:2, :])
    wall_below = wall_plane(below[4:5, :], below[5:6, :])
    wall_above = wall_plane(above[4:5, :], above[5:6, :])
    mark = jnp.where(
        ((row == 0) & (lane % 8 == 0)) | ((row == 7) & (lane % 8 == 7)), 1.0, 0.0
    )
    for j in range(8):
        plane_ref[8 * j : 8 * j + 8, :] = mark
    sum_xy(plane_ref, 1)
    rec = plane_ref[...]
    has_below = jnp.where(q > 0, 1.0, 0.0)
    has_above = jnp.where(q < N_DOM - 1, 1.0, 0.0)
    inner = 1.0 - jnp.minimum(rec + wall, 1.0)
    bottom = 1.0 - jnp.minimum(rec + rec * has_below + (wall + wall_below), 1.0)
    top = 1.0 - jnp.minimum(rec + rec * has_above + (wall + wall_above), 1.0)
    free_ref[0:64, :] = bottom
    free_ref[448:512, :] = top
    for k in range(1, 7):
        free_ref[64 * k : 64 * k + 64, :] = inner

    for k in range(8):
        for j in range(8):
            inverse_ref[(k * 8 + j) * 8 : (k * 8 + j) * 8 + 8, :] = diagonal(geometry, k, j)
    sum_xy(inverse_ref, 8)
    for j in range(8):
        plane_ref[8 * j : 8 * j + 8, :] = diagonal(below, 7, j)
    sum_xy(plane_ref, 1)
    inverse_ref[0:64, :] = inverse_ref[0:64, :] + plane_ref[...]
    for j in range(8):
        plane_ref[8 * j : 8 * j + 8, :] = diagonal(above, 0, j)
    sum_xy(plane_ref, 1)
    inverse_ref[448:512, :] = inverse_ref[448:512, :] + plane_ref[...]
    for k in range(8):
        at = slice(64 * k, 64 * k + 64)
        inverse_ref[at, :] = free_ref[at, :] / inverse_ref[at, :]

    for k in range(8):
        for j in range(8):
            at = slice((k * 8 + j) * 8, (k * 8 + j) * 8 + 8)
            load_ref[at, :] = forcing_ref[at, :] * (
                geometry[3:4, :] * (wcol * float(WEIGHTS[k] * WEIGHTS[j]))
            )
    sum_xy(load_ref, 8)
    for other_ref, k, base in ((below_ref, 7, 0), (above_ref, 0, 448)):
        for j in range(8):
            plane_ref[8 * j : 8 * j + 8, :] = other_ref[8 + 8 * j : 16 + 8 * j, :] * (
                other_ref[3:4, :] * (wcol * float(WEIGHTS[k] * WEIGHTS[j]))
            )
        sum_xy(plane_ref, 1)
        load_ref[base : base + 64, :] = load_ref[base : base + 64, :] + plane_ref[...]


def inverse_multiplicity(q):
    row = iota((64, LANES), 0)
    lane = iota((64, LANES), 1)
    i, j = row % 8, row // 8
    x, y = lane % 8, lane // 8
    along_x = ((i == 0) & (x > 0)) | ((i == 7) & (x < 7))
    along_y = ((j == 0) & (y > 0)) | ((j == 7) & (y < 15))
    inner = jnp.where(along_x, 0.5, 1.0) * jnp.where(along_y, 0.5, 1.0)
    return (
        inner,
        inner * jnp.where(q > 0, 0.5, 1.0),
        inner * jnp.where(q < N_DOM - 1, 0.5, 1.0),
    )


def krylov_step(q, w_ref, inverse_ref, geometry_ref, xmat_ref, v_ref, u_ref, at, moments):
    inner, bottom, top = inverse_multiplicity(q)
    norm = jnp.zeros((64, LANES), jnp.float32)
    for k in range(8):
        rows = slice(64 * k, 64 * k + 64)
        w = w_ref[rows, :]
        v = inverse_ref[rows, :] * w
        v_ref[rows, :] = v
        norm = norm + v * w * (bottom if k == 0 else top if k == 7 else inner)
    energy = apply_local(
        v_ref, geometry_ref[...], xmat_ref, u_ref, tuple(range(8)), dot_with_v=True
    )
    sum_xy(u_ref, 8)
    return moments + lane_value(jnp.sum(norm), at) + lane_value(jnp.sum(energy), at + 1)


def first_kernel(
    place_ref, own_ref, cross_in_ref, inner_in_ref, geometry_ref,
    beside_ref, inverse_ref, free_ref, load_ref, xmat_ref, w_ref, u_ref, edge_ref, lift_ref, moments_ref, cross_ref,
    inner_ref, v_ref, face_ref,
):
    q = place_ref[0]
    below, above = by_side(q, cross_in_ref[...], inner_in_ref[...])
    pick_row = iota((8, LANES), 0)
    pick_lane = iota((8, LANES), 1)
    picks = [
        [
            jnp.where(pick_lane == pick_row * 16 + (8 * odd + 7 * s), 1.0, 0.0)
            for odd in range(2)
        ]
        for s in range(2)
    ]

    layers = (below, own_ref[...], above)
    received = {off: [] for off in range(-1, 2)}
    for s in range(2):
        values = jnp.concatenate([layer[8 * s : 8 * s + 8, :] for layer in layers], axis=1)
        halves = [
            lax.dot_general(
                values, picks[s][odd], (((0,), (0,)), ((), ())),
                precision=HIGHEST, preferred_element_type=jnp.float32,
            )
            for odd in range(2)
        ]
        for n in range(3):
            at = n * LANES
            plane = halves[0][at : at + 64, :] + halves[1][at + 64 : at + 128, :]
            received[n - 1].append([plane[8 * k : 8 * k + 8, :] for k in range(8)])
    lane = iota((8, LANES), 1)
    j_row = iota((8, LANES), 0)
    low = (j_row == 0) & (lane >= 8)
    high = (j_row == 7) & (lane < 120)

    def sum_y(value):
        down = jnp.broadcast_to(pltpu.roll(value, LANES - 8, 1)[0:1, :], (8, LANES))
        up = jnp.broadcast_to(pltpu.roll(value, 8, 1)[7:8, :], (8, LANES))
        return value + jnp.where(high, down, 0.0) + jnp.where(low, up, 0.0)

    count_y = jnp.where(low | high, 2.0, 1.0)
    on_side = [jnp.where(lane % 8 == x, 1.0, 0.0) for x in (0, 7)]

    def boundary(off):
        out = []
        has_below = jnp.where(q + off > 0, 1.0, 0.0)
        has_above = jnp.where(q + off < N_DOM - 1, 1.0, 0.0)
        for s in range(2):
            side = []
            for k in range(8):
                total = received[off][s][k]
                count = count_y * on_side[s]
                if k == 0:
                    if off >= 0:
                        total = total + received[off - 1][s][7]
                    count = count + count * has_below
                if k == 7:
                    if off <= 0:
                        total = total + received[off + 1][s][0]
                    count = count + count * has_above
                side.append(sum_y(total) / jnp.maximum(count, 1.0))
            out.append(jnp.concatenate(side, axis=0))
        return out

    zero = jnp.zeros((64, LANES), jnp.float32)
    for k in range(8):
        v_ref[64 * k : 64 * k + 64, :] = zero
    for off, geometry, plane in ((-1, beside_ref[0:4, :], 7), (1, beside_ref[8:12, :], 0)):
        sides = boundary(off)
        v_ref[pl.ds(0, 64, stride=8), :] = sides[0]
        v_ref[pl.ds(7, 64, stride=8), :] = sides[1]
        at = 0 if off < 0 else 64
        apply_local(v_ref, geometry, xmat_ref, face_ref.at[at : at + 64, :], (plane,))
        sum_xy(face_ref.at[at : at + 64, :], 1)
    sides = boundary(0)
    v_ref[pl.ds(0, 64, stride=8), :] = sides[0]
    v_ref[pl.ds(7, 64, stride=8), :] = sides[1]
    edge_ref[0:64, :] = sides[0]
    edge_ref[64:128, :] = sides[1]
    apply_local(v_ref, geometry_ref[...], xmat_ref, u_ref, tuple(range(8)))
    sum_xy(u_ref, 8)
    lift_ref[0:64, :] = u_ref[0:64, :]
    lift_ref[64:128, :] = u_ref[448:512, :]
    u_ref[0:64, :] = u_ref[0:64, :] + face_ref[0:64, :]
    u_ref[448:512, :] = u_ref[448:512, :] + face_ref[64:128, :]
    for k in range(8):
        rows = slice(64 * k, 64 * k + 64)
        w_ref[rows, :] = free_ref[rows, :] * (load_ref[rows, :] - u_ref[rows, :])
    moments_ref[...] = krylov_step(
        q, w_ref, inverse_ref, geometry_ref, xmat_ref, v_ref, u_ref, 0,
        jnp.zeros((1, LANES), jnp.float32),
    )
    send_faces(q, u_ref, cross_ref, inner_ref)
    up = from_above(q)[0]
    bottom, top = lift_ref[0:64, :], lift_ref[64:128, :]
    cross_ref[64:128, :] = jnp.where(up, top, bottom)
    inner_ref[64:128, :] = jnp.where(up, bottom, top)


def send_faces(q, u_ref, cross_ref, inner_ref):
    up = from_above(q)[0]
    bottom, top = u_ref[0:64, :], u_ref[448:512, :]
    cross_ref[0:64, :] = jnp.where(up, top, bottom)
    inner_ref[0:64, :] = jnp.where(up, bottom, top)


def next_kernel(
    at, place_ref, w_old_ref, u_old_ref, cross_in_ref, inner_in_ref, geometry_ref, inverse_ref,
    free_ref, xmat_ref, moments_old_ref, *refs,
):
    q = place_ref[0]
    if at == 2:
        load_ref, lift_ref, *refs = refs
    w_ref, u_ref, moments_ref, cross_ref, inner_ref, *refs = refs
    v_ref = refs[-1]
    below, above = by_side(q, cross_in_ref[...], inner_in_ref[...])
    for k in range(8):
        rows = slice(64 * k, 64 * k + 64)
        image = u_old_ref[rows, :]
        w_old = w_old_ref[rows, :]
        if k in (0, 7):
            other = below if k == 0 else above
            image = image + other[0:64, :]
            face = slice(0, 64) if k == 0 else slice(64, 128)
            if at == 2:
                w_old = free_ref[rows, :] * (
                    load_ref[rows, :] - (lift_ref[face, :] + other[64:128, :])
                )
                refs[0][face, :] = w_old
        w_ref[rows, :] = free_ref[rows, :] * image - w_old
    row = krylov_step(
        q, w_ref, inverse_ref, geometry_ref, xmat_ref, v_ref, u_ref, at, moments_old_ref[...]
    )
    moments_ref[...] = jnp.broadcast_to(row, moments_ref.shape)
    send_faces(q, u_ref, cross_ref, inner_ref)


def image_kernel(place_ref, u_ref, cross_in_ref, inner_in_ref, free_ref, image_ref):
    below, above = by_side(place_ref[0], cross_in_ref[...], inner_in_ref[...])
    image_ref[...] = free_ref[...] * u_ref[...]
    image_ref[0:64, :] = image_ref[0:64, :] + free_ref[0:64, :] * below
    image_ref[448:512, :] = image_ref[448:512, :] + free_ref[448:512, :] * above


def last_kernel(
    w0_ref, face_ref, w1_ref, w2_ref, image_ref, inverse_ref, edge_ref, moments_ref,
    velocity_ref, residual_ref,
):
    sums = jnp.sum(moments_ref[...], axis=0, keepdims=True)
    h0, a0, h2, a1, h4, a2 = [sums[:, m : m + 1] for m in range(6)]
    h1, h3 = a0 - h0, a1 - h2
    g00, g01, g02, g11, g12, g22 = a0, h2 + h1, h3 + h2, a1, h4 + h3, a2
    b0, b1, b2 = h0, h1, h2
    l10 = g01 / g00
    l20 = g02 / g00
    d1 = g11 - l10 * g01
    e12 = g12 - l10 * g02
    l21 = e12 / d1
    d2 = g22 - l20 * g02 - l21 * e12
    y1 = b1 - l10 * b0
    y2 = b2 - l20 * b0 - l21 * y1
    c2 = y2 / d2
    c1 = y1 / d1 - l21 * c2
    c0 = b0 / g00 - l10 * c1 - l20 * c2
    c0, c1, c2 = [jnp.broadcast_to(c, (64, LANES)) for c in (c0, c1, c2)]
    for k in range(8):
        rows = slice(64 * k, 64 * k + 64)
        w0, w1, w2 = w0_ref[rows, :], w1_ref[rows, :], w2_ref[rows, :]
        if k in (0, 7):
            w0 = face_ref[0:64, :] if k == 0 else face_ref[64:128, :]
        velocity_ref[rows, :] = inverse_ref[rows, :] * (c0 * w0 + c1 * w1 + c2 * w2)
        residual_ref[rows, :] = (
            w0 - c0 * (w1 + w0) - c1 * (w2 + w1) - c2 * image_ref[rows, :]
        )
    for s in range(2):
        rows = pl.ds(7 * s, 64, stride=8)
        velocity_ref[rows, :] = velocity_ref[rows, :] + edge_ref[64 * s : 64 * s + 64, :]


VMEM = pl.BlockSpec(memory_space=pltpu.VMEM)
SMEM = pl.BlockSpec(memory_space=pltpu.SMEM)


def call(kernel, operands, outs, scratch=(), flops=100_000, smem_first=True, mib=12):
    specs = [VMEM] * len(operands)
    if smem_first:
        specs[0] = SMEM
    out_shape = [jax.ShapeDtypeStruct(shape, dtype) for shape, dtype in outs]
    return pl.pallas_call(
        kernel,
        out_shape=out_shape,
        in_specs=specs,
        out_specs=[VMEM] * len(outs),
        scratch_shapes=[pltpu.VMEM(shape, dtype) for shape, dtype in scratch],
        cost_estimate=pl.CostEstimate(flops=flops, bytes_accessed=1_000_000, transcendentals=0),
        compiler_params=pltpu.CompilerParams(vmem_limit_bytes=mib * 1024 * 1024),
    )(*operands)


F32 = jnp.float32
FIELD = ((512, LANES), F32)


def to_all(value):
    return lax.all_to_all(value, "dom", 0, 0, tiled=True)


def to_neighbours(cross_1, inner_1, cross_2=None, inner_2=None):
    lists = ((cross_1, CROSS_1), (cross_2, CROSS_2), (inner_1, INNER_1), (inner_2, INNER_2))
    moved = []
    for value, pairs in lists:
        moved.append(None if value is None else lax.ppermute(value, "dom", pairs))
    return [moved[n] for n in (0, 2, 1, 3) if moved[n] is not None]


def body(donor_fields, interp_weights, donor_owner, donor_element, geometry, wall_flag, forcing):
    place = lax.axis_index("dom").astype(jnp.int32).reshape(1)
    xmat = x_matrix()
    donors = lax.ppermute(donor_fields, "mesh", [(0, 1), (1, 0)])
    owner = donor_owner.reshape(1, N_REC)
    element = donor_element.reshape(1, N_REC)
    asked = ((32, LANES), F32)
    with_head = ((CHUNK, LANES), F32)
    *requests, own, moves = call(
        route_kernel,
        (
            place,
            *(
                pltpu.with_memory_space_constraint(value, pltpu.HBM)
                for value in (interp_weights, owner, element, geometry, wall_flag, forcing)
            ),
        ),
        (with_head, with_head, asked, asked, asked, ((8, CAP), jnp.int32)),
        scratch=(((5, 32, LANES), F32),),
    )
    requests = to_neighbours(*requests)
    (fields,) = call(
        split_kernel, (donors,), (((BY_DOT, 512, 256), jnp.bfloat16),), smem_first=False,
    )
    answer = ((FIELDS, CAP), F32)
    own_answer, inner_1 = call(
        eval_kernel, (fields, donors, own, requests[1]), (answer,) * 2,
        flops=3_000_000_000, smem_first=False, mib=24,
    )
    cross_1, cross_2, inner_2 = call(
        eval_kernel, (fields, donors, requests[0], requests[2], requests[3]), (answer,) * 3,
        flops=4_000_000_000, smem_first=False, mib=24,
    )
    answered = to_neighbours(cross_1, inner_1, cross_2, inner_2)
    inverse, free, load, beside = call(
        prep_kernel, (place, geometry, wall_flag, forcing, requests[0], requests[1]),
        (FIELD, FIELD, FIELD, ((16, LANES), F32)),
        scratch=(((64, LANES), F32), ((72, LANES), F32), ((72, LANES), F32)),
    )
    unpacked = (place, *answered, own_answer, moves, owner)
    (share,) = call(share_kernel, unpacked, (((16, LANES), F32),))
    (interface,) = call(unpack_kernel, unpacked, (((FIELDS, N_REC), F32),))
    face = ((64, LANES), F32)
    two_faces = ((128, LANES), F32)
    w0, u, edge, lift, moments, *faces = call(
        first_kernel,
        (place, share, *to_neighbours(share, share), geometry, beside, inverse, free,
         load, xmat),
        (FIELD, FIELD, two_faces, two_faces, ((1, LANES), F32), two_faces, two_faces),
        scratch=(FIELD, two_faces),
    )
    fixed = (geometry, inverse, free, xmat)
    w1, u, moments, *faces, w0_faces = call(
        functools.partial(next_kernel, 2),
        (place, w0, u, *to_neighbours(*faces), *fixed, moments, load, lift),
        (FIELD, FIELD, ((1, LANES), F32), face, face, two_faces), scratch=(FIELD,),
    )
    w2, u, moments, *faces = call(
        functools.partial(next_kernel, 4),
        (place, w1, u, *to_neighbours(*faces), *fixed, moments),
        (FIELD, FIELD, ((N_DOM, LANES), F32), face, face), scratch=(FIELD,),
    )
    sums = to_all(moments)
    (image,) = call(image_kernel, (place, u, *to_neighbours(*faces), free), (FIELD,))
    velocity, residual = call(
        last_kernel, (w0, w0_faces, w1, w2, image, inverse, edge, sums), (FIELD, FIELD), smem_first=False,
    )
    return velocity, residual, interface


def solution(mesh):
    both = ("mesh", "dom")
    in_specs = (
        P(None, None, both), P(None, None, both), P(both, None), P(both), P(None, both),
        P(None, both), P(None, both),
    )
    out_specs = (P(None, both), P(None, both), P(None, both))

    return jax.shard_map(body, mesh=mesh, in_specs=in_specs, out_specs=out_specs, check_vma=False)
```

```python
import functools

import jax
import jax.numpy as jnp
import numpy as np
from jax import lax
from jax.experimental import pallas as pl
from jax.experimental.pallas import tpu as pltpu
from jax.sharding import PartitionSpec as P


N_DOM = 64
N_REC = 2048
CAP = 1024
FIELDS = 5
BY_DOT = 3
LANES = 128
BLOCK = 512
HALF = 256


def both_ways(lows, distance):
    return [pair for q in lows for pair in ((q, q + distance), (q + distance, q))]


CROSS_1 = both_ways(range(1, N_DOM - 1, 2), 1)
INNER_1 = both_ways(range(0, N_DOM - 1, 2), 1)
MIDDLE_1 = both_ways([q for q in range(N_DOM - 1) if q % 4 == 1], 1)
SHIFTED = [[(4 * g + 2 + t) % N_DOM for t in range(4)] for g in range(16)]
INNER_2 = both_ways([q for q in range(N_DOM - 2) if q % 4 < 2], 2)


def pick_sides(q, inner_1, middle, inner_2, far):
    r = q % 4
    p = (q + 2) % 4

    def across(off):
        return far(jnp.clip(p + off, 0, 3))

    return (
        jnp.where(r < 2, across(-2), inner_2),
        jnp.where(r == 0, across(-1), jnp.where(r == 2, middle, inner_1)),
        jnp.where(r == 3, across(1), jnp.where(r == 1, middle, inner_1)),
        jnp.where(r >= 2, across(2), inner_2),
    )


def legendre_pair(values, degree):
    previous = values * 0.0 + 1.0
    current = values * 1.0
    for order in range(2, degree + 1):
        previous, current = (
            current,
            ((2 * order - 1) * values * current - (order - 1) * previous) / order,
        )
    return current, previous


def gll_tables():
    degree = 7
    count = degree + 1
    nodes = np.cos(np.pi * np.arange(count) / degree)
    for _ in range(80):
        top, lower = legendre_pair(nodes, degree)
        nodes = nodes - (nodes * top - lower) / (count * top)
    nodes = np.sort(nodes)
    top, lower = legendre_pair(nodes, degree)
    weights = 2.0 / (degree * count * top * top)
    identity = np.eye(count)
    spacing = nodes[:, None] - nodes[None, :] + identity
    derivative = top[:, None] / (top[None, :] * spacing) * (1.0 - identity)
    derivative[0, 0] = -degree * count / 4.0
    derivative[degree, degree] = degree * count / 4.0
    return nodes, weights, derivative


NODES, WEIGHTS, DERIV = gll_tables()
STIFF = DERIV.T @ (WEIGHTS[:, None] * DERIV)
STIFF = 0.5 * (STIFF + STIFF.T)
BARY = np.array([1.0 / np.prod([NODES[i] - NODES[j] for j in range(8) if j != i]) for i in range(8)])


def x_matrix():
    full = np.kron(np.diag(WEIGHTS), STIFF).astype(np.float32)
    high = jnp.asarray(full).astype(jnp.bfloat16)
    low = (jnp.asarray(full) - high.astype(jnp.float32)).astype(jnp.bfloat16)
    return jnp.concatenate([high, high, low], axis=1)


def iota(shape, dim):
    return lax.broadcasted_iota(jnp.int32, shape, dim)


def w_column():
    row = iota((8, LANES), 0)
    out = jnp.full((8, LANES), float(WEIGHTS[0]), jnp.float32)
    for i in range(1, 8):
        out = jnp.where(row == i, float(WEIGHTS[i]), out)
    return out


def s_column():
    row = iota((8, LANES), 0)
    out = jnp.full((8, LANES), float(STIFF[0, 0]), jnp.float32)
    for i in range(1, 8):
        out = jnp.where(row == i, float(STIFF[i, i]), out)
    return out


def sum_xy(ref, planes):
    rows = planes * 8
    lane = iota((rows, LANES), 1)
    low = ref[pl.ds(0, rows, stride=8), :]
    high = ref[pl.ds(7, rows, stride=8), :]
    ref[pl.ds(7, rows, stride=8), :] = high + jnp.where(
        lane % 8 < 7, pltpu.roll(low, LANES - 1, 1), 0.0
    )
    ref[pl.ds(0, rows, stride=8), :] = low + jnp.where(lane % 8 > 0, pltpu.roll(high, 1, 1), 0.0)
    lane = iota((8, LANES), 1)
    for k in range(planes):
        low = ref[k * 64 : k * 64 + 8, :]
        high = ref[k * 64 + 56 : k * 64 + 64, :]
        ref[k * 64 + 56 : k * 64 + 64, :] = high + jnp.where(
            lane < 120, pltpu.roll(low, LANES - 8, 1), 0.0
        )
        ref[k * 64 : k * 64 + 8, :] = low + jnp.where(lane >= 8, pltpu.roll(high, 8, 1), 0.0)


def apply_local(v_ref, geometry, xmat_ref, out_ref, planes, dot_with_v=False):
    wcol = w_column()
    gx = geometry[0:1, :]
    gyw = geometry[1:2, :] * wcol
    gzw = geometry[2:3, :] * wcol
    gmw = geometry[3:4, :] * wcol
    total = jnp.zeros((8, LANES), jnp.float32)
    for at in range(0, len(planes), 2):
        pair = range(at, min(at + 2, len(planes)))
        value = [v_ref[planes[n] * 64 : planes[n] * 64 + 64, :] for n in pair]
        value = jnp.concatenate(value, axis=1) if len(value) > 1 else value[0]
        high = value.astype(jnp.bfloat16)
        low = (value - high.astype(jnp.float32)).astype(jnp.bfloat16)
        along_x = lax.dot(
            xmat_ref[...], jnp.concatenate([high, low, high], axis=0),
            preferred_element_type=jnp.float32,
        )
        for n in pair:
            out_ref[n * 64 : n * 64 + 64, :] = along_x[:, (n - at) * LANES : (n - at + 1) * LANES]
    for at, k in enumerate(planes):
        plane = [v_ref[(k * 8 + j) * 8 : (k * 8 + j) * 8 + 8, :] for j in range(8)]
        for j in range(8):
            ysum = plane[0] * float(STIFF[j, 0] * WEIGHTS[k])
            for jj in range(1, 8):
                ysum = ysum + plane[jj] * float(STIFF[j, jj] * WEIGHTS[k])
            zsum = None
            for kk in range(8):
                term = v_ref[(kk * 8 + j) * 8 : (kk * 8 + j) * 8 + 8, :] * float(
                    STIFF[k, kk] * WEIGHTS[j]
                )
                zsum = term if zsum is None else zsum + term
            row = (at * 8 + j) * 8
            value = (
                out_ref[row : row + 8, :] * (gx * float(WEIGHTS[k]))
                + gyw * ysum
                + gzw * zsum
                + gmw * (plane[j] * float(WEIGHTS[k] * WEIGHTS[j]))
            )
            out_ref[row : row + 8, :] = value
            if dot_with_v:
                total = total + value * plane[j]
    return total


def lane_value(value, at):
    return jnp.where(iota((1, LANES), 1) == at, value, 0.0)


def by_side(q, cross, inner):
    odd = q % 2 == 1
    return jnp.where(odd, inner, cross), jnp.where(odd, cross, inner)


def route_kernel(
    place_ref, weights_ref, owner_ref, element_ref, inner_1_ref, middle_ref, inner_2_ref,
    far_ref, own_ref, moves_ref, slots_ref,
):
    q = place_ref[0]
    width = N_REC
    lane = iota((8, width), 1)
    row = iota((8, width), 0)
    distance = owner_ref[...] - q + 2
    mine = distance == row
    count = mine.astype(jnp.int32)
    step = 1
    while step < width:
        count = count + jnp.where(lane >= step, pltpu.roll(count, step, 1), 0)
        step *= 2
    moves = jnp.where(mine, lane - (count - 1), 0)
    totals = count[:, width - 1 : width]
    node_rows = iota((8, width), 0)
    node = jnp.full((8, width), float(NODES[0]), jnp.float32)
    for i in range(1, 8):
        node = jnp.where(node_rows == i, float(NODES[i]), node)
    coords = [jnp.sum(weights_ref[d] * node, axis=0, keepdims=True) for d in range(3)]
    words = element_ref[...].astype(jnp.float32) + 1.0
    base = jnp.where(row % 4 == 3, words, 0.0)
    for d in range(3):
        base = jnp.where(row % 4 == d, coords[d], base)
    packs = [base, base, base]
    for b in range(11):
        step = 1 << b
        incoming = pltpu.roll(moves, width - step, 1)
        moved = (incoming >> b) & 1
        for n in range(3):
            first = jnp.broadcast_to(moved[2 * n : 2 * n + 1, :], (8, width))
            if n < 2:
                second = jnp.broadcast_to(moved[2 * n + 1 : 2 * n + 2, :], (8, width))
                first = jnp.where(row < 4, first, second)
            packs[n] = jnp.where(first == 1, pltpu.roll(packs[n], width - step, 1), packs[n])
        moves = jnp.where(moved == 1, incoming, jnp.where((moves >> b) & 1 == 1, 0, moves))
    moves_ref[...] = moves[:, :CAP]
    lane = iota((4, CAP), 1)
    for s in range(5):
        at = (s % 2) * 4
        slot = jnp.where(lane < totals[s : s + 1, :], packs[s // 2][at : at + 4, :CAP], 0.0)
        for c in range(8):
            slots_ref[s, 4 * c : 4 * c + 4, :] = slot[:, c * LANES : (c + 1) * LANES]
    slots_ref[5] = jnp.zeros((32, LANES), jnp.float32)
    r = q % 4
    p = (q + 2) % 4
    inner_1_ref[...] = slots_ref[jnp.where(q % 2 == 0, 3, 1)]
    middle_ref[...] = slots_ref[jnp.where(r == 1, 3, 1)]
    inner_2_ref[...] = slots_ref[jnp.where(r < 2, 4, 0)]
    for t in range(4):
        off = t - p
        inside = (r + off >= 0) & (r + off <= 3)
        beyond = (off < -2) | (off > 2)
        far_ref[t] = slots_ref[jnp.where(inside | beyond, 5, off + 2)]
    own_ref[...] = slots_ref[2]


def heads_kernel(place_ref, geometry_ref, wall_ref, forcing_ref, cross_ref, inner_ref):
    odd = place_ref[0] % 2 == 1
    spread = jnp.where(iota((8, LANES), 1) % 8 == iota((8, LANES), 0), 1.0, 0.0)
    wall = lax.dot(
        wall_ref[...].astype(jnp.float32), spread, preferred_element_type=jnp.float32
    )
    bottom, top = forcing_ref[0:64, :], forcing_ref[448:512, :]
    for target_ref, up in ((cross_ref, odd), (inner_ref, jnp.logical_not(odd))):
        target_ref[0:4, :] = geometry_ref[...]
        target_ref[4:6, :] = wall
        target_ref[6:8, :] = jnp.zeros((2, LANES), jnp.float32)
        target_ref[8:72, :] = jnp.where(up, top, bottom)


def split_kernel(fields_ref, out_ref):
    for f in range(BY_DOT):
        value = fields_ref[f]
        high = value.astype(jnp.bfloat16)
        out_ref[f, :, 0:LANES] = high
        out_ref[f, :, LANES : 2 * LANES] = (value - high.astype(jnp.float32)).astype(jnp.bfloat16)


def basis_rows(coordinate):
    gaps = [coordinate - float(NODES[i]) for i in range(8)]
    before = [None] * 8
    after = [None] * 8
    for i in range(1, 8):
        before[i] = gaps[i - 1] if i == 1 else before[i - 1] * gaps[i - 1]
    for i in range(6, -1, -1):
        after[i] = gaps[i + 1] if i == 6 else after[i + 1] * gaps[i + 1]
    out = []
    for i in range(8):
        if i == 0:
            value = after[0]
        elif i == 7:
            value = before[7]
        else:
            value = before[i] * after[i]
        out.append(value * float(BARY[i]))
    return out


def eval_kernel(*refs):
    fields_ref, donors_ref, *refs = refs
    half = len(refs) // 2
    pairs = []
    for source, target in zip(refs[:half], refs[half:]):
        if len(source.shape) == 2:
            pairs.append((source, target))
        else:
            pairs += [(source.at[t], target.at[t]) for t in range(source.shape[0])]
    for source, target in pairs:
        words = source[0:32, :]
        valid = jnp.where((iota((32, LANES), 0) % 4 == 3) & (words > 0.0), 1, 0)
        count = jnp.sum(valid)
        blocks = (count + HALF - 1) // BLOCK
        left = (count - blocks * BLOCK + BLOCK - 1) // BLOCK

        def one_block(b, first, size, source=source, target=target):
            start = pl.multiple_of(b * size + first, HALF)
            rows = size // 32
            tiles = source[pl.ds(pl.multiple_of(b * rows + first // 32, 8), rows), :]
            words = jnp.concatenate(
                [tiles[4 * n : 4 * n + 4, :] for n in range(rows // 4)], axis=1
            )
            element = words[3:4, :].astype(jnp.int32) - 1
            hot_rows = iota((LANES, size), 0)
            hot = (hot_rows == element).astype(jnp.float32).astype(jnp.bfloat16)
            hot = jnp.concatenate([hot, hot], axis=0)
            element = jnp.maximum(element, 0)
            along = [basis_rows(words[d : d + 1, :]) for d in range(3)]
            row = iota((8, size), 0)
            wx = jnp.broadcast_to(along[0][0], (8, size))
            for i in range(1, 8):
                wx = jnp.where(row == i, along[0][i], wx)

            def by_gather(f, h):
                part = slice(h * LANES, h * LANES + LANES)
                index = jnp.broadcast_to(element[:, part], (8, LANES))
                wz = [jnp.broadcast_to(w[:, part], (8, LANES)) for w in along[2]]
                over_j = None
                for j in range(8):
                    over_k = None
                    for k in range(8):
                        row = 64 * k + 8 * j
                        term = wz[k] * jnp.take_along_axis(
                            donors_ref[f, row : row + 8, :], index, axis=1,
                            mode="promise_in_bounds",
                        )
                        over_k = term if over_k is None else over_k + term
                    term = over_k * along[1][j][:, part]
                    over_j = term if over_j is None else over_j + term
                target[f : f + 1, pl.ds(start + h * LANES, LANES)] = jnp.sum(
                    over_j * wx[:, part], axis=0, keepdims=True
                )

            gathers = [(f, h) for f in range(BY_DOT, FIELDS) for h in range(size // LANES)]
            for f in range(BY_DOT):
                picked = lax.dot(fields_ref[f], hot, preferred_element_type=jnp.float32)
                share = -(-len(gathers) // (BY_DOT - f))
                for work in gathers[:share]:
                    by_gather(*work)
                gathers = gathers[share:]
                over_k = picked[0:64, :] * along[2][0]
                for k in range(1, 8):
                    over_k = over_k + picked[64 * k : 64 * k + 64, :] * along[2][k]
                over_j = over_k[0:8, :] * along[1][0]
                for j in range(1, 8):
                    over_j = over_j + over_k[8 * j : 8 * j + 8, :] * along[1][j]
                target[f : f + 1, pl.ds(start, size)] = jnp.sum(
                    over_j * wx, axis=0, keepdims=True
                )

        def whole(b, carry, one_block=one_block):
            one_block(b, 0, BLOCK)
            return carry

        def part(b, carry, one_block=one_block, first=blocks * BLOCK):
            one_block(b, first, HALF)
            return carry

        lax.fori_loop(0, blocks, whole, 0)
        lax.fori_loop(0, left, part, 0)


def unpack_kernel(
    place_ref, inner_1_ref, middle_ref, inner_2_ref, far_ref, own_ref, moves_ref, owner_ref,
    out_ref,
):
    q = place_ref[0]
    width = N_REC
    below_2, below_1, above_1, above_2 = pick_sides(
        q, inner_1_ref[...], middle_ref[...], inner_2_ref[...], lambda t: far_ref[t]
    )
    zeros = jnp.zeros((FIELDS, CAP), jnp.float32)
    values = [
        jnp.concatenate([value, zeros], axis=1)
        for value in (below_2, below_1, own_ref[...], above_1, above_2)
    ]
    moves = jnp.concatenate([moves_ref[...], jnp.zeros((8, CAP), jnp.int32)], axis=1)
    for b in range(10, -1, -1):
        step = 1 << b
        incoming = pltpu.roll(moves, step, 1)
        moved = (incoming >> b) & 1
        for s in range(5):
            flag = jnp.broadcast_to(moved[s : s + 1, :], (FIELDS, width))
            values[s] = jnp.where(flag == 1, pltpu.roll(values[s], step, 1), values[s])
        moves = jnp.where(moved == 1, incoming, jnp.where((moves >> b) & 1 == 1, 0, moves))
    distance = jnp.broadcast_to(owner_ref[...] - q + 2, (FIELDS, width))
    out = values[0]
    for s in range(1, 5):
        out = jnp.where(distance == s, values[s], out)
    out_ref[...] = out


def share_kernel(
    place_ref, inner_1_ref, middle_ref, inner_2_ref, far_ref, own_ref, moves_ref, owner_ref,
    cross_head_ref, inner_head_ref, share_ref, cross_ref, inner_ref,
):
    q = place_ref[0]
    width = N_REC
    below_2, below_1, above_1, above_2 = pick_sides(
        q, inner_1_ref[0:1, :], middle_ref[0:1, :], inner_2_ref[0:1, :],
        lambda t: far_ref[t, 0:1, :],
    )
    row = iota((8, CAP), 0)
    values = jnp.broadcast_to(below_2, (8, CAP))
    for s, value in ((1, below_1), (2, own_ref[0:1, :]), (3, above_1), (4, above_2)):
        values = jnp.where(row == s, value, values)
    values = jnp.concatenate([values, jnp.zeros((8, CAP), jnp.float32)], axis=1)
    moves = jnp.concatenate([moves_ref[...], jnp.zeros((8, CAP), jnp.int32)], axis=1)
    for b in range(10, -1, -1):
        step = 1 << b
        incoming = pltpu.roll(moves, step, 1)
        moved = (incoming >> b) & 1
        values = jnp.where(moved == 1, pltpu.roll(values, step, 1), values)
        moves = jnp.where(moved == 1, incoming, jnp.where((moves >> b) & 1 == 1, 0, moves))
    mine = iota((8, width), 0) == owner_ref[...] - q + 2
    out = jnp.sum(jnp.where(mine, values, 0.0), axis=0, keepdims=True)
    for n in range(16):
        share_ref[n : n + 1, :] = out[:, n * LANES : (n + 1) * LANES]
    for target_ref, head_ref in ((cross_ref, cross_head_ref), (inner_ref, inner_head_ref)):
        target_ref[0:16, :] = share_ref[...]
        target_ref[16:88, :] = head_ref[...]


def prep_kernel(
    place_ref, geometry_ref, wall_ref, forcing_ref, cross_ref, inner_ref,
    inverse_ref, free_ref, load_ref, beside_ref, plane_ref, below_ref, above_ref,
):
    q = place_ref[0]
    below_ref[...], above_ref[...] = by_side(q, cross_ref[16:88, :], inner_ref[16:88, :])
    beside_ref[0:8, :] = below_ref[0:8, :]
    beside_ref[8:16, :] = above_ref[0:8, :]
    wcol = w_column()
    scol = s_column()

    def diagonal(geometry, k, j):
        wk, wj = float(WEIGHTS[k]), float(WEIGHTS[j])
        sk, sj = float(STIFF[k, k]), float(STIFF[j, j])
        return (
            geometry[0:1, :] * (scol * (wk * wj))
            + geometry[1:2, :] * (wcol * (wk * sj))
            + geometry[2:3, :] * (wcol * (sk * wj))
            + geometry[3:4, :] * (wcol * (wk * wj))
        )

    geometry = geometry_ref[...]
    below = below_ref[0:8, :]
    above = above_ref[0:8, :]
    lane = iota((8, LANES), 1)
    row = iota((8, LANES), 0)
    zero = jnp.zeros((8, LANES), jnp.float32)

    def wall_plane(low, high):
        for j in range(8):
            plane_ref[8 * j : 8 * j + 8, :] = zero
        plane_ref[0:8, :] = jnp.where(lane < 8, low, 0.0) + zero
        plane_ref[56:64, :] = jnp.where(lane >= 120, high, 0.0) + zero
        sum_xy(plane_ref, 1)
        return plane_ref[...]

    spread = jnp.where(lane % 8 == row, 1.0, 0.0)
    flags = lax.dot(
        wall_ref[...].astype(jnp.float32), spread, preferred_element_type=jnp.float32
    )
    wall = wall_plane(flags[0:1, :], flags[1:2, :])
    wall_below = wall_plane(below[4:5, :], below[5:6, :])
    wall_above = wall_plane(above[4:5, :], above[5:6, :])
    mark = jnp.where(
        ((row == 0) & (lane % 8 == 0)) | ((row == 7) & (lane % 8 == 7)), 1.0, 0.0
    )
    for j in range(8):
        plane_ref[8 * j : 8 * j + 8, :] = mark
    sum_xy(plane_ref, 1)
    rec = plane_ref[...]
    has_below = jnp.where(q > 0, 1.0, 0.0)
    has_above = jnp.where(q < N_DOM - 1, 1.0, 0.0)
    inner = 1.0 - jnp.minimum(rec + wall, 1.0)
    bottom = 1.0 - jnp.minimum(rec + rec * has_below + (wall + wall_below), 1.0)
    top = 1.0 - jnp.minimum(rec + rec * has_above + (wall + wall_above), 1.0)
    free_ref[0:64, :] = bottom
    free_ref[448:512, :] = top
    for k in range(1, 7):
        free_ref[64 * k : 64 * k + 64, :] = inner

    for k in range(8):
        for j in range(8):
            inverse_ref[(k * 8 + j) * 8 : (k * 8 + j) * 8 + 8, :] = diagonal(geometry, k, j)
    sum_xy(inverse_ref, 8)
    for j in range(8):
        plane_ref[8 * j : 8 * j + 8, :] = diagonal(below, 7, j)
    sum_xy(plane_ref, 1)
    inverse_ref[0:64, :] = inverse_ref[0:64, :] + plane_ref[...]
    for j in range(8):
        plane_ref[8 * j : 8 * j + 8, :] = diagonal(above, 0, j)
    sum_xy(plane_ref, 1)
    inverse_ref[448:512, :] = inverse_ref[448:512, :] + plane_ref[...]
    for k in range(8):
        at = slice(64 * k, 64 * k + 64)
        inverse_ref[at, :] = free_ref[at, :] / inverse_ref[at, :]

    for k in range(8):
        for j in range(8):
            at = slice((k * 8 + j) * 8, (k * 8 + j) * 8 + 8)
            load_ref[at, :] = forcing_ref[at, :] * (
                geometry[3:4, :] * (wcol * float(WEIGHTS[k] * WEIGHTS[j]))
            )
    sum_xy(load_ref, 8)
    for other_ref, k, base in ((below_ref, 7, 0), (above_ref, 0, 448)):
        for j in range(8):
            plane_ref[8 * j : 8 * j + 8, :] = other_ref[8 + 8 * j : 16 + 8 * j, :] * (
                other_ref[3:4, :] * (wcol * float(WEIGHTS[k] * WEIGHTS[j]))
            )
        sum_xy(plane_ref, 1)
        load_ref[base : base + 64, :] = load_ref[base : base + 64, :] + plane_ref[...]


def inverse_multiplicity(q):
    row = iota((64, LANES), 0)
    lane = iota((64, LANES), 1)
    i, j = row % 8, row // 8
    x, y = lane % 8, lane // 8
    along_x = ((i == 0) & (x > 0)) | ((i == 7) & (x < 7))
    along_y = ((j == 0) & (y > 0)) | ((j == 7) & (y < 15))
    inner = jnp.where(along_x, 0.5, 1.0) * jnp.where(along_y, 0.5, 1.0)
    return (
        inner,
        inner * jnp.where(q > 0, 0.5, 1.0),
        inner * jnp.where(q < N_DOM - 1, 0.5, 1.0),
    )


def krylov_step(q, w_ref, inverse_ref, geometry_ref, xmat_ref, v_ref, u_ref, at, moments):
    inner, bottom, top = inverse_multiplicity(q)
    norm = jnp.zeros((64, LANES), jnp.float32)
    for k in range(8):
        rows = slice(64 * k, 64 * k + 64)
        w = w_ref[rows, :]
        v = inverse_ref[rows, :] * w
        v_ref[rows, :] = v
        norm = norm + v * w * (bottom if k == 0 else top if k == 7 else inner)
    energy = apply_local(
        v_ref, geometry_ref[...], xmat_ref, u_ref, tuple(range(8)), dot_with_v=True
    )
    sum_xy(u_ref, 8)
    return moments + lane_value(jnp.sum(norm), at) + lane_value(jnp.sum(energy), at + 1)


def first_kernel(
    place_ref, own_ref, cross_in_ref, inner_in_ref, geometry_ref,
    beside_ref, inverse_ref, free_ref, load_ref, xmat_ref, w_ref, u_ref, edge_ref, lift_ref, moments_ref, cross_ref,
    inner_ref, v_ref, face_ref,
):
    q = place_ref[0]
    below, above = by_side(q, cross_in_ref[0:16, :], inner_in_ref[0:16, :])
    pick_row = iota((32, 2 * LANES), 0)
    pick_lane = iota((32, 2 * LANES), 1)
    odd = pick_lane // LANES
    picks = [
        jnp.where(
            (pick_lane % LANES == pick_row % 8 * 16 + (8 * odd + 7 * s)) & (pick_row < 24), 1.0, 0.0
        ).astype(jnp.bfloat16)
        for s in range(2)
    ]

    def bf16_parts(value):
        parts = []
        for _ in range(3):
            part = value.astype(jnp.bfloat16)
            parts.append(part.astype(jnp.float32))
            value = value - parts[-1]
        return jnp.concatenate([*parts, jnp.zeros_like(value)], axis=0).astype(jnp.bfloat16)

    layers = (below, own_ref[...], above)
    received = {off: [] for off in range(-1, 2)}
    for s in range(2):
        values = jnp.concatenate([layer[8 * s : 8 * s + 8, :] for layer in layers], axis=1)
        spread = lax.dot_general(
            bf16_parts(values), picks[s], (((0,), (0,)), ((), ())),
            preferred_element_type=jnp.float32,
        )
        for n in range(3):
            at = n * LANES
            plane = spread[at : at + 64, :LANES] + spread[at + 64 : at + 128, LANES:]
            received[n - 1].append([plane[8 * k : 8 * k + 8, :] for k in range(8)])
    lane = iota((8, LANES), 1)
    j_row = iota((8, LANES), 0)
    low = (j_row == 0) & (lane >= 8)
    high = (j_row == 7) & (lane < 120)

    def sum_y(value):
        down = jnp.broadcast_to(pltpu.roll(value, LANES - 8, 1)[0:1, :], (8, LANES))
        up = jnp.broadcast_to(pltpu.roll(value, 8, 1)[7:8, :], (8, LANES))
        return value + jnp.where(high, down, 0.0) + jnp.where(low, up, 0.0)

    count_y = jnp.where(low | high, 2.0, 1.0)
    on_side = [jnp.where(lane % 8 == x, 1.0, 0.0) for x in (0, 7)]

    def boundary(off):
        out = []
        has_below = jnp.where(q + off > 0, 1.0, 0.0)
        has_above = jnp.where(q + off < N_DOM - 1, 1.0, 0.0)
        for s in range(2):
            side = []
            for k in range(8):
                total = received[off][s][k]
                count = count_y * on_side[s]
                if k == 0:
                    if off >= 0:
                        total = total + received[off - 1][s][7]
                    count = count + count * has_below
                if k == 7:
                    if off <= 0:
                        total = total + received[off + 1][s][0]
                    count = count + count * has_above
                side.append(sum_y(total) / jnp.maximum(count, 1.0))
            out.append(jnp.concatenate(side, axis=0))
        return out

    zero = jnp.zeros((64, LANES), jnp.float32)
    for k in range(8):
        v_ref[64 * k : 64 * k + 64, :] = zero
    for off, geometry, plane in ((-1, beside_ref[0:4, :], 7), (1, beside_ref[8:12, :], 0)):
        sides = boundary(off)
        v_ref[pl.ds(0, 64, stride=8), :] = sides[0]
        v_ref[pl.ds(7, 64, stride=8), :] = sides[1]
        at = 0 if off < 0 else 64
        apply_local(v_ref, geometry, xmat_ref, face_ref.at[at : at + 64, :], (plane,))
        sum_xy(face_ref.at[at : at + 64, :], 1)
    sides = boundary(0)
    v_ref[pl.ds(0, 64, stride=8), :] = sides[0]
    v_ref[pl.ds(7, 64, stride=8), :] = sides[1]
    edge_ref[0:64, :] = sides[0]
    edge_ref[64:128, :] = sides[1]
    apply_local(v_ref, geometry_ref[...], xmat_ref, u_ref, tuple(range(8)))
    sum_xy(u_ref, 8)
    lift_ref[0:64, :] = u_ref[0:64, :]
    lift_ref[64:128, :] = u_ref[448:512, :]
    u_ref[0:64, :] = u_ref[0:64, :] + face_ref[0:64, :]
    u_ref[448:512, :] = u_ref[448:512, :] + face_ref[64:128, :]
    for k in range(8):
        rows = slice(64 * k, 64 * k + 64)
        w_ref[rows, :] = free_ref[rows, :] * (load_ref[rows, :] - u_ref[rows, :])
    moments_ref[...] = krylov_step(
        q, w_ref, inverse_ref, geometry_ref, xmat_ref, v_ref, u_ref, 0,
        jnp.zeros((1, LANES), jnp.float32),
    )
    send_faces(q, u_ref, cross_ref, inner_ref)
    up = q % 2 == 1
    bottom, top = lift_ref[0:64, :], lift_ref[64:128, :]
    cross_ref[64:128, :] = jnp.where(up, top, bottom)
    inner_ref[64:128, :] = jnp.where(up, bottom, top)


def send_faces(q, u_ref, cross_ref, inner_ref):
    up = q % 2 == 1
    bottom, top = u_ref[0:64, :], u_ref[448:512, :]
    cross_ref[0:64, :] = jnp.where(up, top, bottom)
    inner_ref[0:64, :] = jnp.where(up, bottom, top)


def next_kernel(
    at, place_ref, w_old_ref, u_old_ref, cross_in_ref, inner_in_ref, geometry_ref, inverse_ref,
    free_ref, xmat_ref, moments_old_ref, *refs,
):
    q = place_ref[0]
    if at == 2:
        load_ref, lift_ref, *refs = refs
    w_ref, u_ref, moments_ref, cross_ref, inner_ref, *refs = refs
    v_ref = refs[-1]
    below, above = by_side(q, cross_in_ref[...], inner_in_ref[...])
    for k in range(8):
        rows = slice(64 * k, 64 * k + 64)
        image = u_old_ref[rows, :]
        w_old = w_old_ref[rows, :]
        if k in (0, 7):
            other = below if k == 0 else above
            image = image + other[0:64, :]
            face = slice(0, 64) if k == 0 else slice(64, 128)
            if at == 2:
                w_old = free_ref[rows, :] * (
                    load_ref[rows, :] - (lift_ref[face, :] + other[64:128, :])
                )
                refs[0][face, :] = w_old
        w_ref[rows, :] = free_ref[rows, :] * image - w_old
    row = krylov_step(
        q, w_ref, inverse_ref, geometry_ref, xmat_ref, v_ref, u_ref, at, moments_old_ref[...]
    )
    moments_ref[...] = jnp.broadcast_to(row, moments_ref.shape)
    send_faces(q, u_ref, cross_ref, inner_ref)


def image_kernel(place_ref, u_ref, cross_in_ref, inner_in_ref, free_ref, image_ref):
    below, above = by_side(place_ref[0], cross_in_ref[...], inner_in_ref[...])
    image_ref[...] = free_ref[...] * u_ref[...]
    image_ref[0:64, :] = image_ref[0:64, :] + free_ref[0:64, :] * below
    image_ref[448:512, :] = image_ref[448:512, :] + free_ref[448:512, :] * above


def last_kernel(
    w0_ref, face_ref, w1_ref, w2_ref, image_ref, inverse_ref, edge_ref, moments_ref,
    velocity_ref, residual_ref,
):
    sums = jnp.sum(moments_ref[...], axis=0, keepdims=True)
    h0, a0, h2, a1, h4, a2 = [sums[:, m : m + 1] for m in range(6)]
    h1, h3 = a0 - h0, a1 - h2
    g00, g01, g02, g11, g12, g22 = a0, h2 + h1, h3 + h2, a1, h4 + h3, a2
    b0, b1, b2 = h0, h1, h2
    l10 = g01 / g00
    l20 = g02 / g00
    d1 = g11 - l10 * g01
    e12 = g12 - l10 * g02
    l21 = e12 / d1
    d2 = g22 - l20 * g02 - l21 * e12
    y1 = b1 - l10 * b0
    y2 = b2 - l20 * b0 - l21 * y1
    c2 = y2 / d2
    c1 = y1 / d1 - l21 * c2
    c0 = b0 / g00 - l10 * c1 - l20 * c2
    c0, c1, c2 = [jnp.broadcast_to(c, (64, LANES)) for c in (c0, c1, c2)]
    for k in range(8):
        rows = slice(64 * k, 64 * k + 64)
        w0, w1, w2 = w0_ref[rows, :], w1_ref[rows, :], w2_ref[rows, :]
        if k in (0, 7):
            w0 = face_ref[0:64, :] if k == 0 else face_ref[64:128, :]
        velocity_ref[rows, :] = inverse_ref[rows, :] * (c0 * w0 + c1 * w1 + c2 * w2)
        residual_ref[rows, :] = (
            w0 - c0 * (w1 + w0) - c1 * (w2 + w1) - c2 * image_ref[rows, :]
        )
    for s in range(2):
        rows = pl.ds(7 * s, 64, stride=8)
        velocity_ref[rows, :] = velocity_ref[rows, :] + edge_ref[64 * s : 64 * s + 64, :]


VMEM = pl.BlockSpec(memory_space=pltpu.VMEM)
SMEM = pl.BlockSpec(memory_space=pltpu.SMEM)


def call(kernel, operands, outs, scratch=(), flops=100_000, smem_first=True, mib=12):
    specs = [VMEM] * len(operands)
    if smem_first:
        specs[0] = SMEM
    out_shape = [jax.ShapeDtypeStruct(shape, dtype) for shape, dtype in outs]
    return pl.pallas_call(
        kernel,
        out_shape=out_shape,
        in_specs=specs,
        out_specs=[VMEM] * len(outs),
        scratch_shapes=[pltpu.VMEM(shape, dtype) for shape, dtype in scratch],
        cost_estimate=pl.CostEstimate(flops=flops, bytes_accessed=1_000_000, transcendentals=0),
        compiler_params=pltpu.CompilerParams(vmem_limit_bytes=mib * 1024 * 1024),
    )(*operands)


F32 = jnp.float32
FIELD = ((512, LANES), F32)


def to_all(value):
    return lax.all_to_all(value, "dom", 0, 0, tiled=True)


def to_four(inner_1, middle, inner_2, far):
    far = lax.all_to_all(far, "dom", 0, 0, tiled=True, axis_index_groups=SHIFTED)
    near = []
    for value, pairs in ((inner_1, INNER_1), (middle, MIDDLE_1), (inner_2, INNER_2)):
        near.append(lax.ppermute(value, "dom", pairs))
    return (*near, far)


def to_two(cross, inner):
    cross = lax.ppermute(cross, "dom", CROSS_1)
    inner = lax.ppermute(inner, "dom", INNER_1)
    return cross, inner


def body(donor_fields, interp_weights, donor_owner, donor_element, geometry, wall_flag, forcing):
    place = lax.axis_index("dom").astype(jnp.int32).reshape(1)
    xmat = x_matrix()
    donors = lax.ppermute(donor_fields, "mesh", [(0, 1), (1, 0)])
    owner = donor_owner.reshape(1, N_REC)
    element = donor_element.reshape(1, N_REC)
    asked = ((32, LANES), F32)
    *requests, own, moves = call(
        route_kernel,
        (
            place,
            *(
                pltpu.with_memory_space_constraint(value, pltpu.HBM)
                for value in (interp_weights, owner, element)
            ),
        ),
        (asked, asked, asked, ((4, 32, LANES), F32), asked, ((8, CAP), jnp.int32)),
        scratch=(((6, 32, LANES), F32),),
    )
    requests = to_four(*requests)
    (fields,) = call(
        split_kernel, (donors,), (((BY_DOT, 512, 256), jnp.bfloat16),), smem_first=False,
    )
    answer = ((FIELDS, CAP), F32)
    (far,) = call(
        eval_kernel, (fields, donors, requests[3]), (((4, FIELDS, CAP), F32),),
        flops=3_000_000_000, smem_first=False, mib=24,
    )
    own_answer, inner_1, middle, inner_2 = call(
        eval_kernel, (fields, donors, own, *requests[:3]), (answer,) * 4,
        flops=4_000_000_000, smem_first=False, mib=24,
    )
    answered = to_four(inner_1, middle, inner_2, far)
    head = ((72, LANES), F32)
    heads = call(heads_kernel, (place, geometry, wall_flag, forcing), (head, head))
    unpacked = (place, *answered, own_answer, moves, owner)
    with_head = ((88, LANES), F32)
    share, *spread = call(
        share_kernel, (*unpacked, *heads), (((16, LANES), F32), with_head, with_head)
    )
    (interface,) = call(unpack_kernel, unpacked, (((FIELDS, N_REC), F32),))
    spread = to_two(*spread)
    inverse, free, load, beside = call(
        prep_kernel, (place, geometry, wall_flag, forcing, *spread),
        (FIELD, FIELD, FIELD, ((16, LANES), F32)),
        scratch=(((64, LANES), F32), ((72, LANES), F32), ((72, LANES), F32)),
    )
    face = ((64, LANES), F32)
    two_faces = ((128, LANES), F32)
    w0, u, edge, lift, moments, *faces = call(
        first_kernel,
        (place, share, *spread, geometry, beside, inverse, free,
         load, xmat),
        (FIELD, FIELD, two_faces, two_faces, ((1, LANES), F32), two_faces, two_faces),
        scratch=(FIELD, two_faces),
    )
    fixed = (geometry, inverse, free, xmat)
    w1, u, moments, *faces, w0_faces = call(
        functools.partial(next_kernel, 2),
        (place, w0, u, *to_two(*faces), *fixed, moments, load, lift),
        (FIELD, FIELD, ((1, LANES), F32), face, face, two_faces), scratch=(FIELD,),
    )
    w2, u, moments, *faces = call(
        functools.partial(next_kernel, 4),
        (place, w1, u, *to_two(*faces), *fixed, moments),
        (FIELD, FIELD, ((N_DOM, LANES), F32), face, face), scratch=(FIELD,),
    )
    sums = to_all(moments)
    (image,) = call(image_kernel, (place, u, *to_two(*faces), free), (FIELD,))
    velocity, residual = call(
        last_kernel, (w0, w0_faces, w1, w2, image, inverse, edge, sums), (FIELD, FIELD), smem_first=False,
    )
    return velocity, residual, interface


def solution(mesh):
    both = ("mesh", "dom")
    in_specs = (
        P(None, None, both), P(None, None, both), P(both, None), P(both), P(None, both),
        P(None, both), P(None, both),
    )
    out_specs = (P(None, both), P(None, both), P(None, both))

    return jax.shard_map(body, mesh=mesh, in_specs=in_specs, out_specs=out_specs, check_vma=False)
```

```python
import functools

import jax
import jax.numpy as jnp
import numpy as np
from jax import lax
from jax.experimental import pallas as pl
from jax.experimental.pallas import tpu as pltpu
from jax.sharding import PartitionSpec as P


N_DOM = 64
N_REC = 2048
CAP = 1024
FIELDS = 5
BY_DOT = 3
LANES = 128
BLOCK = 512
HALF = 256
CHUNK = 104


def both_ways(lows, distance):
    return [pair for q in lows for pair in ((q, q + distance), (q + distance, q))]


CROSS_1 = both_ways(range(1, N_DOM - 1, 2), 1)
INNER_1 = both_ways(range(0, N_DOM - 1, 2), 1)
CROSS_2 = both_ways([q for q in range(N_DOM - 2) if q % 4 >= 2], 2)
MIDDLE_1 = both_ways([q for q in range(N_DOM - 1) if q % 4 == 1], 1)
SHIFTED = [[(4 * g + 2 + t) % N_DOM for t in range(4)] for g in range(16)]
INNER_2 = both_ways([q for q in range(N_DOM - 2) if q % 4 < 2], 2)


def from_above(q):
    odd = q % 2 == 1
    late = q % 4 >= 2
    return odd, jnp.logical_not(odd), late, jnp.logical_not(late)


def pick_sides(q, inner_1, middle, inner_2, far):
    r = q % 4
    p = (q + 2) % 4

    def across(off):
        return far(jnp.clip(p + off, 0, 3))

    return (
        jnp.where(r < 2, across(-2), inner_2),
        jnp.where(r == 0, across(-1), jnp.where(r == 2, middle, inner_1)),
        jnp.where(r == 3, across(1), jnp.where(r == 1, middle, inner_1)),
        jnp.where(r >= 2, across(2), inner_2),
    )


def legendre_pair(values, degree):
    previous = values * 0.0 + 1.0
    current = values * 1.0
    for order in range(2, degree + 1):
        previous, current = (
            current,
            ((2 * order - 1) * values * current - (order - 1) * previous) / order,
        )
    return current, previous


def gll_tables():
    degree = 7
    count = degree + 1
    nodes = np.cos(np.pi * np.arange(count) / degree)
    for _ in range(80):
        top, lower = legendre_pair(nodes, degree)
        nodes = nodes - (nodes * top - lower) / (count * top)
    nodes = np.sort(nodes)
    top, lower = legendre_pair(nodes, degree)
    weights = 2.0 / (degree * count * top * top)
    identity = np.eye(count)
    spacing = nodes[:, None] - nodes[None, :] + identity
    derivative = top[:, None] / (top[None, :] * spacing) * (1.0 - identity)
    derivative[0, 0] = -degree * count / 4.0
    derivative[degree, degree] = degree * count / 4.0
    return nodes, weights, derivative


NODES, WEIGHTS, DERIV = gll_tables()
STIFF = DERIV.T @ (WEIGHTS[:, None] * DERIV)
STIFF = 0.5 * (STIFF + STIFF.T)
BARY = np.array([1.0 / np.prod([NODES[i] - NODES[j] for j in range(8) if j != i]) for i in range(8)])


def x_matrix():
    full = np.kron(np.diag(WEIGHTS), STIFF).astype(np.float32)
    high = jnp.asarray(full).astype(jnp.bfloat16)
    low = (jnp.asarray(full) - high.astype(jnp.float32)).astype(jnp.bfloat16)
    return jnp.concatenate([high, high, low], axis=1)


def iota(shape, dim):
    return lax.broadcasted_iota(jnp.int32, shape, dim)


def w_column():
    row = iota((8, LANES), 0)
    out = jnp.full((8, LANES), float(WEIGHTS[0]), jnp.float32)
    for i in range(1, 8):
        out = jnp.where(row == i, float(WEIGHTS[i]), out)
    return out


def s_column():
    row = iota((8, LANES), 0)
    out = jnp.full((8, LANES), float(STIFF[0, 0]), jnp.float32)
    for i in range(1, 8):
        out = jnp.where(row == i, float(STIFF[i, i]), out)
    return out


def sum_xy(ref, planes):
    rows = planes * 8
    lane = iota((rows, LANES), 1)
    low = ref[pl.ds(0, rows, stride=8), :]
    high = ref[pl.ds(7, rows, stride=8), :]
    ref[pl.ds(7, rows, stride=8), :] = high + jnp.where(
        lane % 8 < 7, pltpu.roll(low, LANES - 1, 1), 0.0
    )
    ref[pl.ds(0, rows, stride=8), :] = low + jnp.where(lane % 8 > 0, pltpu.roll(high, 1, 1), 0.0)
    lane = iota((8, LANES), 1)
    for k in range(planes):
        low = ref[k * 64 : k * 64 + 8, :]
        high = ref[k * 64 + 56 : k * 64 + 64, :]
        ref[k * 64 + 56 : k * 64 + 64, :] = high + jnp.where(
            lane < 120, pltpu.roll(low, LANES - 8, 1), 0.0
        )
        ref[k * 64 : k * 64 + 8, :] = low + jnp.where(lane >= 8, pltpu.roll(high, 8, 1), 0.0)


def apply_local(v_ref, geometry, xmat_ref, out_ref, planes, dot_with_v=False):
    wcol = w_column()
    gx = geometry[0:1, :]
    gyw = geometry[1:2, :] * wcol
    gzw = geometry[2:3, :] * wcol
    gmw = geometry[3:4, :] * wcol
    total = jnp.zeros((8, LANES), jnp.float32)
    for at in range(0, len(planes), 2):
        pair = range(at, min(at + 2, len(planes)))
        value = [v_ref[planes[n] * 64 : planes[n] * 64 + 64, :] for n in pair]
        value = jnp.concatenate(value, axis=1) if len(value) > 1 else value[0]
        high = value.astype(jnp.bfloat16)
        low = (value - high.astype(jnp.float32)).astype(jnp.bfloat16)
        along_x = lax.dot(
            xmat_ref[...], jnp.concatenate([high, low, high], axis=0),
            preferred_element_type=jnp.float32,
        )
        for n in pair:
            out_ref[n * 64 : n * 64 + 64, :] = along_x[:, (n - at) * LANES : (n - at + 1) * LANES]
    for at, k in enumerate(planes):
        plane = [v_ref[(k * 8 + j) * 8 : (k * 8 + j) * 8 + 8, :] for j in range(8)]
        for j in range(8):
            ysum = plane[0] * float(STIFF[j, 0] * WEIGHTS[k])
            for jj in range(1, 8):
                ysum = ysum + plane[jj] * float(STIFF[j, jj] * WEIGHTS[k])
            zsum = None
            for kk in range(8):
                term = v_ref[(kk * 8 + j) * 8 : (kk * 8 + j) * 8 + 8, :] * float(
                    STIFF[k, kk] * WEIGHTS[j]
                )
                zsum = term if zsum is None else zsum + term
            row = (at * 8 + j) * 8
            value = (
                out_ref[row : row + 8, :] * (gx * float(WEIGHTS[k]))
                + gyw * ysum
                + gzw * zsum
                + gmw * (plane[j] * float(WEIGHTS[k] * WEIGHTS[j]))
            )
            out_ref[row : row + 8, :] = value
            if dot_with_v:
                total = total + value * plane[j]
    return total


def lane_value(value, at):
    return jnp.where(iota((1, LANES), 1) == at, value, 0.0)


def by_side(q, cross_1, inner_1, cross_2=None, inner_2=None):
    above = from_above(q)
    out = (jnp.where(above[0], inner_1, cross_1), jnp.where(above[0], cross_1, inner_1))
    if cross_2 is not None:
        out += (jnp.where(above[2], inner_2, cross_2), jnp.where(above[2], cross_2, inner_2))
    return out


def route_kernel(
    place_ref, weights_ref, owner_ref, element_ref, geometry_ref, wall_ref, forcing_ref,
    cross_1_ref, inner_1_ref, cross_2_ref, inner_2_ref, own_ref, moves_ref, slots_ref,
):
    q = place_ref[0]
    width = N_REC
    lane = iota((8, width), 1)
    row = iota((8, width), 0)
    distance = owner_ref[...] - q + 2
    mine = distance == row
    count = mine.astype(jnp.int32)
    step = 1
    while step < width:
        count = count + jnp.where(lane >= step, pltpu.roll(count, step, 1), 0)
        step *= 2
    moves = jnp.where(mine, lane - (count - 1), 0)
    totals = count[:, width - 1 : width]
    node_rows = iota((8, width), 0)
    node = jnp.full((8, width), float(NODES[0]), jnp.float32)
    for i in range(1, 8):
        node = jnp.where(node_rows == i, float(NODES[i]), node)
    coords = [jnp.sum(weights_ref[d] * node, axis=0, keepdims=True) for d in range(3)]
    words = element_ref[...].astype(jnp.float32) + 1.0
    base = jnp.where(row % 4 == 3, words, 0.0)
    for d in range(3):
        base = jnp.where(row % 4 == d, coords[d], base)
    packs = [base, base, base]
    for b in range(11):
        step = 1 << b
        incoming = pltpu.roll(moves, width - step, 1)
        moved = (incoming >> b) & 1
        for n in range(3):
            first = jnp.broadcast_to(moved[2 * n : 2 * n + 1, :], (8, width))
            if n < 2:
                second = jnp.broadcast_to(moved[2 * n + 1 : 2 * n + 2, :], (8, width))
                first = jnp.where(row < 4, first, second)
            packs[n] = jnp.where(first == 1, pltpu.roll(packs[n], width - step, 1), packs[n])
        moves = jnp.where(moved == 1, incoming, jnp.where((moves >> b) & 1 == 1, 0, moves))
    moves_ref[...] = moves[:, :CAP]
    lane = iota((4, CAP), 1)
    for s in range(5):
        at = (s % 2) * 4
        slot = jnp.where(lane < totals[s : s + 1, :], packs[s // 2][at : at + 4, :CAP], 0.0)
        for c in range(8):
            slots_ref[s, 4 * c : 4 * c + 4, :] = slot[:, c * LANES : (c + 1) * LANES]
    above = from_above(q)
    bottom, top = forcing_ref[0:64, :], forcing_ref[448:512, :]
    spread = jnp.where(iota((8, LANES), 1) % 8 == iota((8, LANES), 0), 1.0, 0.0)
    wall = lax.dot(
        wall_ref[...].astype(jnp.float32), spread, preferred_element_type=jnp.float32
    )
    for target_ref, up in ((cross_1_ref, above[0]), (inner_1_ref, above[1])):
        target_ref[0:32, :] = jnp.where(up, slots_ref[3], slots_ref[1])
        target_ref[32:36, :] = geometry_ref[...]
        target_ref[36:38, :] = wall
        target_ref[38:40, :] = jnp.zeros((2, LANES), jnp.float32)
        target_ref[40:104, :] = jnp.where(up, top, bottom)
    for target_ref, up in ((cross_2_ref, above[2]), (inner_2_ref, above[3])):
        target_ref[...] = jnp.where(up, slots_ref[4], slots_ref[0])
    own_ref[...] = slots_ref[2]


def split_kernel(fields_ref, out_ref):
    for f in range(BY_DOT):
        value = fields_ref[f]
        high = value.astype(jnp.bfloat16)
        out_ref[f, :, 0:LANES] = high
        out_ref[f, :, LANES : 2 * LANES] = (value - high.astype(jnp.float32)).astype(jnp.bfloat16)


def basis_rows(coordinate):
    gaps = [coordinate - float(NODES[i]) for i in range(8)]
    before = [None] * 8
    after = [None] * 8
    for i in range(1, 8):
        before[i] = gaps[i - 1] if i == 1 else before[i - 1] * gaps[i - 1]
    for i in range(6, -1, -1):
        after[i] = gaps[i + 1] if i == 6 else after[i + 1] * gaps[i + 1]
    out = []
    for i in range(8):
        if i == 0:
            value = after[0]
        elif i == 7:
            value = before[7]
        else:
            value = before[i] * after[i]
        out.append(value * float(BARY[i]))
    return out


def eval_kernel(*refs):
    fields_ref, donors_ref, *refs = refs
    half = len(refs) // 2
    for source, target in zip(refs[:half], refs[half:]):
        words = source[0:32, :]
        valid = jnp.where((iota((32, LANES), 0) % 4 == 3) & (words > 0.0), 1, 0)
        count = jnp.sum(valid)
        blocks = (count + HALF - 1) // BLOCK
        left = (count - blocks * BLOCK + BLOCK - 1) // BLOCK

        def one_block(b, first, size, source=source, target=target):
            start = pl.multiple_of(b * size + first, HALF)
            rows = size // 32
            tiles = source[pl.ds(pl.multiple_of(b * rows + first // 32, 8), rows), :]
            words = jnp.concatenate(
                [tiles[4 * n : 4 * n + 4, :] for n in range(rows // 4)], axis=1
            )
            element = words[3:4, :].astype(jnp.int32) - 1
            hot_rows = iota((LANES, size), 0)
            hot = (hot_rows == element).astype(jnp.float32).astype(jnp.bfloat16)
            hot = jnp.concatenate([hot, hot], axis=0)
            element = jnp.maximum(element, 0)
            along = [basis_rows(words[d : d + 1, :]) for d in range(3)]
            row = iota((8, size), 0)
            wx = jnp.broadcast_to(along[0][0], (8, size))
            for i in range(1, 8):
                wx = jnp.where(row == i, along[0][i], wx)

            def by_gather(f, h):
                part = slice(h * LANES, h * LANES + LANES)
                index = jnp.broadcast_to(element[:, part], (8, LANES))
                wz = [jnp.broadcast_to(w[:, part], (8, LANES)) for w in along[2]]
                over_j = None
                for j in range(8):
                    over_k = None
                    for k in range(8):
                        row = 64 * k + 8 * j
                        term = wz[k] * jnp.take_along_axis(
                            donors_ref[f, row : row + 8, :], index, axis=1,
                            mode="promise_in_bounds",
                        )
                        over_k = term if over_k is None else over_k + term
                    term = over_k * along[1][j][:, part]
                    over_j = term if over_j is None else over_j + term
                target[f : f + 1, pl.ds(start + h * LANES, LANES)] = jnp.sum(
                    over_j * wx[:, part], axis=0, keepdims=True
                )

            gathers = [(f, h) for f in range(BY_DOT, FIELDS) for h in range(size // LANES)]
            for f in range(BY_DOT):
                picked = lax.dot(fields_ref[f], hot, preferred_element_type=jnp.float32)
                share = -(-len(gathers) // (BY_DOT - f))
                for work in gathers[:share]:
                    by_gather(*work)
                gathers = gathers[share:]
                over_k = picked[0:64, :] * along[2][0]
                for k in range(1, 8):
                    over_k = over_k + picked[64 * k : 64 * k + 64, :] * along[2][k]
                over_j = over_k[0:8, :] * along[1][0]
                for j in range(1, 8):
                    over_j = over_j + over_k[8 * j : 8 * j + 8, :] * along[1][j]
                target[f : f + 1, pl.ds(start, size)] = jnp.sum(
                    over_j * wx, axis=0, keepdims=True
                )

        def whole(b, carry, one_block=one_block):
            one_block(b, 0, BLOCK)
            return carry

        def part(b, carry, one_block=one_block, first=blocks * BLOCK):
            one_block(b, first, HALF)
            return carry

        lax.fori_loop(0, blocks, whole, 0)
        lax.fori_loop(0, left, part, 0)


def eval_far_kernel(place_ref, fields_ref, donors_ref, *refs):
    *refs, far_ref = refs
    eval_kernel(fields_ref, donors_ref, *refs)
    cross_1_ref, cross_2_ref, _ = refs[3:]
    r = place_ref[0] % 4
    far_ref[...] = jnp.zeros(far_ref.shape, jnp.float32)
    far_ref[r] = cross_2_ref[...]
    far_ref[jnp.where(r % 2 == 0, r + 1, r - 1)] = cross_1_ref[...]


def unpack_kernel(
    place_ref, inner_1_ref, middle_ref, inner_2_ref, far_ref, own_ref, moves_ref, owner_ref,
    out_ref,
):
    q = place_ref[0]
    width = N_REC
    below_2, below_1, above_1, above_2 = pick_sides(
        q, inner_1_ref[...], middle_ref[...], inner_2_ref[...], lambda t: far_ref[t]
    )
    zeros = jnp.zeros((FIELDS, CAP), jnp.float32)
    values = [
        jnp.concatenate([value, zeros], axis=1)
        for value in (below_2, below_1, own_ref[...], above_1, above_2)
    ]
    moves = jnp.concatenate([moves_ref[...], jnp.zeros((8, CAP), jnp.int32)], axis=1)
    for b in range(10, -1, -1):
        step = 1 << b
        incoming = pltpu.roll(moves, step, 1)
        moved = (incoming >> b) & 1
        for s in range(5):
            flag = jnp.broadcast_to(moved[s : s + 1, :], (FIELDS, width))
            values[s] = jnp.where(flag == 1, pltpu.roll(values[s], step, 1), values[s])
        moves = jnp.where(moved == 1, incoming, jnp.where((moves >> b) & 1 == 1, 0, moves))
    distance = jnp.broadcast_to(owner_ref[...] - q + 2, (FIELDS, width))
    out = values[0]
    for s in range(1, 5):
        out = jnp.where(distance == s, values[s], out)
    out_ref[...] = out


def share_kernel(
    place_ref, inner_1_ref, middle_ref, inner_2_ref, far_ref, own_ref, moves_ref, owner_ref,
    share_ref,
):
    q = place_ref[0]
    width = N_REC
    below_2, below_1, above_1, above_2 = pick_sides(
        q, inner_1_ref[0:1, :], middle_ref[0:1, :], inner_2_ref[0:1, :],
        lambda t: far_ref[t, 0:1, :],
    )
    row = iota((8, CAP), 0)
    values = jnp.broadcast_to(below_2, (8, CAP))
    for s, value in ((1, below_1), (2, own_ref[0:1, :]), (3, above_1), (4, above_2)):
        values = jnp.where(row == s, value, values)
    values = jnp.concatenate([values, jnp.zeros((8, CAP), jnp.float32)], axis=1)
    moves = jnp.concatenate([moves_ref[...], jnp.zeros((8, CAP), jnp.int32)], axis=1)
    for b in range(10, -1, -1):
        step = 1 << b
        incoming = pltpu.roll(moves, step, 1)
        moved = (incoming >> b) & 1
        values = jnp.where(moved == 1, pltpu.roll(values, step, 1), values)
        moves = jnp.where(moved == 1, incoming, jnp.where((moves >> b) & 1 == 1, 0, moves))
    mine = iota((8, width), 0) == owner_ref[...] - q + 2
    out = jnp.sum(jnp.where(mine, values, 0.0), axis=0, keepdims=True)
    for n in range(16):
        share_ref[n : n + 1, :] = out[:, n * LANES : (n + 1) * LANES]


def prep_kernel(
    place_ref, geometry_ref, wall_ref, forcing_ref, cross_ref, inner_ref,
    inverse_ref, free_ref, load_ref, beside_ref, plane_ref, below_ref, above_ref,
):
    q = place_ref[0]
    below_ref[...], above_ref[...] = by_side(q, cross_ref[32:104, :], inner_ref[32:104, :])
    beside_ref[0:8, :] = below_ref[0:8, :]
    beside_ref[8:16, :] = above_ref[0:8, :]
    wcol = w_column()
    scol = s_column()

    def diagonal(geometry, k, j):
        wk, wj = float(WEIGHTS[k]), float(WEIGHTS[j])
        sk, sj = float(STIFF[k, k]), float(STIFF[j, j])
        return (
            geometry[0:1, :] * (scol * (wk * wj))
            + geometry[1:2, :] * (wcol * (wk * sj))
            + geometry[2:3, :] * (wcol * (sk * wj))
            + geometry[3:4, :] * (wcol * (wk * wj))
        )

    geometry = geometry_ref[...]
    below = below_ref[0:8, :]
    above = above_ref[0:8, :]
    lane = iota((8, LANES), 1)
    row = iota((8, LANES), 0)
    zero = jnp.zeros((8, LANES), jnp.float32)

    def wall_plane(low, high):
        for j in range(8):
            plane_ref[8 * j : 8 * j + 8, :] = zero
        plane_ref[0:8, :] = jnp.where(lane < 8, low, 0.0) + zero
        plane_ref[56:64, :] = jnp.where(lane >= 120, high, 0.0) + zero
        sum_xy(plane_ref, 1)
        return plane_ref[...]

    spread = jnp.where(lane % 8 == row, 1.0, 0.0)
    flags = lax.dot(
        wall_ref[...].astype(jnp.float32), spread, preferred_element_type=jnp.float32
    )
    wall = wall_plane(flags[0:1, :], flags[1:2, :])
    wall_below = wall_plane(below[4:5, :], below[5:6, :])
    wall_above = wall_plane(above[4:5, :], above[5:6, :])
    mark = jnp.where(
        ((row == 0) & (lane % 8 == 0)) | ((row == 7) & (lane % 8 == 7)), 1.0, 0.0
    )
    for j in range(8):
        plane_ref[8 * j : 8 * j + 8, :] = mark
    sum_xy(plane_ref, 1)
    rec = plane_ref[...]
    has_below = jnp.where(q > 0, 1.0, 0.0)
    has_above = jnp.where(q < N_DOM - 1, 1.0, 0.0)
    inner = 1.0 - jnp.minimum(rec + wall, 1.0)
    bottom = 1.0 - jnp.minimum(rec + rec * has_below + (wall + wall_below), 1.0)
    top = 1.0 - jnp.minimum(rec + rec * has_above + (wall + wall_above), 1.0)
    free_ref[0:64, :] = bottom
    free_ref[448:512, :] = top
    for k in range(1, 7):
        free_ref[64 * k : 64 * k + 64, :] = inner

    for k in range(8):
        for j in range(8):
            inverse_ref[(k * 8 + j) * 8 : (k * 8 + j) * 8 + 8, :] = diagonal(geometry, k, j)
    sum_xy(inverse_ref, 8)
    for j in range(8):
        plane_ref[8 * j : 8 * j + 8, :] = diagonal(below, 7, j)
    sum_xy(plane_ref, 1)
    inverse_ref[0:64, :] = inverse_ref[0:64, :] + plane_ref[...]
    for j in range(8):
        plane_ref[8 * j : 8 * j + 8, :] = diagonal(above, 0, j)
    sum_xy(plane_ref, 1)
    inverse_ref[448:512, :] = inverse_ref[448:512, :] + plane_ref[...]
    for k in range(8):
        at = slice(64 * k, 64 * k + 64)
        inverse_ref[at, :] = free_ref[at, :] / inverse_ref[at, :]

    for k in range(8):
        for j in range(8):
            at = slice((k * 8 + j) * 8, (k * 8 + j) * 8 + 8)
            load_ref[at, :] = forcing_ref[at, :] * (
                geometry[3:4, :] * (wcol * float(WEIGHTS[k] * WEIGHTS[j]))
            )
    sum_xy(load_ref, 8)
    for other_ref, k, base in ((below_ref, 7, 0), (above_ref, 0, 448)):
        for j in range(8):
            plane_ref[8 * j : 8 * j + 8, :] = other_ref[8 + 8 * j : 16 + 8 * j, :] * (
                other_ref[3:4, :] * (wcol * float(WEIGHTS[k] * WEIGHTS[j]))
            )
        sum_xy(plane_ref, 1)
        load_ref[base : base + 64, :] = load_ref[base : base + 64, :] + plane_ref[...]


def inverse_multiplicity(q):
    row = iota((64, LANES), 0)
    lane = iota((64, LANES), 1)
    i, j = row % 8, row // 8
    x, y = lane % 8, lane // 8
    along_x = ((i == 0) & (x > 0)) | ((i == 7) & (x < 7))
    along_y = ((j == 0) & (y > 0)) | ((j == 7) & (y < 15))
    inner = jnp.where(along_x, 0.5, 1.0) * jnp.where(along_y, 0.5, 1.0)
    return (
        inner,
        inner * jnp.where(q > 0, 0.5, 1.0),
        inner * jnp.where(q < N_DOM - 1, 0.5, 1.0),
    )


def krylov_step(q, w_ref, inverse_ref, geometry_ref, xmat_ref, v_ref, u_ref, at, moments):
    inner, bottom, top = inverse_multiplicity(q)
    norm = jnp.zeros((64, LANES), jnp.float32)
    for k in range(8):
        rows = slice(64 * k, 64 * k + 64)
        w = w_ref[rows, :]
        v = inverse_ref[rows, :] * w
        v_ref[rows, :] = v
        norm = norm + v * w * (bottom if k == 0 else top if k == 7 else inner)
    energy = apply_local(
        v_ref, geometry_ref[...], xmat_ref, u_ref, tuple(range(8)), dot_with_v=True
    )
    sum_xy(u_ref, 8)
    return moments + lane_value(jnp.sum(norm), at) + lane_value(jnp.sum(energy), at + 1)


def first_kernel(
    place_ref, own_ref, cross_in_ref, inner_in_ref, geometry_ref,
    beside_ref, inverse_ref, free_ref, load_ref, xmat_ref, w_ref, u_ref, edge_ref, lift_ref, moments_ref, cross_ref,
    inner_ref, v_ref, face_ref,
):
    q = place_ref[0]
    below, above = by_side(q, cross_in_ref[...], inner_in_ref[...])
    pick_row = iota((32, 2 * LANES), 0)
    pick_lane = iota((32, 2 * LANES), 1)
    odd = pick_lane // LANES
    picks = [
        jnp.where(
            (pick_lane % LANES == pick_row % 8 * 16 + (8 * odd + 7 * s)) & (pick_row < 24), 1.0, 0.0
        ).astype(jnp.bfloat16)
        for s in range(2)
    ]

    def bf16_parts(value):
        parts = []
        for _ in range(3):
            part = value.astype(jnp.bfloat16)
            parts.append(part.astype(jnp.float32))
            value = value - parts[-1]
        return jnp.concatenate([*parts, jnp.zeros_like(value)], axis=0).astype(jnp.bfloat16)

    layers = (below, own_ref[...], above)
    received = {off: [] for off in range(-1, 2)}
    for s in range(2):
        values = jnp.concatenate([layer[8 * s : 8 * s + 8, :] for layer in layers], axis=1)
        spread = lax.dot_general(
            bf16_parts(values), picks[s], (((0,), (0,)), ((), ())),
            preferred_element_type=jnp.float32,
        )
        for n in range(3):
            at = n * LANES
            plane = spread[at : at + 64, :LANES] + spread[at + 64 : at + 128, LANES:]
            received[n - 1].append([plane[8 * k : 8 * k + 8, :] for k in range(8)])
    lane = iota((8, LANES), 1)
    j_row = iota((8, LANES), 0)
    low = (j_row == 0) & (lane >= 8)
    high = (j_row == 7) & (lane < 120)

    def sum_y(value):
        down = jnp.broadcast_to(pltpu.roll(value, LANES - 8, 1)[0:1, :], (8, LANES))
        up = jnp.broadcast_to(pltpu.roll(value, 8, 1)[7:8, :], (8, LANES))
        return value + jnp.where(high, down, 0.0) + jnp.where(low, up, 0.0)

    count_y = jnp.where(low | high, 2.0, 1.0)
    on_side = [jnp.where(lane % 8 == x, 1.0, 0.0) for x in (0, 7)]

    def boundary(off):
        out = []
        has_below = jnp.where(q + off > 0, 1.0, 0.0)
        has_above = jnp.where(q + off < N_DOM - 1, 1.0, 0.0)
        for s in range(2):
            side = []
            for k in range(8):
                total = received[off][s][k]
                count = count_y * on_side[s]
                if k == 0:
                    if off >= 0:
                        total = total + received[off - 1][s][7]
                    count = count + count * has_below
                if k == 7:
                    if off <= 0:
                        total = total + received[off + 1][s][0]
                    count = count + count * has_above
                side.append(sum_y(total) / jnp.maximum(count, 1.0))
            out.append(jnp.concatenate(side, axis=0))
        return out

    zero = jnp.zeros((64, LANES), jnp.float32)
    for k in range(8):
        v_ref[64 * k : 64 * k + 64, :] = zero
    for off, geometry, plane in ((-1, beside_ref[0:4, :], 7), (1, beside_ref[8:12, :], 0)):
        sides = boundary(off)
        v_ref[pl.ds(0, 64, stride=8), :] = sides[0]
        v_ref[pl.ds(7, 64, stride=8), :] = sides[1]
        at = 0 if off < 0 else 64
        apply_local(v_ref, geometry, xmat_ref, face_ref.at[at : at + 64, :], (plane,))
        sum_xy(face_ref.at[at : at + 64, :], 1)
    sides = boundary(0)
    v_ref[pl.ds(0, 64, stride=8), :] = sides[0]
    v_ref[pl.ds(7, 64, stride=8), :] = sides[1]
    edge_ref[0:64, :] = sides[0]
    edge_ref[64:128, :] = sides[1]
    apply_local(v_ref, geometry_ref[...], xmat_ref, u_ref, tuple(range(8)))
    sum_xy(u_ref, 8)
    lift_ref[0:64, :] = u_ref[0:64, :]
    lift_ref[64:128, :] = u_ref[448:512, :]
    u_ref[0:64, :] = u_ref[0:64, :] + face_ref[0:64, :]
    u_ref[448:512, :] = u_ref[448:512, :] + face_ref[64:128, :]
    for k in range(8):
        rows = slice(64 * k, 64 * k + 64)
        w_ref[rows, :] = free_ref[rows, :] * (load_ref[rows, :] - u_ref[rows, :])
    moments_ref[...] = krylov_step(
        q, w_ref, inverse_ref, geometry_ref, xmat_ref, v_ref, u_ref, 0,
        jnp.zeros((1, LANES), jnp.float32),
    )
    send_faces(q, u_ref, cross_ref, inner_ref)
    up = from_above(q)[0]
    bottom, top = lift_ref[0:64, :], lift_ref[64:128, :]
    cross_ref[64:128, :] = jnp.where(up, top, bottom)
    inner_ref[64:128, :] = jnp.where(up, bottom, top)


def send_faces(q, u_ref, cross_ref, inner_ref):
    up = from_above(q)[0]
    bottom, top = u_ref[0:64, :], u_ref[448:512, :]
    cross_ref[0:64, :] = jnp.where(up, top, bottom)
    inner_ref[0:64, :] = jnp.where(up, bottom, top)


def next_kernel(
    at, place_ref, w_old_ref, u_old_ref, cross_in_ref, inner_in_ref, geometry_ref, inverse_ref,
    free_ref, xmat_ref, moments_old_ref, *refs,
):
    q = place_ref[0]
    if at == 2:
        load_ref, lift_ref, *refs = refs
    w_ref, u_ref, moments_ref, cross_ref, inner_ref, *refs = refs
    v_ref = refs[-1]
    below, above = by_side(q, cross_in_ref[...], inner_in_ref[...])
    for k in range(8):
        rows = slice(64 * k, 64 * k + 64)
        image = u_old_ref[rows, :]
        w_old = w_old_ref[rows, :]
        if k in (0, 7):
            other = below if k == 0 else above
            image = image + other[0:64, :]
            face = slice(0, 64) if k == 0 else slice(64, 128)
            if at == 2:
                w_old = free_ref[rows, :] * (
                    load_ref[rows, :] - (lift_ref[face, :] + other[64:128, :])
                )
                refs[0][face, :] = w_old
        w_ref[rows, :] = free_ref[rows, :] * image - w_old
    row = krylov_step(
        q, w_ref, inverse_ref, geometry_ref, xmat_ref, v_ref, u_ref, at, moments_old_ref[...]
    )
    moments_ref[...] = jnp.broadcast_to(row, moments_ref.shape)
    send_faces(q, u_ref, cross_ref, inner_ref)


def image_kernel(place_ref, u_ref, cross_in_ref, inner_in_ref, free_ref, image_ref):
    below, above = by_side(place_ref[0], cross_in_ref[...], inner_in_ref[...])
    image_ref[...] = free_ref[...] * u_ref[...]
    image_ref[0:64, :] = image_ref[0:64, :] + free_ref[0:64, :] * below
    image_ref[448:512, :] = image_ref[448:512, :] + free_ref[448:512, :] * above


def last_kernel(
    w0_ref, face_ref, w1_ref, w2_ref, image_ref, inverse_ref, edge_ref, moments_ref,
    velocity_ref, residual_ref,
):
    sums = jnp.sum(moments_ref[...], axis=0, keepdims=True)
    h0, a0, h2, a1, h4, a2 = [sums[:, m : m + 1] for m in range(6)]
    h1, h3 = a0 - h0, a1 - h2
    g00, g01, g02, g11, g12, g22 = a0, h2 + h1, h3 + h2, a1, h4 + h3, a2
    b0, b1, b2 = h0, h1, h2
    l10 = g01 / g00
    l20 = g02 / g00
    d1 = g11 - l10 * g01
    e12 = g12 - l10 * g02
    l21 = e12 / d1
    d2 = g22 - l20 * g02 - l21 * e12
    y1 = b1 - l10 * b0
    y2 = b2 - l20 * b0 - l21 * y1
    c2 = y2 / d2
    c1 = y1 / d1 - l21 * c2
    c0 = b0 / g00 - l10 * c1 - l20 * c2
    c0, c1, c2 = [jnp.broadcast_to(c, (64, LANES)) for c in (c0, c1, c2)]
    for k in range(8):
        rows = slice(64 * k, 64 * k + 64)
        w0, w1, w2 = w0_ref[rows, :], w1_ref[rows, :], w2_ref[rows, :]
        if k in (0, 7):
            w0 = face_ref[0:64, :] if k == 0 else face_ref[64:128, :]
        velocity_ref[rows, :] = inverse_ref[rows, :] * (c0 * w0 + c1 * w1 + c2 * w2)
        residual_ref[rows, :] = (
            w0 - c0 * (w1 + w0) - c1 * (w2 + w1) - c2 * image_ref[rows, :]
        )
    for s in range(2):
        rows = pl.ds(7 * s, 64, stride=8)
        velocity_ref[rows, :] = velocity_ref[rows, :] + edge_ref[64 * s : 64 * s + 64, :]


VMEM = pl.BlockSpec(memory_space=pltpu.VMEM)
SMEM = pl.BlockSpec(memory_space=pltpu.SMEM)


def call(kernel, operands, outs, scratch=(), flops=100_000, smem_first=True, mib=12):
    specs = [VMEM] * len(operands)
    if smem_first:
        specs[0] = SMEM
    out_shape = [jax.ShapeDtypeStruct(shape, dtype) for shape, dtype in outs]
    return pl.pallas_call(
        kernel,
        out_shape=out_shape,
        in_specs=specs,
        out_specs=[VMEM] * len(outs),
        scratch_shapes=[pltpu.VMEM(shape, dtype) for shape, dtype in scratch],
        cost_estimate=pl.CostEstimate(flops=flops, bytes_accessed=1_000_000, transcendentals=0),
        compiler_params=pltpu.CompilerParams(vmem_limit_bytes=mib * 1024 * 1024),
    )(*operands)


F32 = jnp.float32
FIELD = ((512, LANES), F32)


def to_all(value):
    return lax.all_to_all(value, "dom", 0, 0, tiled=True)


def to_neighbours(cross_1, inner_1, cross_2=None, inner_2=None):
    lists = ((cross_1, CROSS_1), (cross_2, CROSS_2), (inner_1, INNER_1), (inner_2, INNER_2))
    moved = []
    for value, pairs in lists:
        moved.append(None if value is None else lax.ppermute(value, "dom", pairs))
    return [moved[n] for n in (0, 2, 1, 3) if moved[n] is not None]


def to_four(inner_1, middle, inner_2, far):
    far = lax.all_to_all(far, "dom", 0, 0, tiled=True, axis_index_groups=SHIFTED)
    near = []
    for value, pairs in ((inner_1, INNER_1), (middle, MIDDLE_1), (inner_2, INNER_2)):
        near.append(lax.ppermute(value, "dom", pairs))
    return (*near, far)


def body(donor_fields, interp_weights, donor_owner, donor_element, geometry, wall_flag, forcing):
    place = lax.axis_index("dom").astype(jnp.int32).reshape(1)
    xmat = x_matrix()
    donors = lax.ppermute(donor_fields, "mesh", [(0, 1), (1, 0)])
    owner = donor_owner.reshape(1, N_REC)
    element = donor_element.reshape(1, N_REC)
    asked = ((32, LANES), F32)
    with_head = ((CHUNK, LANES), F32)
    *requests, own, moves = call(
        route_kernel,
        (
            place,
            *(
                pltpu.with_memory_space_constraint(value, pltpu.HBM)
                for value in (interp_weights, owner, element, geometry, wall_flag, forcing)
            ),
        ),
        (with_head, with_head, asked, asked, asked, ((8, CAP), jnp.int32)),
        scratch=(((5, 32, LANES), F32),),
    )
    requests = to_neighbours(*requests)
    (fields,) = call(
        split_kernel, (donors,), (((BY_DOT, 512, 256), jnp.bfloat16),), smem_first=False,
    )
    answer = ((FIELDS, CAP), F32)
    own_answer, inner_1 = call(
        eval_kernel, (fields, donors, own, requests[1]), (answer,) * 2,
        flops=3_000_000_000, smem_first=False, mib=24,
    )
    middle, _, inner_2, far = call(
        eval_far_kernel, (place, fields, donors, requests[0], requests[2], requests[3]),
        (answer, answer, answer, ((4, FIELDS, CAP), F32)),
        flops=4_000_000_000, mib=24,
    )
    answered = to_four(inner_1, middle, inner_2, far)
    inverse, free, load, beside = call(
        prep_kernel, (place, geometry, wall_flag, forcing, requests[0], requests[1]),
        (FIELD, FIELD, FIELD, ((16, LANES), F32)),
        scratch=(((64, LANES), F32), ((72, LANES), F32), ((72, LANES), F32)),
    )
    unpacked = (place, *answered, own_answer, moves, owner)
    (share,) = call(share_kernel, unpacked, (((16, LANES), F32),))
    (interface,) = call(unpack_kernel, unpacked, (((FIELDS, N_REC), F32),))
    face = ((64, LANES), F32)
    two_faces = ((128, LANES), F32)
    w0, u, edge, lift, moments, *faces = call(
        first_kernel,
        (place, share, *to_neighbours(share, share), geometry, beside, inverse, free,
         load, xmat),
        (FIELD, FIELD, two_faces, two_faces, ((1, LANES), F32), two_faces, two_faces),
        scratch=(FIELD, two_faces),
    )
    fixed = (geometry, inverse, free, xmat)
    w1, u, moments, *faces, w0_faces = call(
        functools.partial(next_kernel, 2),
        (place, w0, u, *to_neighbours(*faces), *fixed, moments, load, lift),
        (FIELD, FIELD, ((1, LANES), F32), face, face, two_faces), scratch=(FIELD,),
    )
    w2, u, moments, *faces = call(
        functools.partial(next_kernel, 4),
        (place, w1, u, *to_neighbours(*faces), *fixed, moments),
        (FIELD, FIELD, ((N_DOM, LANES), F32), face, face), scratch=(FIELD,),
    )
    sums = to_all(moments)
    (image,) = call(image_kernel, (place, u, *to_neighbours(*faces), free), (FIELD,))
    velocity, residual = call(
        last_kernel, (w0, w0_faces, w1, w2, image, inverse, edge, sums), (FIELD, FIELD), smem_first=False,
    )
    return velocity, residual, interface


def solution(mesh):
    both = ("mesh", "dom")
    in_specs = (
        P(None, None, both), P(None, None, both), P(both, None), P(both), P(None, both),
        P(None, both), P(None, both),
    )
    out_specs = (P(None, both), P(None, both), P(None, both))

    return jax.shard_map(body, mesh=mesh, in_specs=in_specs, out_specs=out_specs, check_vma=False)
```

```python
import functools

import jax
import jax.numpy as jnp
import numpy as np
from jax import lax
from jax.experimental import pallas as pl
from jax.experimental.pallas import tpu as pltpu
from jax.sharding import PartitionSpec as P


N_DOM = 64
N_REC = 2048
CAP = 1024
FIELDS = 5
BY_DOT = 3
LANES = 128
BLOCK = 512
HALF = 256
CHUNK = 104


def both_ways(lows, distance):
    return [pair for q in lows for pair in ((q, q + distance), (q + distance, q))]


CROSS_1 = both_ways(range(1, N_DOM - 1, 2), 1)
INNER_1 = both_ways(range(0, N_DOM - 1, 2), 1)
CROSS_2 = both_ways([q for q in range(N_DOM - 2) if q % 4 >= 2], 2)
MIDDLE_1 = both_ways([q for q in range(N_DOM - 1) if q % 4 == 1], 1)
SHIFTED = [[(4 * g + 2 + t) % N_DOM for t in range(4)] for g in range(16)]
INNER_2 = both_ways([q for q in range(N_DOM - 2) if q % 4 < 2], 2)


def from_above(q):
    odd = q % 2 == 1
    late = q % 4 >= 2
    return odd, jnp.logical_not(odd), late, jnp.logical_not(late)


def pick_sides(q, inner_1, middle, inner_2, far):
    r = q % 4
    p = (q + 2) % 4

    def across(off):
        return far(jnp.clip(p + off, 0, 3))

    return (
        jnp.where(r < 2, across(-2), inner_2),
        jnp.where(r == 0, across(-1), jnp.where(r == 2, middle, inner_1)),
        jnp.where(r == 3, across(1), jnp.where(r == 1, middle, inner_1)),
        jnp.where(r >= 2, across(2), inner_2),
    )


def legendre_pair(values, degree):
    previous = values * 0.0 + 1.0
    current = values * 1.0
    for order in range(2, degree + 1):
        previous, current = (
            current,
            ((2 * order - 1) * values * current - (order - 1) * previous) / order,
        )
    return current, previous


def gll_tables():
    degree = 7
    count = degree + 1
    nodes = np.cos(np.pi * np.arange(count) / degree)
    for _ in range(80):
        top, lower = legendre_pair(nodes, degree)
        nodes = nodes - (nodes * top - lower) / (count * top)
    nodes = np.sort(nodes)
    top, lower = legendre_pair(nodes, degree)
    weights = 2.0 / (degree * count * top * top)
    identity = np.eye(count)
    spacing = nodes[:, None] - nodes[None, :] + identity
    derivative = top[:, None] / (top[None, :] * spacing) * (1.0 - identity)
    derivative[0, 0] = -degree * count / 4.0
    derivative[degree, degree] = degree * count / 4.0
    return nodes, weights, derivative


NODES, WEIGHTS, DERIV = gll_tables()
STIFF = DERIV.T @ (WEIGHTS[:, None] * DERIV)
STIFF = 0.5 * (STIFF + STIFF.T)
BARY = np.array([1.0 / np.prod([NODES[i] - NODES[j] for j in range(8) if j != i]) for i in range(8)])


def x_matrix():
    full = np.kron(np.diag(WEIGHTS), STIFF).astype(np.float32)
    high = jnp.asarray(full).astype(jnp.bfloat16)
    low = (jnp.asarray(full) - high.astype(jnp.float32)).astype(jnp.bfloat16)
    return jnp.concatenate([high, high, low], axis=1)


def iota(shape, dim):
    return lax.broadcasted_iota(jnp.int32, shape, dim)


def w_column():
    row = iota((8, LANES), 0)
    out = jnp.full((8, LANES), float(WEIGHTS[0]), jnp.float32)
    for i in range(1, 8):
        out = jnp.where(row == i, float(WEIGHTS[i]), out)
    return out


def s_column():
    row = iota((8, LANES), 0)
    out = jnp.full((8, LANES), float(STIFF[0, 0]), jnp.float32)
    for i in range(1, 8):
        out = jnp.where(row == i, float(STIFF[i, i]), out)
    return out


def sum_xy(ref, planes):
    rows = planes * 8
    lane = iota((rows, LANES), 1)
    low = ref[pl.ds(0, rows, stride=8), :]
    high = ref[pl.ds(7, rows, stride=8), :]
    ref[pl.ds(7, rows, stride=8), :] = high + jnp.where(
        lane % 8 < 7, pltpu.roll(low, LANES - 1, 1), 0.0
    )
    ref[pl.ds(0, rows, stride=8), :] = low + jnp.where(lane % 8 > 0, pltpu.roll(high, 1, 1), 0.0)
    lane = iota((8, LANES), 1)
    for k in range(planes):
        low = ref[k * 64 : k * 64 + 8, :]
        high = ref[k * 64 + 56 : k * 64 + 64, :]
        ref[k * 64 + 56 : k * 64 + 64, :] = high + jnp.where(
            lane < 120, pltpu.roll(low, LANES - 8, 1), 0.0
        )
        ref[k * 64 : k * 64 + 8, :] = low + jnp.where(lane >= 8, pltpu.roll(high, 8, 1), 0.0)


def apply_local(v_ref, geometry, xmat_ref, out_ref, planes, dot_with_v=False):
    wcol = w_column()
    gx = geometry[0:1, :]
    gyw = geometry[1:2, :] * wcol
    gzw = geometry[2:3, :] * wcol
    gmw = geometry[3:4, :] * wcol
    total = jnp.zeros((8, LANES), jnp.float32)
    for at in range(0, len(planes), 2):
        pair = range(at, min(at + 2, len(planes)))
        value = [v_ref[planes[n] * 64 : planes[n] * 64 + 64, :] for n in pair]
        value = jnp.concatenate(value, axis=1) if len(value) > 1 else value[0]
        high = value.astype(jnp.bfloat16)
        low = (value - high.astype(jnp.float32)).astype(jnp.bfloat16)
        along_x = lax.dot(
            xmat_ref[...], jnp.concatenate([high, low, high], axis=0),
            preferred_element_type=jnp.float32,
        )
        for n in pair:
            out_ref[n * 64 : n * 64 + 64, :] = along_x[:, (n - at) * LANES : (n - at + 1) * LANES]
    for at, k in enumerate(planes):
        plane = [v_ref[(k * 8 + j) * 8 : (k * 8 + j) * 8 + 8, :] for j in range(8)]
        for j in range(8):
            ysum = plane[0] * float(STIFF[j, 0] * WEIGHTS[k])
            for jj in range(1, 8):
                ysum = ysum + plane[jj] * float(STIFF[j, jj] * WEIGHTS[k])
            zsum = None
            for kk in range(8):
                term = v_ref[(kk * 8 + j) * 8 : (kk * 8 + j) * 8 + 8, :] * float(
                    STIFF[k, kk] * WEIGHTS[j]
                )
                zsum = term if zsum is None else zsum + term
            row = (at * 8 + j) * 8
            value = (
                out_ref[row : row + 8, :] * (gx * float(WEIGHTS[k]))
                + gyw * ysum
                + gzw * zsum
                + gmw * (plane[j] * float(WEIGHTS[k] * WEIGHTS[j]))
            )
            out_ref[row : row + 8, :] = value
            if dot_with_v:
                total = total + value * plane[j]
    return total


def lane_value(value, at):
    return jnp.where(iota((1, LANES), 1) == at, value, 0.0)


def by_side(q, cross_1, inner_1, cross_2=None, inner_2=None):
    above = from_above(q)
    out = (jnp.where(above[0], inner_1, cross_1), jnp.where(above[0], cross_1, inner_1))
    if cross_2 is not None:
        out += (jnp.where(above[2], inner_2, cross_2), jnp.where(above[2], cross_2, inner_2))
    return out


def route_kernel(
    place_ref, weights_ref, owner_ref, element_ref, geometry_ref, wall_ref, forcing_ref,
    cross_1_ref, inner_1_ref, cross_2_ref, inner_2_ref, own_ref, moves_ref, slots_ref,
):
    q = place_ref[0]
    width = N_REC
    lane = iota((8, width), 1)
    row = iota((8, width), 0)
    distance = owner_ref[...] - q + 2
    mine = distance == row
    count = mine.astype(jnp.int32)
    step = 1
    while step < width:
        count = count + jnp.where(lane >= step, pltpu.roll(count, step, 1), 0)
        step *= 2
    moves = jnp.where(mine, lane - (count - 1), 0)
    totals = count[:, width - 1 : width]
    node_rows = iota((8, width), 0)
    node = jnp.full((8, width), float(NODES[0]), jnp.float32)
    for i in range(1, 8):
        node = jnp.where(node_rows == i, float(NODES[i]), node)
    coords = [jnp.sum(weights_ref[d] * node, axis=0, keepdims=True) for d in range(3)]
    words = element_ref[...].astype(jnp.float32) + 1.0
    base = jnp.where(row % 4 == 3, words, 0.0)
    for d in range(3):
        base = jnp.where(row % 4 == d, coords[d], base)
    packs = [base, base, base]
    for b in range(11):
        step = 1 << b
        incoming = pltpu.roll(moves, width - step, 1)
        moved = (incoming >> b) & 1
        for n in range(3):
            first = jnp.broadcast_to(moved[2 * n : 2 * n + 1, :], (8, width))
            if n < 2:
                second = jnp.broadcast_to(moved[2 * n + 1 : 2 * n + 2, :], (8, width))
                first = jnp.where(row < 4, first, second)
            packs[n] = jnp.where(first == 1, pltpu.roll(packs[n], width - step, 1), packs[n])
        moves = jnp.where(moved == 1, incoming, jnp.where((moves >> b) & 1 == 1, 0, moves))
    moves_ref[...] = moves[:, :CAP]
    lane = iota((4, CAP), 1)
    for s in range(5):
        at = (s % 2) * 4
        slot = jnp.where(lane < totals[s : s + 1, :], packs[s // 2][at : at + 4, :CAP], 0.0)
        for c in range(8):
            slots_ref[s, 4 * c : 4 * c + 4, :] = slot[:, c * LANES : (c + 1) * LANES]
    above = from_above(q)
    bottom, top = forcing_ref[0:64, :], forcing_ref[448:512, :]
    spread = jnp.where(iota((8, LANES), 1) % 8 == iota((8, LANES), 0), 1.0, 0.0)
    wall = lax.dot(
        wall_ref[...].astype(jnp.float32), spread, preferred_element_type=jnp.float32
    )
    for target_ref, up in ((cross_1_ref, above[0]), (inner_1_ref, above[1])):
        target_ref[0:32, :] = jnp.where(up, slots_ref[3], slots_ref[1])
        target_ref[32:36, :] = geometry_ref[...]
        target_ref[36:38, :] = wall
        target_ref[38:40, :] = jnp.zeros((2, LANES), jnp.float32)
        target_ref[40:104, :] = jnp.where(up, top, bottom)
    for target_ref, up in ((cross_2_ref, above[2]), (inner_2_ref, above[3])):
        target_ref[...] = jnp.where(up, slots_ref[4], slots_ref[0])
    own_ref[...] = slots_ref[2]


def split_kernel(fields_ref, out_ref):
    for f in range(BY_DOT):
        value = fields_ref[f]
        high = value.astype(jnp.bfloat16)
        out_ref[f, :, 0:LANES] = high
        out_ref[f, :, LANES : 2 * LANES] = (value - high.astype(jnp.float32)).astype(jnp.bfloat16)


def basis_rows(coordinate):
    gaps = [coordinate - float(NODES[i]) for i in range(8)]
    before = [None] * 8
    after = [None] * 8
    for i in range(1, 8):
        before[i] = gaps[i - 1] if i == 1 else before[i - 1] * gaps[i - 1]
    for i in range(6, -1, -1):
        after[i] = gaps[i + 1] if i == 6 else after[i + 1] * gaps[i + 1]
    out = []
    for i in range(8):
        if i == 0:
            value = after[0]
        elif i == 7:
            value = before[7]
        else:
            value = before[i] * after[i]
        out.append(value * float(BARY[i]))
    return out


def eval_kernel(*refs):
    fields_ref, donors_ref, *refs = refs
    half = len(refs) // 2
    for source, target in zip(refs[:half], refs[half:]):
        words = source[0:32, :]
        valid = jnp.where((iota((32, LANES), 0) % 4 == 3) & (words > 0.0), 1, 0)
        count = jnp.sum(valid)
        blocks = (count + HALF - 1) // BLOCK
        left = (count - blocks * BLOCK + BLOCK - 1) // BLOCK

        def one_block(b, first, size, source=source, target=target):
            start = pl.multiple_of(b * size + first, HALF)
            rows = size // 32
            tiles = source[pl.ds(pl.multiple_of(b * rows + first // 32, 8), rows), :]
            words = jnp.concatenate(
                [tiles[4 * n : 4 * n + 4, :] for n in range(rows // 4)], axis=1
            )
            element = words[3:4, :].astype(jnp.int32) - 1
            hot_rows = iota((LANES, size), 0)
            hot = (hot_rows == element).astype(jnp.float32).astype(jnp.bfloat16)
            hot = jnp.concatenate([hot, hot], axis=0)
            element = jnp.maximum(element, 0)
            along = [basis_rows(words[d : d + 1, :]) for d in range(3)]
            row = iota((8, size), 0)
            wx = jnp.broadcast_to(along[0][0], (8, size))
            for i in range(1, 8):
                wx = jnp.where(row == i, along[0][i], wx)

            def by_gather(f, h):
                part = slice(h * LANES, h * LANES + LANES)
                index = jnp.broadcast_to(element[:, part], (8, LANES))
                wz = [jnp.broadcast_to(w[:, part], (8, LANES)) for w in along[2]]
                over_j = None
                for j in range(8):
                    over_k = None
                    for k in range(8):
                        row = 64 * k + 8 * j
                        term = wz[k] * jnp.take_along_axis(
                            donors_ref[f, row : row + 8, :], index, axis=1,
                            mode="promise_in_bounds",
                        )
                        over_k = term if over_k is None else over_k + term
                    term = over_k * along[1][j][:, part]
                    over_j = term if over_j is None else over_j + term
                target[f : f + 1, pl.ds(start + h * LANES, LANES)] = jnp.sum(
                    over_j * wx[:, part], axis=0, keepdims=True
                )

            gathers = [(f, h) for f in range(BY_DOT, FIELDS) for h in range(size // LANES)]
            for f in range(BY_DOT):
                picked = lax.dot(fields_ref[f], hot, preferred_element_type=jnp.float32)
                share = -(-len(gathers) // (BY_DOT - f))
                for work in gathers[:share]:
                    by_gather(*work)
                gathers = gathers[share:]
                over_k = picked[0:64, :] * along[2][0]
                for k in range(1, 8):
                    over_k = over_k + picked[64 * k : 64 * k + 64, :] * along[2][k]
                over_j = over_k[0:8, :] * along[1][0]
                for j in range(1, 8):
                    over_j = over_j + over_k[8 * j : 8 * j + 8, :] * along[1][j]
                target[f : f + 1, pl.ds(start, size)] = jnp.sum(
                    over_j * wx, axis=0, keepdims=True
                )

        def whole(b, carry, one_block=one_block):
            one_block(b, 0, BLOCK)
            return carry

        def part(b, carry, one_block=one_block, first=blocks * BLOCK):
            one_block(b, first, HALF)
            return carry

        lax.fori_loop(0, blocks, whole, 0)
        lax.fori_loop(0, left, part, 0)


def eval_far_kernel(place_ref, fields_ref, donors_ref, *refs):
    *refs, far_ref = refs
    eval_kernel(fields_ref, donors_ref, *refs)
    cross_1_ref, cross_2_ref = refs[2:]
    r = place_ref[0] % 4
    far_ref[...] = jnp.zeros(far_ref.shape, jnp.float32)
    far_ref[r] = cross_2_ref[...]
    far_ref[jnp.where(r % 2 == 0, r + 1, r - 1)] = cross_1_ref[...]


def unpack_kernel(
    place_ref, inner_1_ref, middle_ref, inner_2_ref, far_ref, own_ref, moves_ref, owner_ref,
    out_ref,
):
    q = place_ref[0]
    width = N_REC
    below_2, below_1, above_1, above_2 = pick_sides(
        q, inner_1_ref[...], middle_ref[...], inner_2_ref[...], lambda t: far_ref[t]
    )
    zeros = jnp.zeros((FIELDS, CAP), jnp.float32)
    values = [
        jnp.concatenate([value, zeros], axis=1)
        for value in (below_2, below_1, own_ref[...], above_1, above_2)
    ]
    moves = jnp.concatenate([moves_ref[...], jnp.zeros((8, CAP), jnp.int32)], axis=1)
    for b in range(10, -1, -1):
        step = 1 << b
        incoming = pltpu.roll(moves, step, 1)
        moved = (incoming >> b) & 1
        for s in range(5):
            flag = jnp.broadcast_to(moved[s : s + 1, :], (FIELDS, width))
            values[s] = jnp.where(flag == 1, pltpu.roll(values[s], step, 1), values[s])
        moves = jnp.where(moved == 1, incoming, jnp.where((moves >> b) & 1 == 1, 0, moves))
    distance = jnp.broadcast_to(owner_ref[...] - q + 2, (FIELDS, width))
    out = values[0]
    for s in range(1, 5):
        out = jnp.where(distance == s, values[s], out)
    out_ref[...] = out


def share_kernel(
    place_ref, inner_1_ref, middle_ref, inner_2_ref, far_ref, own_ref, moves_ref, owner_ref,
    share_ref,
):
    q = place_ref[0]
    width = N_REC
    below_2, below_1, above_1, above_2 = pick_sides(
        q, inner_1_ref[0:1, :], middle_ref[0:1, :], inner_2_ref[0:1, :],
        lambda t: far_ref[t, 0:1, :],
    )
    row = iota((8, CAP), 0)
    values = jnp.broadcast_to(below_2, (8, CAP))
    for s, value in ((1, below_1), (2, own_ref[0:1, :]), (3, above_1), (4, above_2)):
        values = jnp.where(row == s, value, values)
    values = jnp.concatenate([values, jnp.zeros((8, CAP), jnp.float32)], axis=1)
    moves = jnp.concatenate([moves_ref[...], jnp.zeros((8, CAP), jnp.int32)], axis=1)
    for b in range(10, -1, -1):
        step = 1 << b
        incoming = pltpu.roll(moves, step, 1)
        moved = (incoming >> b) & 1
        values = jnp.where(moved == 1, pltpu.roll(values, step, 1), values)
        moves = jnp.where(moved == 1, incoming, jnp.where((moves >> b) & 1 == 1, 0, moves))
    mine = iota((8, width), 0) == owner_ref[...] - q + 2
    out = jnp.sum(jnp.where(mine, values, 0.0), axis=0, keepdims=True)
    for n in range(16):
        share_ref[n : n + 1, :] = out[:, n * LANES : (n + 1) * LANES]


def prep_kernel(
    place_ref, geometry_ref, wall_ref, forcing_ref, cross_ref, inner_ref,
    inverse_ref, free_ref, load_ref, beside_ref, plane_ref, below_ref, above_ref,
):
    q = place_ref[0]
    below_ref[...], above_ref[...] = by_side(q, cross_ref[32:104, :], inner_ref[32:104, :])
    beside_ref[0:8, :] = below_ref[0:8, :]
    beside_ref[8:16, :] = above_ref[0:8, :]
    wcol = w_column()
    scol = s_column()

    def diagonal(geometry, k, j):
        wk, wj = float(WEIGHTS[k]), float(WEIGHTS[j])
        sk, sj = float(STIFF[k, k]), float(STIFF[j, j])
        return (
            geometry[0:1, :] * (scol * (wk * wj))
            + geometry[1:2, :] * (wcol * (wk * sj))
            + geometry[2:3, :] * (wcol * (sk * wj))
            + geometry[3:4, :] * (wcol * (wk * wj))
        )

    geometry = geometry_ref[...]
    below = below_ref[0:8, :]
    above = above_ref[0:8, :]
    lane = iota((8, LANES), 1)
    row = iota((8, LANES), 0)
    zero = jnp.zeros((8, LANES), jnp.float32)

    def wall_plane(low, high):
        for j in range(8):
            plane_ref[8 * j : 8 * j + 8, :] = zero
        plane_ref[0:8, :] = jnp.where(lane < 8, low, 0.0) + zero
        plane_ref[56:64, :] = jnp.where(lane >= 120, high, 0.0) + zero
        sum_xy(plane_ref, 1)
        return plane_ref[...]

    spread = jnp.where(lane % 8 == row, 1.0, 0.0)
    flags = lax.dot(
        wall_ref[...].astype(jnp.float32), spread, preferred_element_type=jnp.float32
    )
    wall = wall_plane(flags[0:1, :], flags[1:2, :])
    wall_below = wall_plane(below[4:5, :], below[5:6, :])
    wall_above = wall_plane(above[4:5, :], above[5:6, :])
    mark = jnp.where(
        ((row == 0) & (lane % 8 == 0)) | ((row == 7) & (lane % 8 == 7)), 1.0, 0.0
    )
    for j in range(8):
        plane_ref[8 * j : 8 * j + 8, :] = mark
    sum_xy(plane_ref, 1)
    rec = plane_ref[...]
    has_below = jnp.where(q > 0, 1.0, 0.0)
    has_above = jnp.where(q < N_DOM - 1, 1.0, 0.0)
    inner = 1.0 - jnp.minimum(rec + wall, 1.0)
    bottom = 1.0 - jnp.minimum(rec + rec * has_below + (wall + wall_below), 1.0)
    top = 1.0 - jnp.minimum(rec + rec * has_above + (wall + wall_above), 1.0)
    free_ref[0:64, :] = bottom
    free_ref[448:512, :] = top
    for k in range(1, 7):
        free_ref[64 * k : 64 * k + 64, :] = inner

    for k in range(8):
        for j in range(8):
            inverse_ref[(k * 8 + j) * 8 : (k * 8 + j) * 8 + 8, :] = diagonal(geometry, k, j)
    sum_xy(inverse_ref, 8)
    for j in range(8):
        plane_ref[8 * j : 8 * j + 8, :] = diagonal(below, 7, j)
    sum_xy(plane_ref, 1)
    inverse_ref[0:64, :] = inverse_ref[0:64, :] + plane_ref[...]
    for j in range(8):
        plane_ref[8 * j : 8 * j + 8, :] = diagonal(above, 0, j)
    sum_xy(plane_ref, 1)
    inverse_ref[448:512, :] = inverse_ref[448:512, :] + plane_ref[...]
    for k in range(8):
        at = slice(64 * k, 64 * k + 64)
        inverse_ref[at, :] = free_ref[at, :] / inverse_ref[at, :]

    for k in range(8):
        for j in range(8):
            at = slice((k * 8 + j) * 8, (k * 8 + j) * 8 + 8)
            load_ref[at, :] = forcing_ref[at, :] * (
                geometry[3:4, :] * (wcol * float(WEIGHTS[k] * WEIGHTS[j]))
            )
    sum_xy(load_ref, 8)
    for other_ref, k, base in ((below_ref, 7, 0), (above_ref, 0, 448)):
        for j in range(8):
            plane_ref[8 * j : 8 * j + 8, :] = other_ref[8 + 8 * j : 16 + 8 * j, :] * (
                other_ref[3:4, :] * (wcol * float(WEIGHTS[k] * WEIGHTS[j]))
            )
        sum_xy(plane_ref, 1)
        load_ref[base : base + 64, :] = load_ref[base : base + 64, :] + plane_ref[...]


def inverse_multiplicity(q):
    row = iota((64, LANES), 0)
    lane = iota((64, LANES), 1)
    i, j = row % 8, row // 8
    x, y = lane % 8, lane // 8
    along_x = ((i == 0) & (x > 0)) | ((i == 7) & (x < 7))
    along_y = ((j == 0) & (y > 0)) | ((j == 7) & (y < 15))
    inner = jnp.where(along_x, 0.5, 1.0) * jnp.where(along_y, 0.5, 1.0)
    return (
        inner,
        inner * jnp.where(q > 0, 0.5, 1.0),
        inner * jnp.where(q < N_DOM - 1, 0.5, 1.0),
    )


def krylov_step(q, w_ref, inverse_ref, geometry_ref, xmat_ref, v_ref, u_ref, at, moments):
    inner, bottom, top = inverse_multiplicity(q)
    norm = jnp.zeros((64, LANES), jnp.float32)
    for k in range(8):
        rows = slice(64 * k, 64 * k + 64)
        w = w_ref[rows, :]
        v = inverse_ref[rows, :] * w
        v_ref[rows, :] = v
        norm = norm + v * w * (bottom if k == 0 else top if k == 7 else inner)
    energy = apply_local(
        v_ref, geometry_ref[...], xmat_ref, u_ref, tuple(range(8)), dot_with_v=True
    )
    sum_xy(u_ref, 8)
    return moments + lane_value(jnp.sum(norm), at) + lane_value(jnp.sum(energy), at + 1)


def first_kernel(
    place_ref, own_ref, cross_in_ref, inner_in_ref, geometry_ref,
    beside_ref, inverse_ref, free_ref, load_ref, xmat_ref, w_ref, u_ref, edge_ref, lift_ref, moments_ref, cross_ref,
    inner_ref, v_ref, face_ref,
):
    q = place_ref[0]
    below, above = by_side(q, cross_in_ref[...], inner_in_ref[...])
    pick_row = iota((32, 2 * LANES), 0)
    pick_lane = iota((32, 2 * LANES), 1)
    odd = pick_lane // LANES
    picks = [
        jnp.where(
            (pick_lane % LANES == pick_row % 8 * 16 + (8 * odd + 7 * s)) & (pick_row < 24), 1.0, 0.0
        ).astype(jnp.bfloat16)
        for s in range(2)
    ]

    def bf16_parts(value):
        parts = []
        for _ in range(3):
            part = value.astype(jnp.bfloat16)
            parts.append(part.astype(jnp.float32))
            value = value - parts[-1]
        return jnp.concatenate([*parts, jnp.zeros_like(value)], axis=0).astype(jnp.bfloat16)

    layers = (below, own_ref[...], above)
    received = {off: [] for off in range(-1, 2)}
    for s in range(2):
        values = jnp.concatenate([layer[8 * s : 8 * s + 8, :] for layer in layers], axis=1)
        spread = lax.dot_general(
            bf16_parts(values), picks[s], (((0,), (0,)), ((), ())),
            preferred_element_type=jnp.float32,
        )
        for n in range(3):
            at = n * LANES
            plane = spread[at : at + 64, :LANES] + spread[at + 64 : at + 128, LANES:]
            received[n - 1].append([plane[8 * k : 8 * k + 8, :] for k in range(8)])
    lane = iota((8, LANES), 1)
    j_row = iota((8, LANES), 0)
    low = (j_row == 0) & (lane >= 8)
    high = (j_row == 7) & (lane < 120)

    def sum_y(value):
        down = jnp.broadcast_to(pltpu.roll(value, LANES - 8, 1)[0:1, :], (8, LANES))
        up = jnp.broadcast_to(pltpu.roll(value, 8, 1)[7:8, :], (8, LANES))
        return value + jnp.where(high, down, 0.0) + jnp.where(low, up, 0.0)

    count_y = jnp.where(low | high, 2.0, 1.0)
    on_side = [jnp.where(lane % 8 == x, 1.0, 0.0) for x in (0, 7)]

    def boundary(off):
        out = []
        has_below = jnp.where(q + off > 0, 1.0, 0.0)
        has_above = jnp.where(q + off < N_DOM - 1, 1.0, 0.0)
        for s in range(2):
            side = []
            for k in range(8):
                total = received[off][s][k]
                count = count_y * on_side[s]
                if k == 0:
                    if off >= 0:
                        total = total + received[off - 1][s][7]
                    count = count + count * has_below
                if k == 7:
                    if off <= 0:
                        total = total + received[off + 1][s][0]
                    count = count + count * has_above
                side.append(sum_y(total) / jnp.maximum(count, 1.0))
            out.append(jnp.concatenate(side, axis=0))
        return out

    zero = jnp.zeros((64, LANES), jnp.float32)
    for k in range(8):
        v_ref[64 * k : 64 * k + 64, :] = zero
    for off, geometry, plane in ((-1, beside_ref[0:4, :], 7), (1, beside_ref[8:12, :], 0)):
        sides = boundary(off)
        v_ref[pl.ds(0, 64, stride=8), :] = sides[0]
        v_ref[pl.ds(7, 64, stride=8), :] = sides[1]
        at = 0 if off < 0 else 64
        apply_local(v_ref, geometry, xmat_ref, face_ref.at[at : at + 64, :], (plane,))
        sum_xy(face_ref.at[at : at + 64, :], 1)
    sides = boundary(0)
    v_ref[pl.ds(0, 64, stride=8), :] = sides[0]
    v_ref[pl.ds(7, 64, stride=8), :] = sides[1]
    edge_ref[0:64, :] = sides[0]
    edge_ref[64:128, :] = sides[1]
    apply_local(v_ref, geometry_ref[...], xmat_ref, u_ref, tuple(range(8)))
    sum_xy(u_ref, 8)
    lift_ref[0:64, :] = u_ref[0:64, :]
    lift_ref[64:128, :] = u_ref[448:512, :]
    u_ref[0:64, :] = u_ref[0:64, :] + face_ref[0:64, :]
    u_ref[448:512, :] = u_ref[448:512, :] + face_ref[64:128, :]
    for k in range(8):
        rows = slice(64 * k, 64 * k + 64)
        w_ref[rows, :] = free_ref[rows, :] * (load_ref[rows, :] - u_ref[rows, :])
    moments_ref[...] = krylov_step(
        q, w_ref, inverse_ref, geometry_ref, xmat_ref, v_ref, u_ref, 0,
        jnp.zeros((1, LANES), jnp.float32),
    )
    send_faces(q, u_ref, cross_ref, inner_ref)
    up = from_above(q)[0]
    bottom, top = lift_ref[0:64, :], lift_ref[64:128, :]
    cross_ref[64:128, :] = jnp.where(up, top, bottom)
    inner_ref[64:128, :] = jnp.where(up, bottom, top)


def send_faces(q, u_ref, cross_ref, inner_ref):
    up = from_above(q)[0]
    bottom, top = u_ref[0:64, :], u_ref[448:512, :]
    cross_ref[0:64, :] = jnp.where(up, top, bottom)
    inner_ref[0:64, :] = jnp.where(up, bottom, top)


def next_kernel(
    at, place_ref, w_old_ref, u_old_ref, cross_in_ref, inner_in_ref, geometry_ref, inverse_ref,
    free_ref, xmat_ref, moments_old_ref, *refs,
):
    q = place_ref[0]
    if at == 2:
        load_ref, lift_ref, *refs = refs
    w_ref, u_ref, moments_ref, cross_ref, inner_ref, *refs = refs
    v_ref = refs[-1]
    below, above = by_side(q, cross_in_ref[...], inner_in_ref[...])
    for k in range(8):
        rows = slice(64 * k, 64 * k + 64)
        image = u_old_ref[rows, :]
        w_old = w_old_ref[rows, :]
        if k in (0, 7):
            other = below if k == 0 else above
            image = image + other[0:64, :]
            face = slice(0, 64) if k == 0 else slice(64, 128)
            if at == 2:
                w_old = free_ref[rows, :] * (
                    load_ref[rows, :] - (lift_ref[face, :] + other[64:128, :])
                )
                refs[0][face, :] = w_old
        w_ref[rows, :] = free_ref[rows, :] * image - w_old
    row = krylov_step(
        q, w_ref, inverse_ref, geometry_ref, xmat_ref, v_ref, u_ref, at, moments_old_ref[...]
    )
    moments_ref[...] = jnp.broadcast_to(row, moments_ref.shape)
    send_faces(q, u_ref, cross_ref, inner_ref)


def image_kernel(place_ref, u_ref, cross_in_ref, inner_in_ref, free_ref, image_ref):
    below, above = by_side(place_ref[0], cross_in_ref[...], inner_in_ref[...])
    image_ref[...] = free_ref[...] * u_ref[...]
    image_ref[0:64, :] = image_ref[0:64, :] + free_ref[0:64, :] * below
    image_ref[448:512, :] = image_ref[448:512, :] + free_ref[448:512, :] * above


def last_kernel(
    w0_ref, face_ref, w1_ref, w2_ref, image_ref, inverse_ref, edge_ref, moments_ref,
    velocity_ref, residual_ref,
):
    sums = jnp.sum(moments_ref[...], axis=0, keepdims=True)
    h0, a0, h2, a1, h4, a2 = [sums[:, m : m + 1] for m in range(6)]
    h1, h3 = a0 - h0, a1 - h2
    g00, g01, g02, g11, g12, g22 = a0, h2 + h1, h3 + h2, a1, h4 + h3, a2
    b0, b1, b2 = h0, h1, h2
    l10 = g01 / g00
    l20 = g02 / g00
    d1 = g11 - l10 * g01
    e12 = g12 - l10 * g02
    l21 = e12 / d1
    d2 = g22 - l20 * g02 - l21 * e12
    y1 = b1 - l10 * b0
    y2 = b2 - l20 * b0 - l21 * y1
    c2 = y2 / d2
    c1 = y1 / d1 - l21 * c2
    c0 = b0 / g00 - l10 * c1 - l20 * c2
    c0, c1, c2 = [jnp.broadcast_to(c, (64, LANES)) for c in (c0, c1, c2)]
    for k in range(8):
        rows = slice(64 * k, 64 * k + 64)
        w0, w1, w2 = w0_ref[rows, :], w1_ref[rows, :], w2_ref[rows, :]
        if k in (0, 7):
            w0 = face_ref[0:64, :] if k == 0 else face_ref[64:128, :]
        velocity_ref[rows, :] = inverse_ref[rows, :] * (c0 * w0 + c1 * w1 + c2 * w2)
        residual_ref[rows, :] = (
            w0 - c0 * (w1 + w0) - c1 * (w2 + w1) - c2 * image_ref[rows, :]
        )
    for s in range(2):
        rows = pl.ds(7 * s, 64, stride=8)
        velocity_ref[rows, :] = velocity_ref[rows, :] + edge_ref[64 * s : 64 * s + 64, :]


VMEM = pl.BlockSpec(memory_space=pltpu.VMEM)
SMEM = pl.BlockSpec(memory_space=pltpu.SMEM)


def call(kernel, operands, outs, scratch=(), flops=100_000, smem_first=True, mib=12):
    specs = [VMEM] * len(operands)
    if smem_first:
        specs[0] = SMEM
    out_shape = [jax.ShapeDtypeStruct(shape, dtype) for shape, dtype in outs]
    return pl.pallas_call(
        kernel,
        out_shape=out_shape,
        in_specs=specs,
        out_specs=[VMEM] * len(outs),
        scratch_shapes=[pltpu.VMEM(shape, dtype) for shape, dtype in scratch],
        cost_estimate=pl.CostEstimate(flops=flops, bytes_accessed=1_000_000, transcendentals=0),
        compiler_params=pltpu.CompilerParams(vmem_limit_bytes=mib * 1024 * 1024),
    )(*operands)


F32 = jnp.float32
FIELD = ((512, LANES), F32)


def to_all(value):
    return lax.all_to_all(value, "dom", 0, 0, tiled=True)


def to_neighbours(cross_1, inner_1, cross_2=None, inner_2=None):
    lists = ((cross_1, CROSS_1), (cross_2, CROSS_2), (inner_1, INNER_1), (inner_2, INNER_2))
    moved = []
    for value, pairs in lists:
        moved.append(None if value is None else lax.ppermute(value, "dom", pairs))
    return [moved[n] for n in (0, 2, 1, 3) if moved[n] is not None]


def to_four(inner_1, middle, inner_2, far):
    far = lax.all_to_all(far, "dom", 0, 0, tiled=True, axis_index_groups=SHIFTED)
    near = []
    for value, pairs in ((inner_1, INNER_1), (middle, MIDDLE_1), (inner_2, INNER_2)):
        near.append(lax.ppermute(value, "dom", pairs))
    return (*near, far)


def body(donor_fields, interp_weights, donor_owner, donor_element, geometry, wall_flag, forcing):
    place = lax.axis_index("dom").astype(jnp.int32).reshape(1)
    xmat = x_matrix()
    donors = lax.ppermute(donor_fields, "mesh", [(0, 1), (1, 0)])
    owner = donor_owner.reshape(1, N_REC)
    element = donor_element.reshape(1, N_REC)
    asked = ((32, LANES), F32)
    with_head = ((CHUNK, LANES), F32)
    *requests, own, moves = call(
        route_kernel,
        (
            place,
            *(
                pltpu.with_memory_space_constraint(value, pltpu.HBM)
                for value in (interp_weights, owner, element, geometry, wall_flag, forcing)
            ),
        ),
        (with_head, with_head, asked, asked, asked, ((8, CAP), jnp.int32)),
        scratch=(((5, 32, LANES), F32),),
    )
    requests = to_neighbours(*requests)
    (fields,) = call(
        split_kernel, (donors,), (((BY_DOT, 512, 256), jnp.bfloat16),), smem_first=False,
    )
    answer = ((FIELDS, CAP), F32)
    own_answer, inner_1 = call(
        eval_kernel, (fields, donors, own, requests[1]), (answer,) * 2,
        flops=3_000_000_000, smem_first=False, mib=24,
    )
    middle, _, far = call(
        eval_far_kernel, (place, fields, donors, requests[0], requests[2]),
        (answer, answer, ((4, FIELDS, CAP), F32)),
        flops=3_000_000_000, mib=24,
    )
    (inner_2,) = call(
        eval_kernel, (fields, donors, requests[3]), (answer,),
        flops=1_000_000_000, smem_first=False, mib=24,
    )
    answered = to_four(inner_1, middle, inner_2, far)
    inverse, free, load, beside = call(
        prep_kernel, (place, geometry, wall_flag, forcing, requests[0], requests[1]),
        (FIELD, FIELD, FIELD, ((16, LANES), F32)),
        scratch=(((64, LANES), F32), ((72, LANES), F32), ((72, LANES), F32)),
    )
    unpacked = (place, *answered, own_answer, moves, owner)
    (share,) = call(share_kernel, unpacked, (((16, LANES), F32),))
    (interface,) = call(unpack_kernel, unpacked, (((FIELDS, N_REC), F32),))
    face = ((64, LANES), F32)
    two_faces = ((128, LANES), F32)
    w0, u, edge, lift, moments, *faces = call(
        first_kernel,
        (place, share, *to_neighbours(share, share), geometry, beside, inverse, free,
         load, xmat),
        (FIELD, FIELD, two_faces, two_faces, ((1, LANES), F32), two_faces, two_faces),
        scratch=(FIELD, two_faces),
    )
    fixed = (geometry, inverse, free, xmat)
    w1, u, moments, *faces, w0_faces = call(
        functools.partial(next_kernel, 2),
        (place, w0, u, *to_neighbours(*faces), *fixed, moments, load, lift),
        (FIELD, FIELD, ((1, LANES), F32), face, face, two_faces), scratch=(FIELD,),
    )
    w2, u, moments, *faces = call(
        functools.partial(next_kernel, 4),
        (place, w1, u, *to_neighbours(*faces), *fixed, moments),
        (FIELD, FIELD, ((N_DOM, LANES), F32), face, face), scratch=(FIELD,),
    )
    sums = to_all(moments)
    (image,) = call(image_kernel, (place, u, *to_neighbours(*faces), free), (FIELD,))
    velocity, residual = call(
        last_kernel, (w0, w0_faces, w1, w2, image, inverse, edge, sums), (FIELD, FIELD), smem_first=False,
    )
    return velocity, residual, interface


def solution(mesh):
    both = ("mesh", "dom")
    in_specs = (
        P(None, None, both), P(None, None, both), P(both, None), P(both), P(None, both),
        P(None, both), P(None, both),
    )
    out_specs = (P(None, both), P(None, both), P(None, both))

    return jax.shard_map(body, mesh=mesh, in_specs=in_specs, out_specs=out_specs, check_vma=False)
```
